256 devices in a mesh: rep: 32 (over y_lo, z, core), tp: 8 (over x, y_hi).
Axes of the slice: x: 4, y: 4 (y_hi: 2, y_lo: 2; y = y_hi * 2 + y_lo), z: 8, core: 2. Of those that a mesh axis runs over, the one named last changes fastest.
Arguments:
- activations: bfloat16 [16384, 6144], P('rep', 'tp'), may hold values from -6 to 6
- norm_gain: float32 [6144], replicated, may hold values from 0.5 to 1.5
- query_gain: float32 [128], replicated, may hold values from 0.5 to 18
- key_gain: float32 [128], replicated, may hold values from 0.5 to 18
- project_in: bfloat16 [6144, 24, 384], P('rep', 'tp'), may hold values from -1 to 1
- project_out: bfloat16 [6144, 3072], P('rep', 'tp'), may hold values from -1 to 1
Outputs:
- attended: bfloat16 [16384, 6144], P('rep', 'tp')
- weight_norms: float32 [2], replicated
The draws below stay inside these ranges and needn't reach their ends.
All inputs are finite; a program needn't handle non-finite values.
Results may differ from the reference program's by a relative error of at most 0.018.
The reference program's roundings to bfloat16 on the way count: a program that leaves them out, or rounds other values in their place, can miss the bound.
Values may be sent and summed in bfloat16 or wider, within the bound.
A program may use at most 128 MiB of HBM per device.

```python
import math
import jax
import jax.numpy as jnp
from jax import lax

D = 6144
HEADS = 24
HEAD_DIM = 128
PATCHES = 256
IMG_REP = 2
TOKENS = 16384
N_REP = 32
N_TP = 8


def gain_common(key, salt):
    inner = jax.random.fold_in(key, salt)
    base = jax.random.uniform(inner, (HEAD_DIM,), jnp.float32, 0.5, 1.5)
    return base


def draw_query_gain(key, part):
    return gain_common(key, 11)


def draw_key_gain(key, part):
    return gain_common(key, 23)


def rising_rows(key, salt, columns, fan_in):
    inner = jax.random.fold_in(key, salt)
    entries = jax.random.truncated_normal(inner, -4.0, 4.0, (D, columns), jnp.float32)
    factor = 5.0
    place = jnp.arange(D).astype(jnp.float32) / (D - 1)
    scales = 1.0 + (factor - 1.0) * place
    scales = scales / jnp.sqrt(jnp.mean(scales * scales))
    return entries * scales[:, None] * fan_in ** (-0.5)


def draw_project_in(key, part):
    values = rising_rows(key, 31, HEADS * 3 * HEAD_DIM, D)
    return values.reshape(D, HEADS, 3 * HEAD_DIM).astype(jnp.bfloat16)


def draw_project_out(key, part):
    return rising_rows(key, 47, HEADS * HEAD_DIM, HEADS * HEAD_DIM).astype(jnp.bfloat16)


def steps_of(rng, dims, pieces, low, high):
    def one(axis_at, parts):
        steps = jax.random.uniform(jax.random.fold_in(jax.random.fold_in(rng, 6), axis_at), (parts,), jnp.float32, low / len(pieces), high / len(pieces))
        return jnp.repeat(jnp.exp(steps), dims[axis_at] // parts).reshape((-1,) + (1,) * (len(dims) - axis_at - 1))

    loudness = one(*pieces[0])
    for cut in pieces[1:]:
        loudness = loudness * one(*cut)
    return loudness


def gaussian(key, dims, deviation, most, pieces=(), dtype=jnp.bfloat16):
    result = deviation * jax.random.normal(key, dims, jnp.float32)
    if pieces:
        result = result * steps_of(key, dims, pieces, -0.22, 0.18)
    return jnp.clip(result, -most, most).astype(dtype)


def setup_inputs(seed: int = 0) -> dict:
    arg_keys = jax.random.split(jax.random.key(seed), 7)
    return {
        "activations": gaussian(arg_keys[0], (TOKENS, D), 1.0, 6.0, ((0, 32), (1, 8))),
        "norm_gain": jnp.clip(1.0 + 0.1 * jax.random.normal(arg_keys[1], (D,), jnp.float32), 0.5, 1.5),
        "query_gain": draw_query_gain(jax.random.fold_in(arg_keys[6], 71), 0),
        "key_gain": draw_key_gain(jax.random.fold_in(arg_keys[6], 71), 0),
        "project_in": draw_project_in(jax.random.fold_in(arg_keys[6], 71), 0),
        "project_out": draw_project_out(jax.random.fold_in(arg_keys[6], 71), 0),
    }


def layer_norm(values, gain):
    average = lax.optimization_barrier(jnp.mean(values, -1, keepdims=True))
    centred = values - average
    variance = lax.optimization_barrier(jnp.mean(centred * centred, -1, keepdims=True))
    return centred * lax.rsqrt(variance + 1e-06) * gain

def reference(activations, norm_gain, query_gain, key_gain, project_in, project_out):
    normed = layer_norm(activations.astype(jnp.float32), norm_gain).astype(jnp.bfloat16)
    projection = project_in.reshape(D, HEADS * 3 * HEAD_DIM)

    def one_image(patches_in):
        projected = jnp.dot(patches_in, projection, preferred_element_type=jnp.float32)
        projected = projected.reshape(PATCHES, HEADS, 3 * HEAD_DIM)
        queries = layer_norm(projected[..., :HEAD_DIM], query_gain).astype(jnp.bfloat16)
        keys_normed = layer_norm(projected[..., HEAD_DIM:2 * HEAD_DIM], key_gain).astype(jnp.bfloat16)
        values = projected[..., 2 * HEAD_DIM:].astype(jnp.bfloat16)
        scores = jnp.einsum('phd,qhd->hpq', queries.astype(jnp.float32), keys_normed.astype(jnp.float32)) / math.sqrt(HEAD_DIM)
        probabilities = jax.nn.softmax(scores, axis=-1).astype(jnp.bfloat16)
        mixed = jnp.einsum('hpq,qhd->phd', probabilities.astype(jnp.float32), values.astype(jnp.float32))
        return mixed.astype(jnp.bfloat16).reshape(PATCHES, HEADS * HEAD_DIM)
    mixed = lax.map(one_image, normed.reshape(IMG_REP * N_REP, PATCHES, D))
    mixed = mixed.reshape(IMG_REP * N_REP * PATCHES, HEADS * HEAD_DIM)
    columns_each = HEADS * HEAD_DIM // N_TP
    total = jnp.zeros((mixed.shape[0], D), jnp.float32)
    for group_index in range(N_TP):
        lower = group_index * columns_each
        partial_value = lax.dot_general(mixed[:, lower:lower + columns_each], project_out[:, lower:lower + columns_each], (((1,), (1,)), ((), ())), preferred_element_type=jnp.float32)
        partial_value = lax.optimization_barrier(partial_value.astype(jnp.bfloat16))
        total = total + partial_value.astype(jnp.float32)
    attended = total.astype(jnp.bfloat16)
    weight_norms = jnp.stack([jnp.sqrt(jnp.sum(jnp.square(project_in.astype(jnp.float32))) / (3 * HEADS * HEAD_DIM)), jnp.sqrt(jnp.sum(jnp.square(project_out.astype(jnp.float32))) / D)])
    return (attended, weight_norms)
```

```python
import math

import jax
import jax.numpy as jnp
from jax import lax
from jax.experimental import pallas as pl
from jax.experimental.pallas import tpu as pltpu
from jax.sharding import PartitionSpec as P

D = 6144
HEADS = 24
HEAD_DIM = 128
PATCHES = 256
NX, NZ = 4, 8
MESH = pl.DeviceIdType.MESH
F32, BF16 = jnp.float32, jnp.bfloat16
EPS = 1e-06
NSEM = 160


def dot_nt(a, b):
    return lax.dot_general(a, b, (((1,), (1,)), ((), ())), preferred_element_type=F32)


def kernel(
    x_ref, gain_ref, qg_ref, kg_ref, w_ref, wo_ref, out_ref, norm_ref,
    gi, go, xg, acc, mixed, part, r1, r2, r3, tsum, nown, nrecv,
    send, recv, local,
):
    rep, tp = lax.axis_index("rep"), lax.axis_index("tp")
    c = lax.rem(rep, 2)
    z = lax.rem(lax.div(rep, 2), NZ)
    yl = lax.div(rep, 2 * NZ)
    x, yh = lax.div(tp, 2), lax.rem(tp, 2)

    def rep_of(yl_, z_, c_):
        return (yl_ * NZ + z_) * 2 + c_

    zp, zm = lax.rem(z + 1, NZ), lax.rem(z + NZ - 1, NZ)
    xp, xm = lax.rem(x + 1, NX), lax.rem(x + NX - 1, NX)
    xf = lax.rem(x + 2, NX)
    dev = {
        "z+": (rep_of(yl, zp, c), tp),
        "z-": (rep_of(yl, zm, c), tp),
        "c": (rep_of(yl, z, 1 - c), tp),
        "y": (rep_of(1 - yl, z, c), tp),
        "x+": (rep, xp * 2 + yh),
        "x-": (rep, xm * 2 + yh),
        "h": (rep, x * 2 + 1 - yh),
    }

    barrier = pltpu.get_barrier_semaphore()
    for d in dev.values():
        pl.semaphore_signal(barrier, inc=1, device_id=d, device_id_type=MESH)
    pl.semaphore_wait(barrier, len(dev))

    ids = {}
    started = []

    def ident(name):
        return ids.setdefault(name, len(ids))

    def push(name, src, dst, to):
        k = ident(name)
        copy = pltpu.make_async_remote_copy(
            src_ref=src, dst_ref=dst, send_sem=send.at[k], recv_sem=recv.at[k],
            device_id=dev[to], device_id_type=MESH,
        )
        copy.start()
        started.append((name, copy))

    def take(name, dst):
        k = ident(name)
        pltpu.make_async_remote_copy(
            src_ref=dst, dst_ref=dst, send_sem=send.at[k], recv_sem=recv.at[k],
            device_id=dev["c"], device_id_type=MESH,
        ).wait_recv()

    def sent(prefix):
        for item in [s for s in started if s[0].startswith(prefix)]:
            item[1].wait_send()
            started.remove(item)

    def piece(other, dz, partner=0):
        yl_ = 1 - yl if other else yl
        c_ = 1 - c if partner else c
        return rep_of(yl_, lax.rem(z + dz + NZ, NZ), c_)

    me_r, me_t = piece(0, 0), tp
    push("ah", x_ref, xg.at[me_t], "h")
    push("ax+own", x_ref, xg.at[me_t], "x+")
    push("ax-own", x_ref, xg.at[me_t], "x-")
    push("iz+1own", w_ref, gi.at[me_r], "z+")
    push("iz-1own", w_ref, gi.at[me_r], "z-")
    push("iy0", w_ref, gi.at[me_r], "y")
    push("ic own0", w_ref, gi.at[me_r], "c")
    locals_ = [
        pltpu.make_async_copy(x_ref, xg.at[me_t], local.at[0]),
        pltpu.make_async_copy(w_ref, gi.at[me_r], local.at[1]),
        pltpu.make_async_copy(wo_ref, go.at[me_r], local.at[2]),
    ]
    for copy in locals_:
        copy.start()

    def half(ref, sign):
        rows = ref.shape[0] // 2
        return ref.at[pl.ds(0 if sign == "+" else rows, rows)]

    def opp(sign):
        return 1 if sign == "+" else -1

    def take_z(kind, buf, col, sign, d):
        r = piece(col == "oth", -opp(sign) * d)
        ref = buf.at[r]
        take(kind + "z" + sign + str(d) + col, half(ref, sign) if d == NZ // 2 else ref)

    def push_z(kind, buf, col, sign, d):
        r = piece(col == "oth", -opp(sign) * (d - 1))
        ref = buf.at[r]
        ref = half(ref, sign) if d == NZ // 2 else ref
        push(kind + "z" + sign + str(d) + col, ref, ref, "z" + sign)

    def swap(kind, buf, col, dz):
        ref = buf.at[piece(col == "oth", dz)]
        push(kind + "c " + col + str(dz), ref, ref, "c")

    def cross(kind, buf, dz):
        ref = buf.at[piece(0, dz)]
        push(kind + "y" + str(dz), ref, ref, "y")

    def take_cross(kind, buf, dz):
        take(kind + "y" + str(dz), buf.at[piece(1, dz)])

    def take_swap(kind, buf, col, dz):
        take(kind + "c " + col + str(dz), buf.at[piece(col == "oth", dz, 1)])

    tile = {
        "own+": xm * 2 + yh, "own-": xp * 2 + yh,
        "par+": xm * 2 + 1 - yh, "par-": xp * 2 + 1 - yh,
        "ownf": xf * 2 + yh, "parf": xf * 2 + 1 - yh,
    }

    def acts_step(who):
        for sign in "+-":
            ref = xg.at[tile[who + sign]]
            take("ax" + sign + who, ref)
            push("ax" + sign + who + "f", half(ref, sign), half(ref, sign), "x" + sign)

    def acts_far(who):
        for sign in "+-":
            take("ax" + sign + who + "f", half(xg.at[tile[who + "f"]], sign))

    for sign in "+-":
        take_z("i", gi, "own", sign, 1)
        push_z("i", gi, "own", sign, 2)
        cross("i", gi, -opp(sign))
        swap("i", gi, "own", -opp(sign))
    take_cross("i", gi, 0)
    swap("i", gi, "oth", 0)
    acts_step("own")
    par = xg.at[x * 2 + 1 - yh]
    take("ah", par)
    push("ax+par", par, par, "x+")
    push("ax-par", par, par, "x-")
    for sign in "+-":
        take_z("i", gi, "own", sign, 2)
        push_z("i", gi, "own", sign, 3)
        swap("i", gi, "own", -2 * opp(sign))
    push("oy0", wo_ref, go.at[me_r], "y")
    push("oc own0", wo_ref, go.at[me_r], "c")
    for sign in "+-":
        take_cross("i", gi, -opp(sign))
        push_z("i", gi, "oth", sign, 2)
        swap("i", gi, "oth", -opp(sign))
    for sign in "+-":
        take_z("i", gi, "own", sign, 3)
        push_z("i", gi, "own", sign, 4)
        swap("i", gi, "own", -3 * opp(sign))
    acts_far("own")
    for sign in "+-":
        take_z("i", gi, "oth", sign, 2)
        push_z("i", gi, "oth", sign, 3)
        swap("i", gi, "oth", -2 * opp(sign))
    acts_step("par")
    for sign in "+-":
        take_z("i", gi, "own", sign, 4)
    swap("i", gi, "own", 4)
    for sign in "+-":
        take_z("i", gi, "oth", sign, 3)
        push_z("i", gi, "oth", sign, 4)
        push("oz" + sign + "1own", wo_ref, go.at[me_r], "z" + sign)
        swap("i", gi, "oth", -3 * opp(sign))
    acts_far("par")
    sent("ax")
    sent("ah")
    locals_[0].wait()

    def norm_rows(i, carry):
        rows = pl.ds(pl.multiple_of(i * 32, 32), 32)

        def lanes(v):
            total = v[:, :128]
            for j in range(1, 6):
                total = total + v[:, j * 128:(j + 1) * 128]
            return total

        total = jnp.zeros((32, 128), F32)
        for t in range(8):
            total = total + lanes(xg[t, rows, :].astype(F32))
        mean = jnp.sum(total, -1, keepdims=True) * (1.0 / D)
        total = jnp.zeros((32, 128), F32)
        for t in range(8):
            v = xg[t, rows, :].astype(F32) - mean
            total = total + lanes(v * v)
        scale = lax.rsqrt(jnp.sum(total, -1, keepdims=True) * (1.0 / D) + EPS)
        for t in range(8):
            v = (xg[t, rows, :].astype(F32) - mean) * scale * gain_ref[pl.ds(t, 1), :]
            xg[t, rows, :] = v.astype(BF16)
        return carry

    lax.fori_loop(0, 16, norm_rows, 0)

    for sign in "+-":
        take_z("i", gi, "oth", sign, 4)
    swap("i", gi, "oth", 4)
    for col in ("own", "oth"):
        for dz in (0, 1, -1, 2, -2, 3, -3, 4):
            take_swap("i", gi, col, dz)
    locals_[1].wait()

    def project(k, first):
        def rows_step(m, carry):
            rows = pl.ds(pl.multiple_of(m * 256, 256), 256)
            w = gi[pl.ds(k * 4, 4)].reshape(768, 1152)
            value = jnp.dot(xg[k, rows, :], w, preferred_element_type=F32)
            if first:
                acc[rows, :] = value
            else:
                acc[rows, :] += value
            return carry

        lax.fori_loop(0, 2, rows_step, 0)

    def project_many(lo, hi):
        def step(k, carry):
            project(k, False)
            return carry

        lax.fori_loop(lo, hi, step, 0)

    def out_ring(d):
        for sign in "+-":
            take_z("o", go, "own", sign, d)
            if d < 4:
                push_z("o", go, "own", sign, d + 1)
                cross("o", go, -opp(sign) * d)
                swap("o", go, "own", -opp(sign) * d)
        if d == 4:
            cross("o", go, 4)
            swap("o", go, "own", 4)

    project(0, True)
    out_ring(1)
    project_many(1, 3)
    out_ring(2)
    project_many(3, 5)
    out_ring(3)
    project_many(5, 8)
    out_ring(4)

    def head_norm(v, gain):
        v = v - jnp.mean(v, -1, keepdims=True)
        var = jnp.mean(v * v, -1, keepdims=True)
        return (v * lax.rsqrt(var + EPS) * gain).astype(BF16)

    def attend(i, carry):
        rows = pl.ds(pl.multiple_of(i * PATCHES, PATCHES), PATCHES)
        for h in range(3):
            lo = h * 3 * HEAD_DIM
            q = head_norm(acc[rows, lo:lo + HEAD_DIM], qg_ref[...])
            k = head_norm(acc[rows, lo + HEAD_DIM:lo + 2 * HEAD_DIM], kg_ref[...])
            v = acc[rows, lo + 2 * HEAD_DIM:lo + 3 * HEAD_DIM].astype(BF16)
            s = dot_nt(q, k) / math.sqrt(HEAD_DIM)
            e = jnp.exp(s - jnp.max(s, -1, keepdims=True))
            p = (e / jnp.sum(e, -1, keepdims=True)).astype(BF16)
            o = jnp.dot(p, v, preferred_element_type=F32)
            mixed[rows, h * HEAD_DIM:(h + 1) * HEAD_DIM] = o.astype(BF16)
        return carry

    lax.fori_loop(0, 2, attend, 0)

    for dz in (0, 1, -1, 2, -2, 3, -3, 4):
        take_cross("o", go, dz)
        swap("o", go, "oth", dz)
    for col in ("own", "oth"):
        for dz in (0, 1, -1, 2, -2, 3, -3, 4):
            take_swap("o", go, col, dz)
    locals_[2].wait()

    def out_part(t):
        w = go[pl.ds(t * 4, 4)].reshape(768, 384)
        part[t] = dot_nt(mixed[...], w).astype(BF16)

    a_rows, b_rows = pl.ds(0, 256), pl.ds(256, 256)
    span = {"+": a_rows, "-": b_rows}
    other = {"+": b_rows, "-": a_rows}
    ys = {"p": 1 - yh, "o": yh}
    near = {"+": xp, "-": xm}

    for g in "po":
        t = xf * 2 + ys[g]
        out_part(t)
        for i, sign in enumerate("+-"):
            push("f" + sign + g, part.at[t, span[sign]], r1.at["po".index(g), i], "x" + sign)
    for g in "po":
        for i, sign in enumerate("+-"):
            t = near[sign] * 2 + ys[g]
            out_part(t)
            push("n" + sign + g + "d", part.at[t, other[sign]], r2.at["po".index(g), i, other[sign]], "x" + sign)
        for i, sign in enumerate("+-"):
            t = near[sign] * 2 + ys[g]
            take("f" + sign + g, r1.at["po".index(g), i])
            part[t, span[sign]] = (part[t, span[sign]].astype(F32) + r1["po".index(g), i].astype(F32)).astype(BF16)
            push("n" + sign + g + "s", part.at[t, span[sign]], r2.at["po".index(g), i, span[sign]], "x" + sign)
        out_part(x * 2 + ys[g])

    def squares(ref, r, total):
        v = ref[r].astype(F32)
        v = v * v
        w = v.shape[1]
        row = v[:, :128]
        for j in range(1, w // 128):
            row = row + v[:, j * 128:(j + 1) * 128]
        return total + jnp.sum(row.reshape(24, 8, 128), 0)

    zero = jnp.zeros((8, 128), F32)
    nown[0, pl.ds(0, 8), :] = lax.fori_loop(0, 32, lambda r, t: squares(gi, r, t), zero)
    nown[0, pl.ds(8, 8), :] = lax.fori_loop(0, 32, lambda r, t: squares(go, r, t), zero)

    x1 = x + 1 - 2 * lax.rem(x, 2)
    dev["n0"] = dev["h"]
    dev["n1"] = (rep, x1 * 2 + yh)
    dev["n2"] = (rep, (NX - 1 - x) * 2 + yh)

    def norm_push(s):
        push("norm" + str(s), nown.at[s], nrecv.at[s], "n" + str(s))

    def norm_take(s):
        take("norm" + str(s), nrecv.at[s])
        nown[s + 1] = nown[s] + nrecv[s]

    norm_push(0)

    def take_near(g, rows, sign):
        i = "+-".index(sign)
        kind = "s" if rows is span[sign] else "d"
        take("n" + sign + g + kind, r2.at["po".index(g), i, rows])

    mine = x * 2 + yh
    theirs = x * 2 + 1 - yh
    for sign in "+-":
        take_near("p", other[sign], sign)
    for sign in "+-":
        take_near("p", span[sign], sign)
    for n, rows in enumerate((a_rows, b_rows)):
        total = part[theirs, rows].astype(F32) + r2[0, 0, rows].astype(F32) + r2[0, 1, rows].astype(F32)
        tsum[rows] = total.astype(BF16)
        push("t" + str(n), tsum.at[rows], r3.at[rows], "h")
    norm_take(0)
    norm_push(1)
    for sign in "+-":
        take_near("o", other[sign], sign)
    norm_take(1)
    norm_push(2)
    norm_take(2)
    total_in = jnp.sum(nown[3, pl.ds(0, 8), :], keepdims=True)
    total_out = jnp.sum(nown[3, pl.ds(8, 8), :], keepdims=True)
    norm_ref[pl.ds(0, 1), :] = jnp.broadcast_to(jnp.sqrt(total_in / (3 * HEADS * HEAD_DIM)), (1, 128))
    norm_ref[pl.ds(1, 1), :] = jnp.broadcast_to(jnp.sqrt(total_out / D), (1, 128))
    for n, rows in enumerate((a_rows, b_rows)):
        take("t" + str(n), r3.at[rows])
    for sign in "+-":
        take_near("o", span[sign], sign)
    for rows in (a_rows, b_rows):
        total = part[mine, rows].astype(F32) + r2[1, 0, rows].astype(F32) + r2[1, 1, rows].astype(F32)
        out_ref[rows] = (total + r3[rows].astype(F32)).astype(BF16)
    sent("")
    assert len(ids) <= NSEM


def shards(activations, norm_gain, query_gain, key_gain, project_in, project_out):
    rows, cols = activations.shape
    depth = project_in.shape[0]
    vmem = pl.BlockSpec(memory_space=pltpu.VMEM)
    out, norms = pl.pallas_call(
        kernel,
        name="block",
        out_shape=(jax.ShapeDtypeStruct((rows, cols), BF16), jax.ShapeDtypeStruct((2, 128), F32)),
        in_specs=[vmem] * 6,
        out_specs=(vmem, vmem),
        scratch_shapes=[
            pltpu.VMEM((32, 192, 1152), BF16),
            pltpu.VMEM((32, 192, 384), BF16),
            pltpu.VMEM((8, 512, 768), BF16),
            pltpu.VMEM((512, 1152), F32),
            pltpu.VMEM((512, 384), BF16),
            pltpu.VMEM((8, 512, 768), BF16),
            pltpu.VMEM((2, 2, 256, 768), BF16),
            pltpu.VMEM((2, 2, 512, 768), BF16),
            pltpu.VMEM((512, 768), BF16),
            pltpu.VMEM((512, 768), BF16),
            pltpu.VMEM((4, 16, 128), F32),
            pltpu.VMEM((3, 16, 128), F32),
            pltpu.SemaphoreType.DMA((NSEM,)),
            pltpu.SemaphoreType.DMA((NSEM,)),
            pltpu.SemaphoreType.DMA((3,)),
        ],
        compiler_params=pltpu.CompilerParams(
            collective_id=0, has_side_effects=True, vmem_limit_bytes=63 * 1024 * 1024
        ),
    )(
        activations,
        norm_gain.reshape(8, 768),
        query_gain.reshape(1, HEAD_DIM),
        key_gain.reshape(1, HEAD_DIM),
        project_in.reshape(depth, -1),
        project_out,
    )
    return out, norms[:, 0]


def solution(mesh):
    return jax.shard_map(
        shards,
        mesh=mesh,
        in_specs=(P("rep", "tp"), P(), P(), P(), P("rep", "tp", None), P("rep", "tp")),
        out_specs=(P("rep", "tp"), P()),
        check_vma=False,
    )
```

```python
import math

import jax
import jax.numpy as jnp
from jax import lax
from jax.experimental import pallas as pl
from jax.experimental.pallas import tpu as pltpu
from jax.sharding import PartitionSpec as P

D = 6144
HEADS = 24
HEAD_DIM = 128
PATCHES = 256
NX, NZ = 4, 8
MESH = pl.DeviceIdType.MESH
F32, BF16 = jnp.float32, jnp.bfloat16
EPS = 1e-06
NSEM = 160


def dot_nt(a, b):
    return lax.dot_general(a, b, (((1,), (1,)), ((), ())), preferred_element_type=F32)


def kernel(
    x_ref, gain_ref, qg_ref, kg_ref, w_ref, wo_ref, out_ref, norm_ref,
    gi, go, xg, acc, mixed, part, r1, r2, r3, r4, tsum, nown, nrecv,
    send, recv, local,
):
    rep, tp = lax.axis_index("rep"), lax.axis_index("tp")
    c = lax.rem(rep, 2)
    z = lax.rem(lax.div(rep, 2), NZ)
    yl = lax.div(rep, 2 * NZ)
    x, yh = lax.div(tp, 2), lax.rem(tp, 2)

    def rep_of(yl_, z_, c_):
        return (yl_ * NZ + z_) * 2 + c_

    zp, zm = lax.rem(z + 1, NZ), lax.rem(z + NZ - 1, NZ)
    xp, xm = lax.rem(x + 1, NX), lax.rem(x + NX - 1, NX)
    xf = lax.rem(x + 2, NX)
    dev = {
        "z+": (rep_of(yl, zp, c), tp),
        "z-": (rep_of(yl, zm, c), tp),
        "c": (rep_of(yl, z, 1 - c), tp),
        "y": (rep_of(1 - yl, z, c), tp),
        "x+": (rep, xp * 2 + yh),
        "x-": (rep, xm * 2 + yh),
        "h": (rep, x * 2 + 1 - yh),
    }

    ids = {}
    started = []

    def ident(name):
        return ids.setdefault(name, len(ids))

    def push(name, src, dst, to):
        k = ident(name)
        copy = pltpu.make_async_remote_copy(
            src_ref=src, dst_ref=dst, send_sem=send.at[k], recv_sem=recv.at[k],
            device_id=dev[to], device_id_type=MESH,
        )
        copy.start()
        started.append((name, copy))

    def take(name, dst):
        k = ident(name)
        pltpu.make_async_remote_copy(
            src_ref=dst, dst_ref=dst, send_sem=send.at[k], recv_sem=recv.at[k],
            device_id=dev["c"], device_id_type=MESH,
        ).wait_recv()

    def sent(prefix):
        for item in [s for s in started if s[0].startswith(prefix)]:
            item[1].wait_send()
            started.remove(item)

    def piece(other, dz, partner=0):
        yl_ = 1 - yl if other else yl
        c_ = 1 - c if partner else c
        return rep_of(yl_, lax.rem(z + dz + NZ, NZ), c_)

    me_r, me_t = piece(0, 0), tp
    own_x, own_w, own_o = xg.at[me_t], gi.at[me_r], go.at[me_r]
    fetch = [pltpu.make_async_copy(x_ref, own_x, local.at[0])]
    for h in range(3):
        fetch.append(pltpu.make_async_copy(w_ref.at[h], own_w.at[:, pl.ds(h * 384, 384)], local.at[1 + h]))
    fetch.append(pltpu.make_async_copy(wo_ref, own_o, local.at[4]))
    for copy in fetch:
        copy.start()

    barrier = pltpu.get_barrier_semaphore()
    for d in dev.values():
        pl.semaphore_signal(barrier, inc=1, device_id=d, device_id_type=MESH)
    pl.semaphore_wait(barrier, len(dev))

    fetch[0].wait()
    push("ah", own_x, own_x, "h")
    push("ax+own", own_x, own_x, "x+")
    push("ax-own", own_x, own_x, "x-")
    for copy in fetch[1:4]:
        copy.wait()
    rows96 = (pl.ds(0, 96), pl.ds(96, 96))
    for n in (0, 1):
        for sign, m in (("+", n), ("-", 1 - n)):
            ref = gi.at[me_r, rows96[m]]
            push("iz" + sign + "1own" + str(m), ref, ref, "z" + sign)
    push("ic own0", own_w, own_w, "c")
    fetch[4].wait()

    def rows_of(ref, n):
        rows = ref.shape[0] // 2
        return ref.at[pl.ds(n * rows, rows)]

    def opp(sign):
        return 1 if sign == "+" else -1

    def lead(sign):
        return 0 if sign == "+" else 1

    def take_z(kind, buf, col, sign, d, n):
        ref = rows_of(buf.at[piece(col == "oth", -opp(sign) * d)], n)
        take(kind + "z" + sign + str(d) + col + str(n), ref)

    def push_z(kind, buf, col, sign, d, n):
        ref = rows_of(buf.at[piece(col == "oth", -opp(sign) * (d - 1))], n)
        push(kind + "z" + sign + str(d) + col + str(n), ref, ref, "z" + sign)

    def swap(kind, buf, col, dz):
        ref = buf.at[piece(col == "oth", dz)]
        push(kind + "c " + col + str(dz), ref, ref, "c")

    def cross(kind, buf, dz):
        ref = buf.at[piece(0, dz)]
        push(kind + "y" + str(dz), ref, ref, "y")

    def take_cross(kind, buf, dz):
        take(kind + "y" + str(dz), buf.at[piece(1, dz)])

    def take_swap(kind, buf, col, dz):
        take(kind + "c " + col + str(dz), buf.at[piece(col == "oth", dz, 1)])

    tile = {
        "own+": xm * 2 + yh, "own-": xp * 2 + yh,
        "par+": xm * 2 + 1 - yh, "par-": xp * 2 + 1 - yh,
        "ownf": xf * 2 + yh, "parf": xf * 2 + 1 - yh,
    }

    def acts_step(who):
        for sign in "+-":
            ref = xg.at[tile[who + sign]]
            take("ax" + sign + who, ref)
            ref = rows_of(ref, lead(sign))
            push("ax" + sign + who + "f", ref, ref, "x" + sign)

    def acts_far(who):
        for sign in "+-":
            take("ax" + sign + who + "f", rows_of(xg.at[tile[who + "f"]], lead(sign)))

    def relay(kind, buf, col, d, which, onward=True):
        for sign in "+-":
            n = lead(sign) if which == "lead" else 1 - lead(sign)
            take_z(kind, buf, col, sign, d, n)
            if onward and (d < 3 or (d == 3 and which == "lead")):
                push_z(kind, buf, col, sign, d + 1, n)

    def swap_both(kind, buf, col, d):
        for sign in "+-":
            swap(kind, buf, col, -opp(sign) * d)

    def whole(kind, buf, d):
        for which in ("lead", "rest"):
            relay(kind, buf, "own", d, which)
        for sign in "+-":
            cross(kind, buf, -opp(sign) * d)
            swap(kind, buf, "own", -opp(sign) * d)

    relay("i", gi, "own", 1, "lead")
    relay("i", gi, "own", 1, "rest")
    for dz in (1, -1):
        cross("i", gi, dz)
        swap("i", gi, "own", dz)
    push("iy0", own_w, own_w, "y")
    push("oy0", own_o, own_o, "y")
    push("oc own0", own_o, own_o, "c")
    for sign in "+-":
        for n in (lead(sign), 1 - lead(sign)):
            push_z("o", go, "own", sign, 1, n)
    relay("i", gi, "own", 2, "lead")
    par = xg.at[x * 2 + 1 - yh]
    take("ah", par)
    push("ax+par", par, par, "x+")
    push("ax-par", par, par, "x-")
    acts_step("own")
    relay("i", gi, "own", 2, "rest")
    swap_both("i", gi, "own", 2)
    relay("i", gi, "own", 3, "lead")
    whole("o", go, 1)
    take_cross("i", gi, 1)
    for n in (1, 0):
        push_z("i", gi, "oth", "-", 2, n)
    swap("i", gi, "oth", 1)
    relay("i", gi, "own", 3, "rest")
    swap_both("i", gi, "own", 3)
    take_cross("i", gi, -1)
    for n in (0, 1):
        push_z("i", gi, "oth", "+", 2, n)
    swap("i", gi, "oth", -1)
    relay("i", gi, "own", 4, "lead", False)
    swap("i", gi, "own", 4)
    acts_step("par")
    whole("o", go, 2)
    acts_far("own")
    relay("i", gi, "oth", 2, "lead")
    take_cross("i", gi, 0)
    swap("i", gi, "oth", 0)
    relay("i", gi, "oth", 2, "rest")
    swap_both("i", gi, "oth", 2)
    whole("o", go, 3)
    acts_far("par")
    sent("ax")
    sent("ah")

    def norm_rows(i, carry):
        rows = pl.ds(pl.multiple_of(i * 32, 32), 32)

        def lanes(v):
            total = v[:, :128]
            for j in range(1, 6):
                total = total + v[:, j * 128:(j + 1) * 128]
            return total

        total = jnp.zeros((32, 128), F32)
        for t in range(8):
            total = total + lanes(xg[t, rows, :].astype(F32))
        mean = jnp.sum(total, -1, keepdims=True) * (1.0 / D)
        total = jnp.zeros((32, 128), F32)
        for t in range(8):
            v = xg[t, rows, :].astype(F32) - mean
            total = total + lanes(v * v)
        scale = lax.rsqrt(jnp.sum(total, -1, keepdims=True) * (1.0 / D) + EPS)
        for t in range(8):
            v = (xg[t, rows, :].astype(F32) - mean) * scale * gain_ref[pl.ds(t * 768, 768)].reshape(1, 768)
            xg[t, rows, :] = v.astype(BF16)
        return carry

    lax.fori_loop(0, 16, norm_rows, 0)

    relay("i", gi, "oth", 3, "lead")
    for dz in (0, 1, -1, 2, -2, 3, -3, 4):
        take_swap("i", gi, "own", dz)

    def project(k, first):
        def rows_step(m, carry):
            rows = pl.ds(pl.multiple_of(m * 256, 256), 256)
            w = gi[pl.ds(k * 4, 4)].reshape(768, 1152)
            value = jnp.dot(xg[k, rows, :], w, preferred_element_type=F32)
            if first:
                acc[rows, :] = value
            else:
                acc[rows, :] += value
            return carry

        lax.fori_loop(0, 2, rows_step, 0)

    def project_many(lo, hi):
        def step(k, carry):
            project(k, False)
            return carry

        lax.fori_loop(lo, hi, step, 0)

    near_k, far_k = yl * 4, (1 - yl) * 4
    project(near_k, True)
    project_many(near_k + 1, near_k + 3)
    relay("i", gi, "oth", 3, "rest")
    swap_both("i", gi, "oth", 3)
    project_many(near_k + 3, near_k + 4)
    relay("o", go, "own", 4, "lead", False)
    cross("o", go, 4)
    swap("o", go, "own", 4)
    for dz in (0, 1, -1, 2, -2, 3, -3):
        take_swap("i", gi, "oth", dz)
    last = lax.div(lax.rem(z + 4, NZ), 2)

    def far_step(j, carry):
        project(far_k + lax.rem(last + 1 + j, 4), False)
        return carry

    lax.fori_loop(0, 2, far_step, 0)
    relay("i", gi, "oth", 4, "lead", False)
    swap("i", gi, "oth", 4)
    lax.fori_loop(2, 3, far_step, 0)
    take_swap("i", gi, "oth", 4)
    lax.fori_loop(3, 4, far_step, 0)

    def head_norm(v, gain):
        v = v - jnp.mean(v, -1, keepdims=True)
        var = jnp.mean(v * v, -1, keepdims=True)
        return (v * lax.rsqrt(var + EPS) * gain).astype(BF16)

    def attend(i, carry):
        rows = pl.ds(pl.multiple_of(i * PATCHES, PATCHES), PATCHES)
        for h in range(3):
            lo = h * 3 * HEAD_DIM
            q = head_norm(acc[rows, lo:lo + HEAD_DIM], qg_ref[...].reshape(1, HEAD_DIM))
            k = head_norm(acc[rows, lo + HEAD_DIM:lo + 2 * HEAD_DIM], kg_ref[...].reshape(1, HEAD_DIM))
            v = acc[rows, lo + 2 * HEAD_DIM:lo + 3 * HEAD_DIM].astype(BF16)
            s = dot_nt(q, k) / math.sqrt(HEAD_DIM)
            e = jnp.exp(s - jnp.max(s, -1, keepdims=True))
            p = (e / jnp.sum(e, -1, keepdims=True)).astype(BF16)
            o = jnp.dot(p, v, preferred_element_type=F32)
            mixed[rows, h * HEAD_DIM:(h + 1) * HEAD_DIM] = o.astype(BF16)
        return carry

    lax.fori_loop(0, 2, attend, 0)

    for dz in (0, 1, -1, 2, -2, 3, -3, 4):
        take_cross("o", go, dz)
        swap("o", go, "oth", dz)
    for col in ("own", "oth"):
        for dz in (0, 1, -1, 2, -2, 3, -3, 4):
            take_swap("o", go, col, dz)

    def out_part(t):
        w = go[pl.ds(t * 4, 4)].reshape(768, 384)
        part[t] = dot_nt(mixed[...], w).astype(BF16)

    a_rows, b_rows = pl.ds(0, 256), pl.ds(256, 256)
    span = {"+": a_rows, "-": b_rows}
    other = {"+": b_rows, "-": a_rows}
    ys = {"p": 1 - yh, "o": yh}
    near = {"+": xp, "-": xm}

    far_p, far_o = xf * 2 + ys["p"], xf * 2 + ys["o"]
    out_part(far_p)
    push("fh", part.at[far_p], r4, "h")
    for sign in "+-":
        t = near[sign] * 2 + ys["p"]
        out_part(t)
        for i, rows in enumerate((a_rows, b_rows)):
            push("n" + sign + "p" + str(i), part.at[t, rows], r2.at[0, "+-".index(sign), rows], "x" + sign)
    out_part(far_o)
    for sign in "+-":
        out_part(near[sign] * 2 + ys["o"])
    for g in "po":
        out_part(x * 2 + ys[g])

    def squares(ref, r, total):
        v = ref[r].astype(F32)
        v = v * v
        w = v.shape[1]
        row = v[:, :128]
        for j in range(1, w // 128):
            row = row + v[:, j * 128:(j + 1) * 128]
        return total + jnp.sum(row.reshape(24, 8, 128), 0)

    zero = jnp.zeros((8, 128), F32)
    nown[0, pl.ds(0, 8), :] = lax.fori_loop(0, 32, lambda r, t: squares(gi, r, t), zero)
    nown[0, pl.ds(8, 8), :] = lax.fori_loop(0, 32, lambda r, t: squares(go, r, t), zero)

    x1 = x + 1 - 2 * lax.rem(x, 2)
    dev["n0"] = dev["h"]
    dev["n1"] = (rep, x1 * 2 + yh)
    dev["n2"] = (rep, (NX - 1 - x) * 2 + yh)

    def norm_push(s):
        push("norm" + str(s), nown.at[s], nrecv.at[s], "n" + str(s))

    def norm_take(s):
        take("norm" + str(s), nrecv.at[s])
        nown[s + 1] = nown[s] + nrecv[s]

    norm_push(0)

    mine = x * 2 + yh
    theirs = x * 2 + 1 - yh

    def hand_over(n):
        rows = (a_rows, b_rows)[n]
        for i, sign in enumerate("+-"):
            take("n" + sign + "p" + str(n), r2.at[0, i, rows])
        total = part[theirs, rows].astype(F32) + r2[0, 0, rows].astype(F32) + r2[0, 1, rows].astype(F32)
        tsum[rows] = total.astype(BF16)
        push("t" + str(n), tsum.at[rows], r3.at[rows], "h")

    hand_over(0)
    take("fh", r4)
    for i, sign in enumerate("+-"):
        rows = span[sign]
        part[far_o, rows] = (part[far_o, rows].astype(F32) + r4[rows].astype(F32)).astype(BF16)
        push("f" + sign, part.at[far_o, rows], r1.at[i], "x" + sign)
    for i, sign in enumerate("+-"):
        t = near[sign] * 2 + yh
        push("n" + sign + "od", part.at[t, other[sign]], r2.at[1, i, other[sign]], "x" + sign)
    hand_over(1)
    norm_take(0)
    norm_push(1)
    for i, sign in enumerate("+-"):
        t = near[sign] * 2 + yh
        take("f" + sign, r1.at[i])
        part[t, span[sign]] = (part[t, span[sign]].astype(F32) + r1[i].astype(F32)).astype(BF16)
        push("n" + sign + "os", part.at[t, span[sign]], r2.at[1, i, span[sign]], "x" + sign)
    norm_take(1)
    norm_push(2)
    for i, sign in enumerate("+-"):
        take("n" + sign + "od", r2.at[1, i, other[sign]])
    for n, rows in enumerate((a_rows, b_rows)):
        take("t" + str(n), r3.at[rows])
    norm_take(2)
    total_in = jnp.sum(nown[3, pl.ds(0, 8), :], keepdims=True)
    total_out = jnp.sum(nown[3, pl.ds(8, 8), :], keepdims=True)
    norm_ref[0] = (total_in / (3 * HEADS * HEAD_DIM))[0, 0]
    norm_ref[1] = (total_out / D)[0, 0]
    for i, sign in enumerate("+-"):
        take("n" + sign + "os", r2.at[1, i, span[sign]])
    for rows in (a_rows, b_rows):
        total = part[mine, rows].astype(F32) + r2[1, 0, rows].astype(F32) + r2[1, 1, rows].astype(F32)
        out_ref[rows] = (total + r3[rows].astype(F32)).astype(BF16)
    sent("")
    assert len(ids) <= NSEM


def shards(activations, norm_gain, query_gain, key_gain, project_in, project_out):
    rows, cols = activations.shape
    hbm = pl.BlockSpec(memory_space=pl.ANY)
    vmem = pl.BlockSpec(memory_space=pltpu.VMEM)
    out, norms = pl.pallas_call(
        kernel,
        name="block",
        out_shape=(jax.ShapeDtypeStruct((rows, cols), BF16), jax.ShapeDtypeStruct((2,), F32)),
        in_specs=[hbm, vmem, vmem, vmem, hbm, hbm],
        out_specs=(vmem, pl.BlockSpec(memory_space=pltpu.SMEM)),
        scratch_shapes=[
            pltpu.VMEM((32, 192, 1152), BF16),
            pltpu.VMEM((32, 192, 384), BF16),
            pltpu.VMEM((8, 512, 768), BF16),
            pltpu.VMEM((512, 1152), F32),
            pltpu.VMEM((512, 384), BF16),
            pltpu.VMEM((8, 512, 768), BF16),
            pltpu.VMEM((2, 256, 768), BF16),
            pltpu.VMEM((2, 2, 512, 768), BF16),
            pltpu.VMEM((512, 768), BF16),
            pltpu.VMEM((512, 768), BF16),
            pltpu.VMEM((512, 768), BF16),
            pltpu.VMEM((4, 16, 128), F32),
            pltpu.VMEM((3, 16, 128), F32),
            pltpu.SemaphoreType.DMA((NSEM,)),
            pltpu.SemaphoreType.DMA((NSEM,)),
            pltpu.SemaphoreType.DMA((5,)),
        ],
        compiler_params=pltpu.CompilerParams(
            collective_id=0, has_side_effects=True, vmem_limit_bytes=63 * 1024 * 1024
        ),
    )(
        activations,
        norm_gain,
        query_gain,
        key_gain,
        project_in.transpose(1, 0, 2),
        project_out,
    )
    return out, jnp.sqrt(norms)


def solution(mesh):
    return jax.shard_map(
        shards,
        mesh=mesh,
        in_specs=(P("rep", "tp"), P(), P(), P(), P("rep", "tp", None), P("rep", "tp")),
        out_specs=(P("rep", "tp"), P()),
        check_vma=False,
    )
```

```python
import math

import jax
import jax.numpy as jnp
from jax import lax
from jax.experimental import pallas as pl
from jax.experimental.pallas import tpu as pltpu
from jax.sharding import PartitionSpec as P

D = 6144
HEADS = 24
HEAD_DIM = 128
PATCHES = 256
NX, NZ = 4, 8
MESH = pl.DeviceIdType.MESH
F32, BF16 = jnp.float32, jnp.bfloat16
EPS = 1e-06
NSEM = 85


def dot_nt(a, b):
    return lax.dot_general(a, b, (((1,), (1,)), ((), ())), preferred_element_type=F32)


def kernel(
    x_ref, gain_ref, qg_ref, kg_ref, w_ref, wo_ref, out_ref, norm_ref,
    gi, go, xg, means, spread, stage, acc, mixed, part, r1, r2, r3, r4, tsum, nown, nrecv,
    send, recv, local,
):
    rep, tp = lax.axis_index("rep"), lax.axis_index("tp")
    c = lax.rem(rep, 2)
    z = lax.rem(lax.div(rep, 2), NZ)
    yl = lax.div(rep, 2 * NZ)
    x, yh = lax.div(tp, 2), lax.rem(tp, 2)

    def rep_of(yl_, z_, c_):
        return (yl_ * NZ + z_) * 2 + c_

    zp, zm = lax.rem(z + 1, NZ), lax.rem(z + NZ - 1, NZ)
    xp, xm = lax.rem(x + 1, NX), lax.rem(x + NX - 1, NX)
    xf = lax.rem(x + 2, NX)
    dev = {
        "z+": (rep_of(yl, zp, c), tp),
        "z-": (rep_of(yl, zm, c), tp),
        "c": (rep_of(yl, z, 1 - c), tp),
        "y": (rep_of(1 - yl, z, c), tp),
        "x+": (rep, xp * 2 + yh),
        "x-": (rep, xm * 2 + yh),
        "h": (rep, x * 2 + 1 - yh),
    }

    ids, parity = {}, [None]
    groups = "aiors"
    sizes = {(g, which): 0 for g in groups for which in (None, 0, 1)}

    def on(which, action):
        @pl.when(lax.rem(z, 2) == which)
        def _():
            parity[0] = which
            action()
            parity[0] = None

    def ident(name):
        return ids.setdefault(name, len(ids))

    def push(name, src, dst, to, group=None):
        k = ident(name)
        group = group or name[0]
        pltpu.make_async_remote_copy(
            src_ref=src, dst_ref=dst, send_sem=send.at[groups.index(group)], recv_sem=recv.at[k],
            device_id=dev[to], device_id_type=MESH,
        ).start()
        sizes[group, parity[0]] += math.prod(src.shape)

    def take(name, dst):
        k = ident(name)
        pltpu.make_async_remote_copy(
            src_ref=dst, dst_ref=dst, send_sem=send.at[0], recv_sem=recv.at[k],
            device_id=dev["c"], device_id_type=MESH,
        ).wait_recv()

    def sent(group, which=None):
        like = {"a": xg, "i": gi, "o": go, "r": part, "s": nown}[group]
        total = sizes[group, None] + (sizes[group, which] if which is not None else 0)
        count, rest = divmod(total, math.prod(like.shape[1:]))
        assert rest == 0 and count <= like.shape[0]
        ref = like.at[pl.ds(0, count)]
        pltpu.make_async_remote_copy(
            src_ref=ref, dst_ref=ref, send_sem=send.at[groups.index(group)], recv_sem=recv.at[0],
            device_id=dev["c"], device_id_type=MESH,
        ).wait_send()

    table = {
        (other, dz, partner): rep_of(
            1 - yl if other else yl, lax.rem(z + dz + NZ, NZ), 1 - c if partner else c
        )
        for other in (0, 1) for dz in range(-4, 5) for partner in (0, 1)
    }

    def piece(other, dz, partner=0):
        return table[int(other), dz, partner]

    me_r, me_t = piece(0, 0), tp
    own_x, own_w, own_o = xg.at[me_t], gi.at[me_r], go.at[me_r]
    fetch = [pltpu.make_async_copy(x_ref, own_x, local.at[0])]
    for h in range(3):
        fetch.append(pltpu.make_async_copy(w_ref.at[h], own_w.at[:, pl.ds(h * 384, 384)], local.at[1 + h]))
    fetch.append(pltpu.make_async_copy(wo_ref, own_o, local.at[4]))
    for copy in fetch:
        copy.start()

    barrier = pltpu.get_barrier_semaphore()
    for d in dev.values():
        pl.semaphore_signal(barrier, inc=1, device_id=d, device_id_type=MESH)
    pl.semaphore_wait(barrier, len(dev))

    fetch[0].wait()
    push("ah", own_x, own_x, "h")
    push("ax+own", own_x, own_x, "x+")
    push("ax-own", own_x, own_x, "x-")
    for copy in fetch[1:4]:
        copy.wait()
    rows96 = (pl.ds(0, 96), pl.ds(96, 96))
    for n in (0, 1):
        for sign, m in (("+", n), ("-", 1 - n)):
            ref = gi.at[me_r, rows96[m]]
            push("iz" + sign + "1own" + str(m), ref, ref, "z" + sign)
    push("icown", own_w, own_w, "c")
    fetch[4].wait()

    def rows_of(ref, n):
        rows = ref.shape[0] // 2
        return ref.at[pl.ds(n * rows, rows)]

    def opp(sign):
        return 1 if sign == "+" else -1

    def lead(sign):
        return 0 if sign == "+" else 1

    def take_z(kind, buf, col, sign, d, n):
        ref = rows_of(buf.at[piece(col == "oth", -opp(sign) * d)], n)
        take(kind + "z" + sign + str(d) + col + str(n), ref)

    def push_z(kind, buf, col, sign, d, n):
        ref = rows_of(buf.at[piece(col == "oth", -opp(sign) * (d - 1))], n)
        push(kind + "z" + sign + str(d) + col + str(n), ref, ref, "z" + sign)

    def swap(col, dz):
        ref = gi.at[piece(col == "oth", dz)]
        push("ic" + (col if dz < 4 or col == "own" else "last"), ref, ref, "c")

    def swap_o(wave, col, dz):
        ref = go.at[piece(col == "oth", dz)]
        push("oc" + str(wave), ref, ref, "c")

    def cross_o(wave, dz):
        ref = go.at[piece(0, dz)]
        push("oy" + str(wave), ref, ref, "y")

    def cross_half(buf, dz, n):
        ref = rows_of(buf.at[piece(0, dz)], n)
        push("iy" + str(dz) + "h" + str(n), ref, ref, "y")

    def take_cross_half(buf, dz, n):
        take("iy" + str(dz) + "h" + str(n), rows_of(buf.at[piece(1, dz)], n))

    tile = {
        "own+": xm * 2 + yh, "own-": xp * 2 + yh,
        "par+": xm * 2 + 1 - yh, "par-": xp * 2 + 1 - yh,
        "ownf": xf * 2 + yh, "parf": xf * 2 + 1 - yh,
    }

    def acts_step(who):
        for sign in "+-":
            ref = xg.at[tile[who + sign]]
            take("ax" + sign + who, ref)
            ref = rows_of(ref, lead(sign))
            push("ax" + sign + who + "f", ref, ref, "x" + sign)

    def acts_far(who):
        for sign in "+-":
            take("ax" + sign + who + "f", rows_of(xg.at[tile[who + "f"]], lead(sign)))

    def relay(kind, buf, col, d, which, onward=True):
        for sign in "+-":
            n = lead(sign) if which == "lead" else 1 - lead(sign)
            take_z(kind, buf, col, sign, d, n)
            if onward and (d < 3 or (d == 3 and which == "lead")):
                push_z(kind, buf, col, sign, d + 1, n)

    def swap_both(col, d):
        for sign in "+-":
            swap(col, -opp(sign) * d)

    def o_ref(col, sign, d, at):
        ref = go.at[piece(col == "oth", -opp(sign) * at)]
        return rows_of(ref, lead(sign)) if d == 4 else ref

    def push_o(col, d):
        for sign in "+-":
            ref = o_ref(col, sign, d, d - 1)
            push("oz" + sign + str(d) + col, ref, ref, "z" + sign)

    def take_o(col, d):
        for sign in "+-":
            take("oz" + sign + str(d) + col, o_ref(col, sign, d, d))

    def offsets(d):
        return (d,) if d in (0, 4) else (-d, d)

    def first_wave(d):
        def step():
            if d:
                take_o("own", d)
            if d < 4:
                push_o("own", d + 1)
            for dz in offsets(d):
                cross_o(1, dz)
                swap_o(1, "own", dz)

        on(d % 2, step)

    def first_wave_over():
        take("oy1", go.at[pl.ds(0, 4)])
        for which in (0, 1):
            def step(which=which):
                for d in range(which, 5, 2):
                    for dz in offsets(d):
                        swap_o(1, "oth", dz)

            on(which, step)

    def second_wave_cross():
        on(1, lambda: cross_o(2, 0))

    def second_wave(d, *cols):
        def step():
            for col in cols:
                if d:
                    take_o(col, d)
                elif col == "oth":
                    take("oy2", go.at[piece(1, 0)])
                if d < 4:
                    push_o(col, d + 1)
                for dz in offsets(d):
                    swap_o(2, col, dz)

        on(1 - d % 2, step)

    def lane_tiles(t, rows):
        return [xg[t, rows, j * 128:(j + 1) * 128].astype(F32) for j in range(6)]

    def measure(t, first=False):
        def step(i, carry):
            for part_ in range(4):
                rows = pl.ds(pl.multiple_of(i * 128 + part_ * 32, 32), 32)
                tiles = lane_tiles(t, rows)
                total = tiles[0]
                for v in tiles[1:]:
                    total = total + v
                mean = jnp.sum(total, -1, keepdims=True) * (1.0 / 768)
                square = jnp.zeros((32, 128), F32)
                for v in tiles:
                    v = v - mean
                    square = square + v * v
                means[t, rows, :] = jnp.broadcast_to(mean, (32, 128))
                spread[rows, :] = square if first else spread[rows, :] + square
            return carry

        lax.fori_loop(0, 4, step, 0)

    def norm_rows(i, carry):
        for part_ in range(4):
            rows = pl.ds(pl.multiple_of(i * 128 + part_ * 32, 32), 32)
            mean = means[0, rows, :]
            for t in range(1, 8):
                mean = mean + means[t, rows, :]
            mean = mean * (1.0 / 8)
            apart = jnp.zeros((32, 128), F32)
            for t in range(8):
                v = means[t, rows, :] - mean
                apart = apart + v * v
            variance = (jnp.sum(spread[rows, :], -1, keepdims=True) + 768.0 * apart) * (1.0 / D)
            scale = lax.rsqrt(variance + EPS)
            for t in range(8):
                for j, v in enumerate(lane_tiles(t, rows)):
                    gain = gain_ref[pl.ds(t * 768 + j * 128, 128)].reshape(1, 128)
                    xg[t, rows, j * 128:(j + 1) * 128] = ((v - mean) * scale * gain).astype(BF16)
        return carry

    measure(me_t, True)
    relay("i", gi, "own", 1, "lead")
    relay("i", gi, "own", 1, "rest")
    for dz, n in ((1, 1), (-1, 0), (1, 0), (-1, 1)):
        cross_half(gi, dz, n)
    for dz in (1, -1):
        swap("own", dz)
    push("iy0", own_w, own_w, "y")
    first_wave(0)
    second_wave_cross()
    relay("i", gi, "own", 2, "lead")
    par = xg.at[x * 2 + 1 - yh]
    take("ah", par)
    push("ax+par", par, par, "x+")
    push("ax-par", par, par, "x-")
    acts_step("own")
    relay("i", gi, "own", 2, "rest")
    swap_both("own", 2)
    measure(x * 2 + 1 - yh)
    for sign in "+-":
        measure(tile["own" + sign])
    relay("i", gi, "own", 3, "lead")
    first_wave(1)
    for dz, sign in ((1, "-"), (-1, "+")):
        take_cross_half(gi, dz, lead(sign))
        push_z("i", gi, "oth", sign, 2, lead(sign))
    relay("i", gi, "own", 3, "rest")
    swap_both("own", 3)
    for dz, sign in ((1, "-"), (-1, "+")):
        take_cross_half(gi, dz, 1 - lead(sign))
        push_z("i", gi, "oth", sign, 2, 1 - lead(sign))
        swap("oth", dz)
    relay("i", gi, "own", 4, "lead", False)
    swap("own", 4)
    acts_step("par")
    for sign in "+-":
        measure(tile["par" + sign])
    first_wave(2)
    relay("i", gi, "oth", 2, "lead")
    acts_far("own")
    measure(tile["ownf"])
    take("iy0", gi.at[piece(1, 0)])
    swap("oth", 0)
    relay("i", gi, "oth", 2, "rest")
    swap_both("oth", 2)
    first_wave(3)
    acts_far("par")
    measure(tile["parf"])
    sent("a")
    lax.fori_loop(0, 4, norm_rows, 0)
    relay("i", gi, "oth", 3, "lead")
    take("icown", gi.at[pl.ds(0, 8)])

    def product(k):
        return jnp.dot(xg[k], gi[pl.ds(k * 4, 4)].reshape(768, 1152), preferred_element_type=F32)

    near_k, far_k = yl * 4, (1 - yl) * 4
    acc[...] = product(near_k) + product(near_k + 1)
    relay("i", gi, "oth", 3, "rest")
    swap_both("oth", 3)
    first_wave(4)
    second_wave(0, "own", "oth")
    acc[...] += product(near_k + 2) + product(near_k + 3)
    take("icoth", gi.at[pl.ds(0, 7)])
    last = lax.div(lax.rem(z + 4, NZ), 2)

    def far_chunk(j):
        return product(far_k + lax.rem(last + 1 + j, 4))

    acc[...] += far_chunk(0) + far_chunk(1)
    relay("i", gi, "oth", 4, "lead", False)
    swap("oth", 4)
    first_wave_over()
    acc[...] += far_chunk(2)
    take("iclast", gi.at[piece(1, 4, 1)])
    acc[...] += far_chunk(3)
    second_wave(1, "own")

    def head_norm(v, gain):
        v = v - jnp.mean(v, -1, keepdims=True)
        var = jnp.mean(v * v, -1, keepdims=True)
        return (v * lax.rsqrt(var + EPS) * gain).astype(BF16)

    def attend(i, carry):
        rows = pl.ds(pl.multiple_of(i * PATCHES, PATCHES), PATCHES)
        for h in range(3):
            lo = h * 3 * HEAD_DIM
            q = head_norm(acc[rows, lo:lo + HEAD_DIM], qg_ref[...].reshape(1, HEAD_DIM))
            k = head_norm(acc[rows, lo + HEAD_DIM:lo + 2 * HEAD_DIM], kg_ref[...].reshape(1, HEAD_DIM))
            v = acc[rows, lo + 2 * HEAD_DIM:lo + 3 * HEAD_DIM].astype(BF16)
            s = dot_nt(q, k) / math.sqrt(HEAD_DIM)
            e = jnp.exp(s - jnp.max(s, -1, keepdims=True))
            p = (e / jnp.sum(e, -1, keepdims=True)).astype(BF16)
            o = jnp.dot(p, v, preferred_element_type=F32)
            mixed[rows, h * HEAD_DIM:(h + 1) * HEAD_DIM] = o.astype(BF16)
        return carry

    lax.fori_loop(0, 2, attend, 0)

    second_wave(1, "oth")
    take("oc1", go.at[pl.ds(0, 8)])

    def out_part(t, n):
        w = go[pl.ds(t * 4 + n * 2, 2)].reshape(384, 384)
        part[t, n] = dot_nt(mixed[...], w).astype(BF16)

    a_rows, b_rows = pl.ds(0, 256), pl.ds(256, 256)
    span = {"+": a_rows, "-": b_rows}
    other = {"+": b_rows, "-": a_rows}
    near_o = {"+": xp * 2 + yh, "-": xm * 2 + yh}
    near_p = {"+": xp * 2 + 1 - yh, "-": xm * 2 + 1 - yh}
    far_o, far_p = xf * 2 + yh, xf * 2 + 1 - yh
    mine, theirs = x * 2 + yh, x * 2 + 1 - yh
    signs = tuple(enumerate("+-"))

    def launch(n):
        for i, sign in signs:
            t = near_p[sign]
            out_part(t, n)
            push("n" + sign + "p" + str(n), part.at[t, n], r2.at[0, i, n], "x" + sign, "r")
        out_part(far_p, n)
        push("fh" + str(n), part.at[far_p, n], r4.at[n], "h", "r")
        for i, sign in signs:
            t = near_o[sign]
            out_part(t, n)
            push("n" + sign + "d" + str(n), part.at[t, n, other[sign]], r2.at[1, i, n, other[sign]], "x" + sign, "r")
        out_part(far_o, n)
        out_part(theirs, n)
        out_part(mine, n)

    def plus(a, b):
        return (a.astype(F32) + b.astype(F32)).astype(BF16)

    def far(n):
        take("fh" + str(n), r4.at[n])
        for i, sign in signs:
            rows = span[sign]
            part[far_o, n, rows] = plus(part[far_o, n, rows], r4[n, rows])
            push("f" + sign + str(n), part.at[far_o, n, rows], r1.at[n, i], "x" + sign, "r")

    def near_add(n):
        for i, sign in signs:
            t, rows = near_o[sign], span[sign]
            take("f" + sign + str(n), r1.at[n, i])
            part[t, n, rows] = plus(part[t, n, rows], r1[n, i])

    def near_push(n):
        for i, sign in signs:
            t, rows = near_o[sign], span[sign]
            push("n" + sign + "s" + str(n), part.at[t, n, rows], r2.at[1, i, n, rows], "x" + sign, "r")

    def hand_over(n):
        for i, sign in signs:
            take("n" + sign + "p" + str(n), r2.at[0, i, n])
        total = part[theirs, n].astype(F32) + r2[0, 0, n].astype(F32) + r2[0, 1, n].astype(F32)
        tsum[n] = total.astype(BF16)
        push("t" + str(n), tsum.at[n], r3.at[n], "h", "r")

    done = []

    def finish(n):
        take("t" + str(n), r3.at[n])
        for i, sign in signs:
            take("n" + sign + "d" + str(n), r2.at[1, i, n, other[sign]])
        for i, sign in signs:
            take("n" + sign + "s" + str(n), r2.at[1, i, n, span[sign]])
            rows = span[sign]
            total = part[mine, n, rows].astype(F32) + r2[1, 0, n, rows].astype(F32)
            total = total + r2[1, 1, n, rows].astype(F32)
            stage[n, rows] = (total + r3[n, rows].astype(F32)).astype(BF16)
            copy = pltpu.make_async_copy(
                stage.at[n, rows], out_ref.at[rows, pl.ds(n * 384, 384)], local.at[2 * n + i]
            )
            copy.start()
            done.append(copy)

    def squares(ref, r, total):
        v = ref[r].astype(F32)
        v = v * v
        row = v[:, :128]
        for j in range(1, v.shape[1] // 128):
            row = row + v[:, j * 128:(j + 1) * 128]
        return total + jnp.sum(row.reshape(24, 8, 128), 0)

    zero = jnp.zeros((8, 128), F32)
    x1 = x + 1 - 2 * lax.rem(x, 2)
    dev["n0"] = dev["c"]
    dev["n1"] = (rep, x1 * 2 + yh)
    dev["n2"] = (rep, (NX - 1 - x) * 2 + yh)
    dev["n3"] = dev["h"]

    def norm_push(k):
        push("norm" + str(k), nown.at[k], nrecv.at[k], "n" + str(k), "s")

    def norm_take(k):
        take("norm" + str(k), nrecv.at[k])
        nown[k + 1] = nown[k] + nrecv[k]

    launch(0)
    second_wave(2, "own")
    nown[0, pl.ds(0, 8), :] = lax.fori_loop(0, 16, lambda r, t: squares(gi, 2 * r + c, t), zero)
    second_wave(2, "oth")
    second_wave(3, "own")
    hand_over(0)
    far(0)
    second_wave(3, "oth")
    second_wave(4, "own", "oth")
    take("oc2", go.at[pl.ds(0, 8)])
    launch(1)
    nown[0, pl.ds(8, 8), :] = lax.fori_loop(0, 16, lambda r, t: squares(go, 2 * r + c, t), zero)
    norm_push(0)
    near_add(0)
    norm_take(0)
    norm_push(1)
    hand_over(1)
    far(1)
    near_push(0)
    norm_take(1)
    norm_push(2)
    near_add(1)
    near_push(1)
    norm_take(2)
    norm_push(3)
    finish(0)
    norm_take(3)
    total_in = jnp.sum(nown[4, pl.ds(0, 8), :], keepdims=True)
    total_out = jnp.sum(nown[4, pl.ds(8, 8), :], keepdims=True)
    norm_ref[0] = (total_in / (3 * HEADS * HEAD_DIM))[0, 0]
    norm_ref[1] = (total_out / D)[0, 0]
    finish(1)
    for copy in done:
        copy.wait()
    for group in "irs":
        sent(group)
    for which in (0, 1):
        pl.when(lax.rem(z, 2) == which)(lambda which=which: sent("o", which))
    assert len(ids) == NSEM, len(ids)


def shards(activations, norm_gain, query_gain, key_gain, project_in, project_out):
    rows, cols = activations.shape
    hbm = pl.BlockSpec(memory_space=pl.ANY)
    vmem = pl.BlockSpec(memory_space=pltpu.VMEM)
    out, norms = pl.pallas_call(
        kernel,
        name="block",
        out_shape=(jax.ShapeDtypeStruct((rows, cols), BF16), jax.ShapeDtypeStruct((2,), F32)),
        in_specs=[hbm, vmem, vmem, vmem, hbm, hbm],
        out_specs=(hbm, pl.BlockSpec(memory_space=pltpu.SMEM)),
        scratch_shapes=[
            pltpu.VMEM((32, 192, 1152), BF16),
            pltpu.VMEM((32, 192, 384), BF16),
            pltpu.VMEM((8, 512, 768), BF16),
            pltpu.VMEM((8, 512, 128), F32),
            pltpu.VMEM((512, 128), F32),
            pltpu.VMEM((2, 512, 384), BF16),
            pltpu.VMEM((512, 1152), F32),
            pltpu.VMEM((512, 384), BF16),
            pltpu.VMEM((8, 2, 512, 384), BF16),
            pltpu.VMEM((2, 2, 256, 384), BF16),
            pltpu.VMEM((2, 2, 2, 512, 384), BF16),
            pltpu.VMEM((2, 512, 384), BF16),
            pltpu.VMEM((2, 512, 384), BF16),
            pltpu.VMEM((2, 512, 384), BF16),
            pltpu.VMEM((5, 16, 128), F32),
            pltpu.VMEM((4, 16, 128), F32),
            pltpu.SemaphoreType.DMA((5,)),
            pltpu.SemaphoreType.DMA((NSEM,)),
            pltpu.SemaphoreType.DMA((5,)),
        ],
        compiler_params=pltpu.CompilerParams(
            collective_id=0, has_side_effects=True, vmem_limit_bytes=63 * 1024 * 1024
        ),
    )(
        activations,
        norm_gain,
        query_gain,
        key_gain,
        project_in.transpose(1, 0, 2),
        project_out,
    )
    return out, jnp.sqrt(norms)


def solution(mesh):
    return jax.shard_map(
        shards,
        mesh=mesh,
        in_specs=(P("rep", "tp"), P(), P(), P(), P("rep", "tp", None), P("rep", "tp")),
        out_specs=(P("rep", "tp"), P()),
        check_vma=False,
    )
```

```python
import math

import jax
import jax.numpy as jnp
from jax import lax
from jax.experimental import pallas as pl
from jax.experimental.pallas import tpu as pltpu
from jax.sharding import PartitionSpec as P

D = 6144
HEADS = 24
HEAD_DIM = 128
PATCHES = 256
NX, NZ = 4, 8
MESH = pl.DeviceIdType.MESH
F32, BF16 = jnp.float32, jnp.bfloat16
EPS = 1e-06
NSEM = 96


def dot_nt(a, b):
    return lax.dot_general(a, b, (((1,), (1,)), ((), ())), preferred_element_type=F32)


def kernel(
    x_ref, gain_ref, qg_ref, kg_ref, w_ref, wo_ref, out_ref, norm_ref,
    gi, go, xg, means, spread, stage, acc, mixed, part, r1, r2, r3, r4, tsum, nown, nrecv,
    send, recv, local,
):
    rep, tp = lax.axis_index("rep"), lax.axis_index("tp")
    c = lax.rem(rep, 2)
    z = lax.rem(lax.div(rep, 2), NZ)
    yl = lax.div(rep, 2 * NZ)
    x, yh = lax.div(tp, 2), lax.rem(tp, 2)

    def rep_of(yl_, z_, c_):
        return (yl_ * NZ + z_) * 2 + c_

    zp, zm = lax.rem(z + 1, NZ), lax.rem(z + NZ - 1, NZ)
    xp, xm = lax.rem(x + 1, NX), lax.rem(x + NX - 1, NX)
    xf = lax.rem(x + 2, NX)
    dev = {
        "z+": (rep_of(yl, zp, c), tp),
        "z-": (rep_of(yl, zm, c), tp),
        "z++": (rep_of(yl, lax.rem(z + 2, NZ), c), tp),
        "z--": (rep_of(yl, lax.rem(z + NZ - 2, NZ), c), tp),
        "c": (rep_of(yl, z, 1 - c), tp),
        "y": (rep_of(1 - yl, z, c), tp),
        "x+": (rep, xp * 2 + yh),
        "x-": (rep, xm * 2 + yh),
        "h": (rep, x * 2 + 1 - yh),
    }

    ids, parity = {}, [None]
    groups = "aiorsw"
    sizes = {(g, which): 0 for g in groups for which in (None, 0, 1)}

    def on(which, action):
        @pl.when(lax.rem(z, 2) == which)
        def _():
            parity[0] = which
            action()
            parity[0] = None

    def ident(name):
        return ids.setdefault(name, len(ids))

    def push(name, src, dst, to, group=None):
        k = ident(name)
        group = group or name[0]
        pltpu.make_async_remote_copy(
            src_ref=src, dst_ref=dst, send_sem=send.at[groups.index(group)], recv_sem=recv.at[k],
            device_id=dev[to], device_id_type=MESH,
        ).start()
        sizes[group, parity[0]] += math.prod(src.shape)

    def take(name, dst):
        k = ident(name)
        pltpu.make_async_remote_copy(
            src_ref=dst, dst_ref=dst, send_sem=send.at[0], recv_sem=recv.at[k],
            device_id=dev["c"], device_id_type=MESH,
        ).wait_recv()

    def sent(group, which=None):
        like = {"a": xg, "i": gi, "o": go, "w": go, "r": part, "s": nown}[group]
        total = sizes[group, None] + (sizes[group, which] if which is not None else 0)
        count, rest = divmod(total, math.prod(like.shape[1:]))
        assert rest == 0 and count <= like.shape[0]
        ref = like.at[pl.ds(0, count)]
        pltpu.make_async_remote_copy(
            src_ref=ref, dst_ref=ref, send_sem=send.at[groups.index(group)], recv_sem=recv.at[0],
            device_id=dev["c"], device_id_type=MESH,
        ).wait_send()

    table = {
        (other, dz, partner): rep_of(
            1 - yl if other else yl, lax.rem(z + dz + NZ, NZ), 1 - c if partner else c
        )
        for other in (0, 1) for dz in range(-4, 5) for partner in (0, 1)
    }

    def piece(other, dz, partner=0):
        return table[int(other), dz, partner]

    me_r, me_t = piece(0, 0), tp
    own_x, own_w, own_o = xg.at[me_t], gi.at[me_r], go.at[me_r]
    fetch = [pltpu.make_async_copy(x_ref, own_x, local.at[0])]
    for h in range(3):
        fetch.append(pltpu.make_async_copy(w_ref.at[h], own_w.at[:, pl.ds(h * 384, 384)], local.at[1 + h]))
    fetch.append(pltpu.make_async_copy(wo_ref, own_o, local.at[4]))
    for copy in fetch:
        copy.start()

    barrier = pltpu.get_barrier_semaphore()
    for d in dev.values():
        pl.semaphore_signal(barrier, inc=1, device_id=d, device_id_type=MESH)
    pl.semaphore_wait(barrier, len(dev))

    fetch[0].wait()
    push("ah", own_x, own_x, "h")
    push("ax+own", own_x, own_x, "x+")
    push("ax-own", own_x, own_x, "x-")
    for copy in fetch[1:4]:
        copy.wait()
    rows96 = (pl.ds(0, 96), pl.ds(96, 96))
    for n in (0, 1):
        for sign, m in (("+", n), ("-", 1 - n)):
            ref = gi.at[me_r, rows96[m]]
            push("iz" + sign + "1own" + str(m), ref, ref, "z" + sign)
    push("icown", own_w, own_w, "c")
    fetch[4].wait()

    def rows_of(ref, n):
        rows = ref.shape[0] // 2
        return ref.at[pl.ds(n * rows, rows)]

    def opp(sign):
        return 1 if sign == "+" else -1

    def lead(sign):
        return 0 if sign == "+" else 1

    def take_z(kind, buf, col, sign, d, n):
        ref = rows_of(buf.at[piece(col == "oth", -opp(sign) * d)], n)
        take(kind + "z" + sign + str(d) + col + str(n), ref)

    def push_z(kind, buf, col, sign, d, n):
        ref = rows_of(buf.at[piece(col == "oth", -opp(sign) * (d - 1))], n)
        push(kind + "z" + sign + str(d) + col + str(n), ref, ref, "z" + sign)

    def swap(col, dz):
        ref = gi.at[piece(col == "oth", dz)]
        push("ic" + (col if abs(dz) < 3 or col == "own" else str(abs(dz))), ref, ref, "c")

    def swap_o(wave, col, dz):
        ref = go.at[piece(col == "oth", dz)]
        push("oc" + str(wave), ref, ref, "c", " ow"[wave])

    def cross_o(wave, dz):
        ref = go.at[piece(0, dz)]
        push("oy" + str(wave), ref, ref, "y", " ow"[wave])

    def cross_half(buf, dz, n):
        ref = rows_of(buf.at[piece(0, dz)], n)
        push("iy" + str(dz) + "h" + str(n), ref, ref, "y")

    def take_cross_half(buf, dz, n):
        take("iy" + str(dz) + "h" + str(n), rows_of(buf.at[piece(1, dz)], n))

    def quarter(col, sign, over_y):
        rows = 96 * (1 - lead(sign)) + (0 if over_y else 48)
        return gi.at[piece(col == "oth", -opp(sign) * (2 if over_y else 1)), pl.ds(rows, 48)]

    tile = {
        "own+": xm * 2 + yh, "own-": xp * 2 + yh,
        "par+": xm * 2 + 1 - yh, "par-": xp * 2 + 1 - yh,
        "ownf": xf * 2 + yh, "parf": xf * 2 + 1 - yh,
    }

    def acts_step(who):
        for sign in "+-":
            ref = xg.at[tile[who + sign]]
            take("ax" + sign + who, ref)
            ref = rows_of(ref, lead(sign))
            push("ax" + sign + who + "f", ref, ref, "x" + sign)

    def acts_far(who):
        for sign in "+-":
            take("ax" + sign + who + "f", rows_of(xg.at[tile[who + "f"]], lead(sign)))

    def relay(kind, buf, col, d, which, onward=True):
        for sign in "+-":
            n = lead(sign) if which == "lead" else 1 - lead(sign)
            take_z(kind, buf, col, sign, d, n)
            if onward and (d < 3 or (d == 3 and which == "lead")):
                push_z(kind, buf, col, sign, d + 1, n)

    def swap_both(col, d):
        for sign in "+-":
            swap(col, -opp(sign) * d)

    def o_ref(col, sign, d, at):
        ref = go.at[piece(col == "oth", -opp(sign) * at)]
        return rows_of(ref, lead(sign)) if d == 4 else ref

    def push_o(col, d):
        for sign in "+-":
            ref = o_ref(col, sign, d, d - 1)
            push("oz" + sign + str(d) + col, ref, ref, "z" + sign)

    def take_o(col, d):
        for sign in "+-":
            take("oz" + sign + str(d) + col, o_ref(col, sign, d, d))

    def offsets(d):
        return (d,) if d in (0, 4) else (-d, d)

    def first_wave(d):
        def step():
            if d:
                take_o("own", d)
            if d < 4:
                push_o("own", d + 1)
            for dz in offsets(d):
                cross_o(1, dz)
                swap_o(1, "own", dz)

        on(d % 2, step)

    def first_wave_over():
        take("oy1", go.at[pl.ds(0, 4)])
        for which in (0, 1):
            def step(which=which):
                for d in range(which, 5, 2):
                    for dz in offsets(d):
                        swap_o(1, "oth", dz)

            on(which, step)

    def second_wave_cross():
        on(1, lambda: cross_o(2, 0))

    def push_two(col, d):
        for step in (2, 1):
            for sign in "+-":
                ref = o_ref(col, sign, d + step, d)
                push("oz" + sign + str(d + step) + col + "w", ref, ref, "z" + sign * step, "w")

    def take_two(col, d):
        for sign in "+-":
            take("oz" + sign + str(d) + col + "w", o_ref(col, sign, d, d))
        for dz in offsets(d):
            swap_o(2, col, dz)

    def second_wave_start():
        def step():
            push_two("own", 0)
            swap_o(2, "own", 0)
            take("oy2", go.at[piece(1, 0)])
            push_two("oth", 0)
            swap_o(2, "oth", 0)

        on(1, step)

    def second_wave_relay(col):
        def step():
            for sign in "+-":
                take("oz" + sign + "2" + col + "w", o_ref(col, sign, 2, 2))
            push_two(col, 2)
            for dz in offsets(2):
                swap_o(2, col, dz)

        on(1, step)

    def second_wave_leaf(first):
        def even():
            for col in ("own", "oth"):
                take_two(col, 1 if first else 3)

        def odd():
            for col in ("own", "oth"):
                take_two(col, 4)

        on(0, even)
        if not first:
            on(1, odd)

    def lane_tiles(t, rows):
        return [xg[t, rows, j * 128:(j + 1) * 128].astype(F32) for j in range(6)]

    def measure(t, first=False):
        def step(i, carry):
            for part_ in range(4):
                rows = pl.ds(pl.multiple_of(i * 128 + part_ * 32, 32), 32)
                tiles = lane_tiles(t, rows)
                total = tiles[0]
                for v in tiles[1:]:
                    total = total + v
                mean = jnp.sum(total, -1, keepdims=True) * (1.0 / 768)
                square = jnp.zeros((32, 128), F32)
                for v in tiles:
                    v = v - mean
                    square = square + v * v
                means[t, rows, :] = jnp.broadcast_to(mean, (32, 128))
                spread[rows, :] = square if first else spread[rows, :] + square
            return carry

        lax.fori_loop(0, 4, step, 0)

    def norm_rows(i, carry):
        for part_ in range(4):
            rows = pl.ds(pl.multiple_of(i * 128 + part_ * 32, 32), 32)
            mean = means[0, rows, :]
            for t in range(1, 8):
                mean = mean + means[t, rows, :]
            mean = mean * (1.0 / 8)
            apart = jnp.zeros((32, 128), F32)
            for t in range(8):
                v = means[t, rows, :] - mean
                apart = apart + v * v
            variance = (jnp.sum(spread[rows, :], -1, keepdims=True) + 768.0 * apart) * (1.0 / D)
            scale = lax.rsqrt(variance + EPS)
            for t in range(8):
                for j, v in enumerate(lane_tiles(t, rows)):
                    gain = gain_ref[pl.ds(t * 768 + j * 128, 128)].reshape(1, 128)
                    xg[t, rows, j * 128:(j + 1) * 128] = ((v - mean) * scale * gain).astype(BF16)
        return carry

    measure(me_t, True)
    relay("i", gi, "own", 1, "lead")
    relay("i", gi, "own", 1, "rest")
    for dz, n in ((1, 1), (-1, 0), (1, 0), (-1, 1)):
        cross_half(gi, dz, n)
    for dz in (1, -1):
        swap("own", dz)
    first_wave(0)
    relay("i", gi, "own", 2, "lead")
    par = xg.at[x * 2 + 1 - yh]
    take("ah", par)
    push("ax+par", par, par, "x+")
    push("ax-par", par, par, "x-")
    acts_step("own")
    relay("i", gi, "own", 2, "rest")
    for sign in "-+":
        ref = quarter("own", sign, True)
        push("iyq" + sign, ref, ref, "y")
    push("iy0", own_w, own_w, "y")
    second_wave_cross()
    swap_both("own", 2)
    measure(x * 2 + 1 - yh)
    for sign in "+-":
        measure(tile["own" + sign])
    relay("i", gi, "own", 3, "lead")
    first_wave(1)
    for dz, sign in ((1, "-"), (-1, "+")):
        take_cross_half(gi, dz, lead(sign))
        push_z("i", gi, "oth", sign, 2, lead(sign))
    relay("i", gi, "own", 3, "rest")
    swap_both("own", 3)
    for dz, sign in ((1, "-"), (-1, "+")):
        take_cross_half(gi, dz, 1 - lead(sign))
        ref = quarter("oth", sign, False)
        push("izq" + sign, ref, ref, "z" + sign)
        swap("oth", dz)
    relay("i", gi, "own", 4, "lead", False)
    swap("own", 4)
    acts_step("par")
    for sign in "+-":
        measure(tile["par" + sign])
    first_wave(2)
    relay("i", gi, "oth", 2, "lead")
    acts_far("own")
    measure(tile["ownf"])
    for sign in "+-":
        take("iyq" + sign, quarter("oth", sign, True))
        rows = 96 * (1 - lead(sign)) + 48
        take("izq" + sign, gi.at[piece(1, -2 * opp(sign)), pl.ds(rows, 48)])
        push_z("i", gi, "oth", sign, 3, 1 - lead(sign))
    swap_both("oth", 2)
    first_wave(3)
    acts_far("par")
    measure(tile["parf"])
    take("iy0", gi.at[piece(1, 0)])
    swap("oth", 0)
    sent("a")
    lax.fori_loop(0, 2, norm_rows, 0)
    relay("i", gi, "oth", 3, "lead")
    lax.fori_loop(2, 4, norm_rows, 0)
    take("icown", gi.at[pl.ds(0, 8)])

    def product(k):
        return jnp.dot(xg[k], gi[pl.ds(k * 4, 4)].reshape(768, 1152), preferred_element_type=F32)

    near_k, far_k = yl * 4, (1 - yl) * 4
    acc[...] = product(near_k) + product(near_k + 1)
    relay("i", gi, "oth", 3, "rest")
    swap_both("oth", 3)
    first_wave(4)
    second_wave_start()
    acc[...] += product(near_k + 2) + product(near_k + 3)
    take("icoth", gi.at[pl.ds(0, 5)])
    last = lax.div(lax.rem(z + 4, NZ), 2)
    odd = lax.rem(z, 2)

    def far_chunk(j):
        return product(far_k + lax.rem(last + (1 + odd, 2 + odd, 3 - 2 * odd, 4)[j], 4))

    acc[...] += far_chunk(0) + far_chunk(1)
    relay("i", gi, "oth", 4, "lead", False)
    swap("oth", 4)
    first_wave_over()
    take("ic3", gi.at[pl.ds(0, 2)])
    acc[...] += far_chunk(2)
    take("ic4", gi.at[piece(1, 4, 1)])
    second_wave_relay("own")
    acc[...] += far_chunk(3)

    def head_norm(v, gain):
        v = v - jnp.mean(v, -1, keepdims=True)
        var = jnp.mean(v * v, -1, keepdims=True)
        return (v * lax.rsqrt(var + EPS) * gain).astype(BF16)

    def attend(i, carry):
        rows = pl.ds(pl.multiple_of(i * PATCHES, PATCHES), PATCHES)
        for h in range(3):
            lo = h * 3 * HEAD_DIM
            q = head_norm(acc[rows, lo:lo + HEAD_DIM], qg_ref[...].reshape(1, HEAD_DIM))
            k = head_norm(acc[rows, lo + HEAD_DIM:lo + 2 * HEAD_DIM], kg_ref[...].reshape(1, HEAD_DIM))
            v = acc[rows, lo + 2 * HEAD_DIM:lo + 3 * HEAD_DIM].astype(BF16)
            s = dot_nt(q, k) / math.sqrt(HEAD_DIM)
            e = jnp.exp(s - jnp.max(s, -1, keepdims=True))
            p = (e / jnp.sum(e, -1, keepdims=True)).astype(BF16)
            o = jnp.dot(p, v, preferred_element_type=F32)
            mixed[rows, h * HEAD_DIM:(h + 1) * HEAD_DIM] = o.astype(BF16)
        return carry

    lax.fori_loop(0, 2, attend, 0)

    second_wave_relay("oth")
    take("oc1", go.at[pl.ds(0, 8)])

    def out_part(t, n):
        w = go[pl.ds(t * 4 + n * 2, 2)].reshape(384, 384)
        part[t, n] = dot_nt(mixed[...], w).astype(BF16)

    a_rows, b_rows = pl.ds(0, 256), pl.ds(256, 256)
    span = {"+": a_rows, "-": b_rows}
    other = {"+": b_rows, "-": a_rows}
    near_o = {"+": xp * 2 + yh, "-": xm * 2 + yh}
    near_p = {"+": xp * 2 + 1 - yh, "-": xm * 2 + 1 - yh}
    far_o, far_p = xf * 2 + yh, xf * 2 + 1 - yh
    mine, theirs = x * 2 + yh, x * 2 + 1 - yh
    signs = tuple(enumerate("+-"))

    def launch(n):
        for i, sign in signs:
            t = near_p[sign]
            out_part(t, n)
            push("n" + sign + "p" + str(n), part.at[t, n], r2.at[0, i, n], "x" + sign, "r")
        out_part(far_p, n)
        push("fh" + str(n), part.at[far_p, n], r4.at[n], "h", "r")

    def launch_rest(n):
        for i, sign in signs:
            t = near_o[sign]
            out_part(t, n)
            push("n" + sign + "d" + str(n), part.at[t, n, other[sign]], r2.at[1, i, n, other[sign]], "x" + sign, "r")
        out_part(far_o, n)
        out_part(theirs, n)
        out_part(mine, n)

    def plus(a, b):
        return (a.astype(F32) + b.astype(F32)).astype(BF16)

    def far(n):
        take("fh" + str(n), r4.at[n])
        for i, sign in signs:
            rows = span[sign]
            part[far_o, n, rows] = plus(part[far_o, n, rows], r4[n, rows])
            push("f" + sign + str(n), part.at[far_o, n, rows], r1.at[n, i], "x" + sign, "r")

    def near_add(n):
        for i, sign in signs:
            t, rows = near_o[sign], span[sign]
            take("f" + sign + str(n), r1.at[n, i])
            part[t, n, rows] = plus(part[t, n, rows], r1[n, i])

    def near_push(n):
        for i, sign in signs:
            t, rows = near_o[sign], span[sign]
            push("n" + sign + "s" + str(n), part.at[t, n, rows], r2.at[1, i, n, rows], "x" + sign, "r")

    def hand_over(n):
        for i, sign in signs:
            take("n" + sign + "p" + str(n), r2.at[0, i, n])
        total = part[theirs, n].astype(F32) + r2[0, 0, n].astype(F32) + r2[0, 1, n].astype(F32)
        tsum[n] = total.astype(BF16)
        push("t" + str(n), tsum.at[n], r3.at[n], "h", "r")

    done = []

    def finish(n):
        take("t" + str(n), r3.at[n])
        for i, sign in signs:
            take("n" + sign + "d" + str(n), r2.at[1, i, n, other[sign]])
        for i, sign in signs:
            take("n" + sign + "s" + str(n), r2.at[1, i, n, span[sign]])
            rows = span[sign]
            total = part[mine, n, rows].astype(F32) + r2[1, 0, n, rows].astype(F32)
            total = total + r2[1, 1, n, rows].astype(F32)
            stage[n, rows] = (total + r3[n, rows].astype(F32)).astype(BF16)
            copy = pltpu.make_async_copy(
                stage.at[n, rows], out_ref.at[rows, pl.ds(n * 384, 384)], local.at[2 * n + i]
            )
            copy.start()
            done.append(copy)

    def squares(ref, r, total):
        v = ref[r].astype(F32)
        v = v * v
        row = v[:, :128]
        for j in range(1, v.shape[1] // 128):
            row = row + v[:, j * 128:(j + 1) * 128]
        return total + jnp.sum(row.reshape(24, 8, 128), 0)

    zero = jnp.zeros((8, 128), F32)
    x1 = x + 1 - 2 * lax.rem(x, 2)
    dev["n0"] = dev["c"]
    dev["n1"] = (rep, x1 * 2 + yh)
    dev["n2"] = (rep, (NX - 1 - x) * 2 + yh)
    dev["n3"] = dev["h"]

    def norm_push(k):
        push("norm" + str(k), nown.at[k], nrecv.at[k], "n" + str(k), "s")

    def norm_take(k):
        take("norm" + str(k), nrecv.at[k])
        nown[k + 1] = nown[k] + nrecv[k]

    launch(0)
    second_wave_leaf(True)
    launch_rest(0)
    second_wave_leaf(False)
    hand_over(0)
    far(0)
    take("oc2", go.at[pl.ds(0, 8)])
    launch(1)
    launch_rest(1)
    nown[0, pl.ds(0, 8), :] = lax.fori_loop(0, 16, lambda r, t: squares(gi, 2 * r + c, t), zero)
    nown[0, pl.ds(8, 8), :] = lax.fori_loop(0, 16, lambda r, t: squares(go, 2 * r + c, t), zero)
    norm_push(0)
    near_add(0)
    norm_take(0)
    norm_push(1)
    hand_over(1)
    far(1)
    near_push(0)
    norm_take(1)
    norm_push(2)
    near_add(1)
    near_push(1)
    norm_take(2)
    norm_push(3)
    finish(0)
    norm_take(3)
    total_in = jnp.sum(nown[4, pl.ds(0, 8), :], keepdims=True)
    total_out = jnp.sum(nown[4, pl.ds(8, 8), :], keepdims=True)
    norm_ref[0] = (total_in / (3 * HEADS * HEAD_DIM))[0, 0]
    norm_ref[1] = (total_out / D)[0, 0]
    finish(1)
    for copy in done:
        copy.wait()
    for group in "irs":
        sent(group)
    for which in (0, 1):
        pl.when(lax.rem(z, 2) == which)(lambda which=which: (sent("o", which), sent("w", which))[0])
    assert len(ids) == NSEM, len(ids)


def shards(activations, norm_gain, query_gain, key_gain, project_in, project_out):
    rows, cols = activations.shape
    hbm = pl.BlockSpec(memory_space=pl.ANY)
    vmem = pl.BlockSpec(memory_space=pltpu.VMEM)
    out, norms = pl.pallas_call(
        kernel,
        name="block",
        out_shape=(jax.ShapeDtypeStruct((rows, cols), BF16), jax.ShapeDtypeStruct((2,), F32)),
        in_specs=[hbm, vmem, vmem, vmem, hbm, hbm],
        out_specs=(hbm, pl.BlockSpec(memory_space=pltpu.SMEM)),
        scratch_shapes=[
            pltpu.VMEM((32, 192, 1152), BF16),
            pltpu.VMEM((32, 192, 384), BF16),
            pltpu.VMEM((8, 512, 768), BF16),
            pltpu.VMEM((8, 512, 128), F32),
            pltpu.VMEM((512, 128), F32),
            pltpu.VMEM((2, 512, 384), BF16),
            pltpu.VMEM((512, 1152), F32),
            pltpu.VMEM((512, 384), BF16),
            pltpu.VMEM((8, 2, 512, 384), BF16),
            pltpu.VMEM((2, 2, 256, 384), BF16),
            pltpu.VMEM((2, 2, 2, 512, 384), BF16),
            pltpu.VMEM((2, 512, 384), BF16),
            pltpu.VMEM((2, 512, 384), BF16),
            pltpu.VMEM((2, 512, 384), BF16),
            pltpu.VMEM((5, 16, 128), F32),
            pltpu.VMEM((4, 16, 128), F32),
            pltpu.SemaphoreType.DMA((6,)),
            pltpu.SemaphoreType.DMA((NSEM,)),
            pltpu.SemaphoreType.DMA((5,)),
        ],
        compiler_params=pltpu.CompilerParams(
            collective_id=0, has_side_effects=True, vmem_limit_bytes=63 * 1024 * 1024
        ),
    )(
        activations,
        norm_gain,
        query_gain,
        key_gain,
        project_in.transpose(1, 0, 2),
        project_out,
    )
    return out, jnp.sqrt(norms)


def solution(mesh):
    return jax.shard_map(
        shards,
        mesh=mesh,
        in_specs=(P("rep", "tp"), P(), P(), P(), P("rep", "tp", None), P("rep", "tp")),
        out_specs=(P("rep", "tp"), P()),
        check_vma=False,
    )
```

```python
import math

import jax
import jax.numpy as jnp
from jax import lax
from jax.experimental import pallas as pl
from jax.experimental.pallas import tpu as pltpu
from jax.sharding import PartitionSpec as P

D = 6144
HEADS = 24
HEAD_DIM = 128
PATCHES = 256
NX, NZ = 4, 8
MESH = pl.DeviceIdType.MESH
F32, BF16 = jnp.float32, jnp.bfloat16
EPS = 1e-06
NSEM = 115


def dot_nt(a, b):
    return lax.dot_general(a, b, (((1,), (1,)), ((), ())), preferred_element_type=F32)


def kernel(
    x_ref, gain_ref, qg_ref, kg_ref, w_ref, wo_ref, out_ref, norm_ref,
    gi, go, xg, means, spread, stage, acc, mixed, part, r1, r2, r3, r4, tsum, nown, nrecv,
    send, recv, local,
):
    rep, tp = lax.axis_index("rep"), lax.axis_index("tp")
    c = lax.rem(rep, 2)
    z = lax.rem(lax.div(rep, 2), NZ)
    yl = lax.div(rep, 2 * NZ)
    x, yh = lax.div(tp, 2), lax.rem(tp, 2)

    def rep_of(yl_, z_, c_):
        return (yl_ * NZ + z_) * 2 + c_

    zp, zm = lax.rem(z + 1, NZ), lax.rem(z + NZ - 1, NZ)
    xp, xm = lax.rem(x + 1, NX), lax.rem(x + NX - 1, NX)
    xf = lax.rem(x + 2, NX)
    dev = {
        "z+": (rep_of(yl, zp, c), tp),
        "z-": (rep_of(yl, zm, c), tp),
        "z++": (rep_of(yl, lax.rem(z + 2, NZ), c), tp),
        "z--": (rep_of(yl, lax.rem(z + NZ - 2, NZ), c), tp),
        "c": (rep_of(yl, z, 1 - c), tp),
        "y": (rep_of(1 - yl, z, c), tp),
        "x+": (rep, xp * 2 + yh),
        "x-": (rep, xm * 2 + yh),
        "h": (rep, x * 2 + 1 - yh),
    }

    ids, parity = {}, [None]
    groups = "abiorsw"
    sizes = {(g, which): 0 for g in groups for which in (None, 0, 1)}

    def on(which, action):
        @pl.when(lax.rem(z, 2) == which)
        def _():
            parity[0] = which
            action()
            parity[0] = None

    def ident(name):
        return ids.setdefault(name, len(ids))

    def push(name, src, dst, to, group=None):
        k = ident(name)
        group = group or name[0]
        pltpu.make_async_remote_copy(
            src_ref=src, dst_ref=dst, send_sem=send.at[groups.index(group)], recv_sem=recv.at[k],
            device_id=dev[to], device_id_type=MESH,
        ).start()
        sizes[group, parity[0]] += math.prod(src.shape)

    def take(name, dst):
        k = ident(name)
        pltpu.make_async_remote_copy(
            src_ref=dst, dst_ref=dst, send_sem=send.at[0], recv_sem=recv.at[k],
            device_id=dev["c"], device_id_type=MESH,
        ).wait_recv()

    def sent(group, which=None):
        if group in "ab":
            assert sizes[group, None] == 7 * 256 * 768
            ref = xg.at[pl.ds(0, 7), pl.ds(0, 256)]
            pltpu.make_async_remote_copy(
                src_ref=ref, dst_ref=ref, send_sem=send.at[groups.index(group)], recv_sem=recv.at[0],
                device_id=dev["c"], device_id_type=MESH,
            ).wait_send()
            return
        like = {"i": gi, "o": go, "w": go, "r": part, "s": nown}[group]
        total = sizes[group, None] + (sizes[group, which] if which is not None else 0)
        count, rest = divmod(total, math.prod(like.shape[1:]))
        assert rest == 0 and count <= like.shape[0]
        ref = like.at[pl.ds(0, count)]
        pltpu.make_async_remote_copy(
            src_ref=ref, dst_ref=ref, send_sem=send.at[groups.index(group)], recv_sem=recv.at[0],
            device_id=dev["c"], device_id_type=MESH,
        ).wait_send()

    table = {
        (other, dz, partner): rep_of(
            1 - yl if other else yl, lax.rem(z + dz + NZ, NZ), 1 - c if partner else c
        )
        for other in (0, 1) for dz in range(-4, 5) for partner in (0, 1)
    }

    def piece(other, dz, partner=0):
        return table[int(other), dz, partner]

    me_r, me_t = piece(0, 0), tp
    own_x, own_w, own_o = xg.at[me_t], gi.at[me_r], go.at[me_r]
    fetch = [pltpu.make_async_copy(x_ref, own_x, local.at[0])]
    for h in range(3):
        fetch.append(pltpu.make_async_copy(w_ref.at[h], own_w.at[:, pl.ds(h * 384, 384)], local.at[1 + h]))
    fetch.append(pltpu.make_async_copy(wo_ref, own_o, local.at[4]))
    for copy in fetch:
        copy.start()

    barrier = pltpu.get_barrier_semaphore()
    for d in dev.values():
        pl.semaphore_signal(barrier, inc=1, device_id=d, device_id_type=MESH)
    pl.semaphore_wait(barrier, len(dev))

    fetch[0].wait()
    def image(ref, i):
        return ref.at[pl.ds(i * PATCHES, PATCHES)]

    for i in (0, 1):
        ref = image(own_x, i)
        push("ah" + str(i), ref, ref, "h", "ab"[i])
        for sign in "+-":
            push("ax" + sign + "own" + str(i), ref, ref, "x" + sign, "ab"[i])
    for copy in fetch[1:4]:
        copy.wait()
    rows96 = (pl.ds(0, 96), pl.ds(96, 96))
    for n in (0, 1):
        for sign, m in (("+", n), ("-", 1 - n)):
            ref = gi.at[me_r, rows96[m]]
            push("iz" + sign + "1own" + str(m), ref, ref, "z" + sign)
    push("icown", own_w, own_w, "c")
    fetch[4].wait()

    def rows_of(ref, n):
        rows = ref.shape[0] // 2
        return ref.at[pl.ds(n * rows, rows)]

    def opp(sign):
        return 1 if sign == "+" else -1

    def lead(sign):
        return 0 if sign == "+" else 1

    def take_z(kind, buf, col, sign, d, n):
        ref = rows_of(buf.at[piece(col == "oth", -opp(sign) * d)], n)
        take(kind + "z" + sign + str(d) + col + str(n), ref)

    def push_z(kind, buf, col, sign, d, n):
        ref = rows_of(buf.at[piece(col == "oth", -opp(sign) * (d - 1))], n)
        push(kind + "z" + sign + str(d) + col + str(n), ref, ref, "z" + sign)

    def swap(col, dz):
        ref = gi.at[piece(col == "oth", dz)]
        push("ic" + (col if abs(dz) < 3 or col == "own" else str(abs(dz))), ref, ref, "c")

    def swap_o(wave, col, dz):
        ref = go.at[piece(col == "oth", dz)]
        push("oc" + str(wave), ref, ref, "c", " ow"[wave])

    def cross_o(wave, dz):
        ref = go.at[piece(0, dz)]
        push("oy" + str(wave), ref, ref, "y", " ow"[wave])

    def cross_half(buf, dz, n):
        ref = rows_of(buf.at[piece(0, dz)], n)
        push("iy" + str(dz) + "h" + str(n), ref, ref, "y")

    def take_cross_half(buf, dz, n):
        take("iy" + str(dz) + "h" + str(n), rows_of(buf.at[piece(1, dz)], n))

    def quarter(col, sign, over_y):
        rows = 96 * (1 - lead(sign)) + (0 if over_y else 48)
        return gi.at[piece(col == "oth", -opp(sign) * (2 if over_y else 1)), pl.ds(rows, 48)]

    tile = {
        "own+": xm * 2 + yh, "own-": xp * 2 + yh,
        "par+": xm * 2 + 1 - yh, "par-": xp * 2 + 1 - yh,
        "ownf": xf * 2 + yh, "parf": xf * 2 + 1 - yh,
    }

    def acts_half(t, i, sign):
        return xg.at[t, pl.ds(i * PATCHES + lead(sign) * 128, 128)]

    def acts_par(i):
        ref = image(xg.at[x * 2 + 1 - yh], i)
        take("ah" + str(i), ref)
        for sign in "+-":
            push("ax" + sign + "par" + str(i), ref, ref, "x" + sign, "ab"[i])

    def acts_step(who, i):
        for sign in "+-":
            t = tile[who + sign]
            take("ax" + sign + who + str(i), image(xg.at[t], i))
            ref = acts_half(t, i, sign)
            push("ax" + sign + who + "f" + str(i), ref, ref, "x" + sign, "ab"[i])

    def acts_far(who, i):
        for sign in "+-":
            take("ax" + sign + who + "f" + str(i), acts_half(tile[who + "f"], i, sign))

    def relay(kind, buf, col, d, which, onward=True):
        for sign in "+-":
            n = lead(sign) if which == "lead" else 1 - lead(sign)
            take_z(kind, buf, col, sign, d, n)
            if onward and (d < 3 or (d == 3 and which == "lead")):
                push_z(kind, buf, col, sign, d + 1, n)

    def swap_both(col, d):
        for sign in "+-":
            swap(col, -opp(sign) * d)

    def o_ref(col, sign, d, at):
        ref = go.at[piece(col == "oth", -opp(sign) * at)]
        return rows_of(ref, lead(sign)) if d == 4 else ref

    def push_o(col, d):
        for sign in "+-":
            ref = o_ref(col, sign, d, d - 1)
            push("oz" + sign + str(d) + col, ref, ref, "z" + sign)

    def take_o(col, d):
        for sign in "+-":
            take("oz" + sign + str(d) + col, o_ref(col, sign, d, d))

    def offsets(d):
        return (d,) if d in (0, 4) else (-d, d)

    def first_wave(d):
        def step():
            if d:
                take_o("own", d)
            if d < 4:
                push_o("own", d + 1)
            for dz in offsets(d):
                cross_o(1, dz)
                swap_o(1, "own", dz)

        on(d % 2, step)

    def first_wave_over():
        take("oy1", go.at[pl.ds(0, 4)])
        for which in (0, 1):
            def step(which=which):
                for d in range(which, 5, 2):
                    for dz in offsets(d):
                        swap_o(1, "oth", dz)

            on(which, step)

    def second_wave_cross():
        on(1, lambda: cross_o(2, 0))

    def push_two(col, d):
        for step in (2, 1):
            for sign in "+-":
                ref = o_ref(col, sign, d + step, d)
                push("oz" + sign + str(d + step) + col + "w", ref, ref, "z" + sign * step, "w")

    def take_two(col, d):
        for sign in "+-":
            take("oz" + sign + str(d) + col + "w", o_ref(col, sign, d, d))
        for dz in offsets(d):
            swap_o(2, col, dz)

    def second_wave_start():
        def step():
            push_two("own", 0)
            swap_o(2, "own", 0)
            take("oy2", go.at[piece(1, 0)])
            push_two("oth", 0)
            swap_o(2, "oth", 0)

        on(1, step)

    def second_wave_relay(col):
        def step():
            for sign in "+-":
                take("oz" + sign + "2" + col + "w", o_ref(col, sign, 2, 2))
            push_two(col, 2)
            for dz in offsets(2):
                swap_o(2, col, dz)

        on(1, step)

    def second_wave_leaf():
        def even():
            for d in (1, 3):
                for col in ("own", "oth"):
                    take_two(col, d)

        def odd():
            for col in ("own", "oth"):
                take_two(col, 4)

        on(0, even)
        on(1, odd)

    def lane_tiles(t, rows):
        return [xg[t, rows, j * 128:(j + 1) * 128].astype(F32) for j in range(6)]

    def measure(t, image_, first=False):
        def step(i, carry):
            for part_ in range(4):
                rows = pl.ds(pl.multiple_of(i * 128 + part_ * 32, 32), 32)
                tiles = lane_tiles(t, rows)
                total = tiles[0]
                for v in tiles[1:]:
                    total = total + v
                mean = jnp.sum(total, -1, keepdims=True) * (1.0 / 768)
                square = jnp.zeros((32, 128), F32)
                for v in tiles:
                    v = v - mean
                    square = square + v * v
                means[t, rows, :] = jnp.broadcast_to(mean, (32, 128))
                spread[rows, :] = square if first else spread[rows, :] + square
            return carry

        lax.fori_loop(2 * image_, 2 * image_ + 2, step, 0)

    def norm_rows(i, carry):
        for part_ in range(4):
            rows = pl.ds(pl.multiple_of(i * 128 + part_ * 32, 32), 32)
            mean = means[0, rows, :]
            for t in range(1, 8):
                mean = mean + means[t, rows, :]
            mean = mean * (1.0 / 8)
            apart = jnp.zeros((32, 128), F32)
            for t in range(8):
                v = means[t, rows, :] - mean
                apart = apart + v * v
            variance = (jnp.sum(spread[rows, :], -1, keepdims=True) + 768.0 * apart) * (1.0 / D)
            scale = lax.rsqrt(variance + EPS)
            for t in range(8):
                for j, v in enumerate(lane_tiles(t, rows)):
                    gain = gain_ref[pl.ds(t * 768 + j * 128, 128)].reshape(1, 128)
                    xg[t, rows, j * 128:(j + 1) * 128] = ((v - mean) * scale * gain).astype(BF16)
        return carry

    near_k, far_k = yl * 4, (1 - yl) * 4
    last = lax.div(lax.rem(z + 4, NZ), 2)
    odd = lax.rem(z, 2)

    def near_chunks(i, j):
        rows = pl.ds(i * PATCHES, PATCHES)
        total = None
        for k in (near_k + j, near_k + j + 1):
            w = gi[pl.ds(k * 4, 4)].reshape(768, 1152)
            value = jnp.dot(xg[k, rows], w, preferred_element_type=F32)
            total = value if total is None else total + value
        acc[rows] = total if j == 0 else acc[rows] + total

    def far_chunk(j, rows=slice(None)):
        k = far_k + lax.rem(last + (1 + odd, 2 + odd, 3 - 2 * odd, 4)[j], 4)
        return jnp.dot(xg[k, rows], gi[pl.ds(k * 4, 4)].reshape(768, 1152), preferred_element_type=F32)

    for i in (0, 1):
        measure(me_t, i, True)
    relay("i", gi, "own", 1, "lead")
    relay("i", gi, "own", 1, "rest")
    for dz, n in ((1, 1), (-1, 0), (1, 0), (-1, 1)):
        cross_half(gi, dz, n)
    for dz in (1, -1):
        swap("own", dz)
    first_wave(0)
    acts_par(0)
    acts_step("own", 0)
    relay("i", gi, "own", 2, "lead")
    relay("i", gi, "own", 2, "rest")
    for sign in "-+":
        ref = quarter("own", sign, True)
        push("iyq" + sign, ref, ref, "y")
    push("iy0", own_w, own_w, "y")
    second_wave_cross()
    swap_both("own", 2)
    measure(x * 2 + 1 - yh, 0)
    for sign in "+-":
        measure(tile["own" + sign], 0)
    relay("i", gi, "own", 3, "lead")
    first_wave(1)
    acts_step("par", 0)
    acts_par(1)
    acts_step("own", 1)
    for dz, sign in ((1, "-"), (-1, "+")):
        take_cross_half(gi, dz, lead(sign))
        push_z("i", gi, "oth", sign, 2, lead(sign))
    for sign in "+-":
        measure(tile["par" + sign], 0)
    relay("i", gi, "own", 3, "rest")
    swap_both("own", 3)
    acts_far("own", 0)
    measure(tile["ownf"], 0)
    acts_far("par", 0)
    measure(tile["parf"], 0)
    for dz, sign in ((1, "-"), (-1, "+")):
        take_cross_half(gi, dz, 1 - lead(sign))
        ref = quarter("oth", sign, False)
        push("izq" + sign, ref, ref, "z" + sign)
        swap("oth", dz)
    relay("i", gi, "own", 4, "lead", False)
    swap("own", 4)
    sent("a")
    lax.fori_loop(0, 2, norm_rows, 0)
    first_wave(2)
    take("icown", gi.at[pl.ds(0, 8)])
    near_chunks(0, 0)
    relay("i", gi, "oth", 2, "lead")
    acts_step("par", 1)
    near_chunks(0, 2)
    for sign in "+-":
        take("iyq" + sign, quarter("oth", sign, True))
        rows = 96 * (1 - lead(sign)) + 48
        take("izq" + sign, gi.at[piece(1, -2 * opp(sign)), pl.ds(rows, 48)])
        push_z("i", gi, "oth", sign, 3, 1 - lead(sign))
    swap_both("oth", 2)
    measure(x * 2 + 1 - yh, 1)
    for who in ("own", "par"):
        for sign in "+-":
            measure(tile[who + sign], 1)
    acts_far("own", 1)
    measure(tile["ownf"], 1)
    first_wave(3)
    acts_far("par", 1)
    measure(tile["parf"], 1)
    take("iy0", gi.at[piece(1, 0)])
    swap("oth", 0)
    sent("b")
    lax.fori_loop(2, 3, norm_rows, 0)
    relay("i", gi, "oth", 3, "lead")
    lax.fori_loop(3, 4, norm_rows, 0)
    near_chunks(1, 0)
    relay("i", gi, "oth", 3, "rest")
    swap_both("oth", 3)
    first_wave(4)
    near_chunks(1, 2)
    second_wave_start()
    take("icoth", gi.at[pl.ds(0, 5)])
    acc[...] += far_chunk(0) + far_chunk(1)
    take("ic3", gi.at[pl.ds(0, 2)])
    relay("i", gi, "oth", 4, "lead", False)
    swap("oth", 4)
    acc[...] += far_chunk(2)
    first_wave_over()
    second_wave_relay("own")
    take("ic4", gi.at[piece(1, 4, 1)])

    def head_norm(v, gain):
        v = v - jnp.mean(v, -1, keepdims=True)
        var = jnp.mean(v * v, -1, keepdims=True)
        return (v * lax.rsqrt(var + EPS) * gain).astype(BF16)

    def attend(i):
        rows = pl.ds(i * PATCHES, PATCHES)
        acc[rows] += far_chunk(3, rows)
        for h in range(3):
            lo = h * 3 * HEAD_DIM
            q = head_norm(acc[rows, lo:lo + HEAD_DIM], qg_ref[...].reshape(1, HEAD_DIM))
            k = head_norm(acc[rows, lo + HEAD_DIM:lo + 2 * HEAD_DIM], kg_ref[...].reshape(1, HEAD_DIM))
            v = acc[rows, lo + 2 * HEAD_DIM:lo + 3 * HEAD_DIM].astype(BF16)
            s = dot_nt(q, k) / math.sqrt(HEAD_DIM)
            e = jnp.exp(s - jnp.max(s, -1, keepdims=True))
            p = (e / jnp.sum(e, -1, keepdims=True)).astype(BF16)
            o = jnp.dot(p, v, preferred_element_type=F32)
            mixed[rows, h * HEAD_DIM:(h + 1) * HEAD_DIM] = o.astype(BF16)


    def out_part(t, n):
        w = go[pl.ds(t * 4 + n * 2, 2)].reshape(384, 384)
        part[t, n] = dot_nt(mixed[...], w).astype(BF16)

    a_rows, b_rows = pl.ds(0, 256), pl.ds(256, 256)
    span = {"+": a_rows, "-": b_rows}
    other = {"+": b_rows, "-": a_rows}
    near_o = {"+": xp * 2 + yh, "-": xm * 2 + yh}
    near_p = {"+": xp * 2 + 1 - yh, "-": xm * 2 + 1 - yh}
    far_o, far_p = xf * 2 + yh, xf * 2 + 1 - yh
    mine, theirs = x * 2 + yh, x * 2 + 1 - yh
    signs = tuple(enumerate("+-"))

    def launch_near(n, i):
        rows = pl.ds(i * PATCHES, PATCHES)
        w_of = lambda t: go[pl.ds(t * 4 + n * 2, 2)].reshape(384, 384)
        for k, sign in signs:
            t = near_p[sign]
            part[t, n, rows] = dot_nt(mixed[rows], w_of(t)).astype(BF16)
            ref = part.at[t, n, rows]
            push("n" + sign + "p" + str(n) + str(i), ref, r2.at[0, k, n, rows], "x" + sign, "r")

    def launch_far(n, i):
        rows = pl.ds(i * PATCHES, PATCHES)
        w = go[pl.ds(far_p * 4 + n * 2, 2)].reshape(384, 384)
        part[far_p, n, rows] = dot_nt(mixed[rows], w).astype(BF16)
        push("fh" + str(n) + str(i), part.at[far_p, n, rows], r4.at[n, rows], "h", "r")

    def direct(n, j):
        for i, sign in signs:
            rows = pl.ds((256 if sign == "+" else 0) + 128 * j, 128)
            ref = part.at[near_o[sign], n, rows]
            push("n" + sign + "d" + str(n) + str(j), ref, r2.at[1, i, n, rows], "x" + sign, "r")

    def launch_rest(n):
        for i, sign in signs:
            out_part(near_o[sign], n)
        direct(n, 0)
        out_part(far_o, n)
        out_part(theirs, n)
        out_part(mine, n)

    def plus(a, b):
        return (a.astype(F32) + b.astype(F32)).astype(BF16)

    def far(n):
        for i, sign in signs:
            rows = span[sign]
            take("fh" + str(n) + str(i), r4.at[n, rows])
            part[far_o, n, rows] = plus(part[far_o, n, rows], r4[n, rows])
            push("f" + sign + str(n), part.at[far_o, n, rows], r1.at[n, i], "x" + sign, "r")

    def near_add(n):
        for i, sign in signs:
            t, rows = near_o[sign], span[sign]
            take("f" + sign + str(n), r1.at[n, i])
            part[t, n, rows] = plus(part[t, n, rows], r1[n, i])

    def near_push(n):
        for i, sign in signs:
            t, rows = near_o[sign], span[sign]
            push("n" + sign + "s" + str(n), part.at[t, n, rows], r2.at[1, i, n, rows], "x" + sign, "r")

    def hand_over(n):
        for j in (0, 1):
            for i, sign in signs:
                take("n" + sign + "p" + str(n) + str(j), r2.at[0, i, n, pl.ds(j * PATCHES, PATCHES)])
        total = part[theirs, n].astype(F32) + r2[0, 0, n].astype(F32) + r2[0, 1, n].astype(F32)
        tsum[n] = total.astype(BF16)
        push("t" + str(n), tsum.at[n], r3.at[n], "h", "r")

    done = []

    def finish(n):
        take("t" + str(n), r3.at[n])
        for i, sign in signs:
            for j in (0, 1):
                rows = pl.ds((256 if sign == "+" else 0) + 128 * j, 128)
                take("n" + sign + "d" + str(n) + str(j), r2.at[1, i, n, rows])
        for i, sign in signs:
            take("n" + sign + "s" + str(n), r2.at[1, i, n, span[sign]])
            rows = span[sign]
            total = part[mine, n, rows].astype(F32) + r2[1, 0, n, rows].astype(F32)
            total = total + r2[1, 1, n, rows].astype(F32)
            stage[n, rows] = (total + r3[n, rows].astype(F32)).astype(BF16)
            copy = pltpu.make_async_copy(
                stage.at[n, rows], out_ref.at[rows, pl.ds(n * 384, 384)], local.at[2 * n + i]
            )
            copy.start()
            done.append(copy)

    def squares(ref, r, total):
        v = ref[r].astype(F32)
        v = v * v
        row = v[:, :128]
        for j in range(1, v.shape[1] // 128):
            row = row + v[:, j * 128:(j + 1) * 128]
        return total + jnp.sum(row.reshape(24, 8, 128), 0)

    zero = jnp.zeros((8, 128), F32)
    x1 = x + 1 - 2 * lax.rem(x, 2)
    dev["n0"] = dev["c"]
    dev["n1"] = (rep, x1 * 2 + yh)
    dev["n2"] = (rep, (NX - 1 - x) * 2 + yh)
    dev["n3"] = dev["h"]

    def norm_push(k):
        push("norm" + str(k), nown.at[k], nrecv.at[k], "n" + str(k), "s")

    def norm_take(k):
        take("norm" + str(k), nrecv.at[k])
        nown[k + 1] = nown[k] + nrecv[k]

    attend(0)
    take("oc1", go.at[pl.ds(0, 8)])
    launch_near(0, 0)
    launch_far(0, 0)
    attend(1)
    launch_near(0, 1)
    launch_far(0, 1)
    second_wave_relay("oth")
    launch_rest(0)
    nown[0, pl.ds(0, 8), :] = lax.fori_loop(0, 16, lambda r, t: squares(gi, 2 * r + c, t), zero)
    hand_over(0)
    far(0)
    direct(0, 1)
    second_wave_leaf()
    near_add(0)
    near_push(0)
    take("oc2", go.at[pl.ds(0, 8)])
    for i in (0, 1):
        launch_near(1, i)
        launch_far(1, i)
    launch_rest(1)
    nown[0, pl.ds(8, 8), :] = lax.fori_loop(0, 16, lambda r, t: squares(go, 2 * r + c, t), zero)
    norm_push(0)
    norm_take(0)
    norm_push(1)
    hand_over(1)
    far(1)
    direct(1, 1)
    norm_take(1)
    norm_push(2)
    near_add(1)
    near_push(1)
    norm_take(2)
    norm_push(3)
    finish(0)
    norm_take(3)
    total_in = jnp.sum(nown[4, pl.ds(0, 8), :], keepdims=True)
    total_out = jnp.sum(nown[4, pl.ds(8, 8), :], keepdims=True)
    norm_ref[0] = (total_in / (3 * HEADS * HEAD_DIM))[0, 0]
    norm_ref[1] = (total_out / D)[0, 0]
    finish(1)
    for copy in done:
        copy.wait()
    for group in "irs":
        sent(group)
    for which in (0, 1):
        pl.when(lax.rem(z, 2) == which)(lambda which=which: (sent("o", which), sent("w", which))[0])
    assert len(ids) == NSEM, len(ids)


def shards(activations, norm_gain, query_gain, key_gain, project_in, project_out):
    rows, cols = activations.shape
    hbm = pl.BlockSpec(memory_space=pl.ANY)
    vmem = pl.BlockSpec(memory_space=pltpu.VMEM)
    out, norms = pl.pallas_call(
        kernel,
        name="block",
        out_shape=(jax.ShapeDtypeStruct((rows, cols), BF16), jax.ShapeDtypeStruct((2,), F32)),
        in_specs=[hbm, vmem, vmem, vmem, hbm, hbm],
        out_specs=(hbm, pl.BlockSpec(memory_space=pltpu.SMEM)),
        scratch_shapes=[
            pltpu.VMEM((32, 192, 1152), BF16),
            pltpu.VMEM((32, 192, 384), BF16),
            pltpu.VMEM((8, 512, 768), BF16),
            pltpu.VMEM((8, 512, 128), F32),
            pltpu.VMEM((512, 128), F32),
            pltpu.VMEM((2, 512, 384), BF16),
            pltpu.VMEM((512, 1152), F32),
            pltpu.VMEM((512, 384), BF16),
            pltpu.VMEM((8, 2, 512, 384), BF16),
            pltpu.VMEM((2, 2, 256, 384), BF16),
            pltpu.VMEM((2, 2, 2, 512, 384), BF16),
            pltpu.VMEM((2, 512, 384), BF16),
            pltpu.VMEM((2, 512, 384), BF16),
            pltpu.VMEM((2, 512, 384), BF16),
            pltpu.VMEM((5, 16, 128), F32),
            pltpu.VMEM((4, 16, 128), F32),
            pltpu.SemaphoreType.DMA((7,)),
            pltpu.SemaphoreType.DMA((NSEM,)),
            pltpu.SemaphoreType.DMA((5,)),
        ],
        compiler_params=pltpu.CompilerParams(
            collective_id=0, has_side_effects=True, vmem_limit_bytes=63 * 1024 * 1024
        ),
    )(
        activations,
        norm_gain,
        query_gain,
        key_gain,
        project_in.transpose(1, 0, 2),
        project_out,
    )
    return out, jnp.sqrt(norms)


def solution(mesh):
    return jax.shard_map(
        shards,
        mesh=mesh,
        in_specs=(P("rep", "tp"), P(), P(), P(), P("rep", "tp", None), P("rep", "tp")),
        out_specs=(P("rep", "tp"), P()),
        check_vma=False,
    )
```

```python
import math

import jax
import jax.numpy as jnp
from jax import lax
from jax.experimental import pallas as pl
from jax.experimental.pallas import tpu as pltpu
from jax.sharding import PartitionSpec as P

D = 6144
HEADS = 24
HEAD_DIM = 128
PATCHES = 256
NX, NZ = 4, 8
MESH = pl.DeviceIdType.MESH
F32, BF16 = jnp.float32, jnp.bfloat16
EPS = 1e-06
NSEM = 115


def dot_nt(a, b):
    return lax.dot_general(a, b, (((1,), (1,)), ((), ())), preferred_element_type=F32)


def kernel(
    x_ref, gain_ref, qg_ref, kg_ref, w_ref, wo_ref, out_ref, norm_ref,
    gi, go, xg, means, spread, stage, acc, mixed, part, r1, r2, r3, r4, tsum, nown, nrecv,
    send, recv, local,
):
    rep, tp = lax.axis_index("rep"), lax.axis_index("tp")
    c = lax.rem(rep, 2)
    z = lax.rem(lax.div(rep, 2), NZ)
    yl = lax.div(rep, 2 * NZ)
    x, yh = lax.div(tp, 2), lax.rem(tp, 2)

    def rep_of(yl_, z_, c_):
        return (yl_ * NZ + z_) * 2 + c_

    zp, zm = lax.rem(z + 1, NZ), lax.rem(z + NZ - 1, NZ)
    xp, xm = lax.rem(x + 1, NX), lax.rem(x + NX - 1, NX)
    xf = lax.rem(x + 2, NX)
    dev = {
        "z+": (rep_of(yl, zp, c), tp),
        "z-": (rep_of(yl, zm, c), tp),
        "z++": (rep_of(yl, lax.rem(z + 2, NZ), c), tp),
        "z--": (rep_of(yl, lax.rem(z + NZ - 2, NZ), c), tp),
        "c": (rep_of(yl, z, 1 - c), tp),
        "y": (rep_of(1 - yl, z, c), tp),
        "x+": (rep, xp * 2 + yh),
        "x-": (rep, xm * 2 + yh),
        "h": (rep, x * 2 + 1 - yh),
    }

    ids, parity = {}, [None]
    groups = "abiorsw"
    sizes = {(g, which): 0 for g in groups for which in (None, 0, 1)}

    def on(which, action):
        @pl.when(lax.rem(z, 2) == which)
        def _():
            parity[0] = which
            action()
            parity[0] = None

    def ident(name):
        return ids.setdefault(name, len(ids))

    def push(name, src, dst, to, group=None):
        k = ident(name)
        group = group or name[0]
        pltpu.make_async_remote_copy(
            src_ref=src, dst_ref=dst, send_sem=send.at[groups.index(group)], recv_sem=recv.at[k],
            device_id=dev[to], device_id_type=MESH,
        ).start()
        sizes[group, parity[0]] += math.prod(src.shape)

    def take(name, dst):
        k = ident(name)
        pltpu.make_async_remote_copy(
            src_ref=dst, dst_ref=dst, send_sem=send.at[0], recv_sem=recv.at[k],
            device_id=dev["c"], device_id_type=MESH,
        ).wait_recv()

    def sent(group, which=None):
        if group in "ab":
            assert sizes[group, None] == 7 * 256 * 768
            ref = xg.at[pl.ds(0, 7), pl.ds(0, 256)]
            pltpu.make_async_remote_copy(
                src_ref=ref, dst_ref=ref, send_sem=send.at[groups.index(group)], recv_sem=recv.at[0],
                device_id=dev["c"], device_id_type=MESH,
            ).wait_send()
            return
        like = {"i": gi, "o": go, "w": go, "r": part, "s": nown}[group]
        total = sizes[group, None] + (sizes[group, which] if which is not None else 0)
        count, rest = divmod(total, math.prod(like.shape[1:]))
        assert rest == 0 and count <= like.shape[0]
        ref = like.at[pl.ds(0, count)]
        pltpu.make_async_remote_copy(
            src_ref=ref, dst_ref=ref, send_sem=send.at[groups.index(group)], recv_sem=recv.at[0],
            device_id=dev["c"], device_id_type=MESH,
        ).wait_send()

    table = {
        (other, dz, partner): rep_of(
            1 - yl if other else yl, lax.rem(z + dz + NZ, NZ), 1 - c if partner else c
        )
        for other in (0, 1) for dz in range(-4, 5) for partner in (0, 1)
    }

    def piece(other, dz, partner=0):
        return table[int(other), dz, partner]

    me_r, me_t = piece(0, 0), tp
    own_x, own_w, own_o = xg.at[me_t], gi.at[me_r], go.at[me_r]
    fetch = [pltpu.make_async_copy(x_ref, own_x, local.at[0])]
    for h in range(3):
        fetch.append(pltpu.make_async_copy(w_ref.at[h], own_w.at[:, pl.ds(h * 384, 384)], local.at[1 + h]))
    fetch.append(pltpu.make_async_copy(wo_ref, own_o, local.at[4]))
    for copy in fetch:
        copy.start()

    barrier = pltpu.get_barrier_semaphore()
    for d in dev.values():
        pl.semaphore_signal(barrier, inc=1, device_id=d, device_id_type=MESH)
    pl.semaphore_wait(barrier, len(dev))

    fetch[0].wait()
    def image(ref, i):
        return ref.at[pl.ds(i * PATCHES, PATCHES)]

    for i in (0, 1):
        ref = image(own_x, i)
        push("ah" + str(i), ref, ref, "h", "ab"[i])
        for sign in "+-":
            push("ax" + sign + "own" + str(i), ref, ref, "x" + sign, "ab"[i])
    for copy in fetch[1:4]:
        copy.wait()
    rows96 = (pl.ds(0, 96), pl.ds(96, 96))
    for n in (0, 1):
        for sign, m in (("+", n), ("-", 1 - n)):
            ref = gi.at[me_r, rows96[m]]
            push("iz" + sign + "1own" + str(m), ref, ref, "z" + sign)
    push("icown", own_w, own_w, "c")
    fetch[4].wait()

    def rows_of(ref, n):
        rows = ref.shape[0] // 2
        return ref.at[pl.ds(n * rows, rows)]

    def opp(sign):
        return 1 if sign == "+" else -1

    def lead(sign):
        return 0 if sign == "+" else 1

    def take_z(kind, buf, col, sign, d, n):
        ref = rows_of(buf.at[piece(col == "oth", -opp(sign) * d)], n)
        take(kind + "z" + sign + str(d) + col + str(n), ref)

    def push_z(kind, buf, col, sign, d, n):
        ref = rows_of(buf.at[piece(col == "oth", -opp(sign) * (d - 1))], n)
        push(kind + "z" + sign + str(d) + col + str(n), ref, ref, "z" + sign)

    def swap(col, dz):
        ref = gi.at[piece(col == "oth", dz)]
        push("ic" + (col if abs(dz) < 3 or col == "own" else str(abs(dz))), ref, ref, "c")

    def swap_o(wave, col, dz):
        ref = go.at[piece(col == "oth", dz)]
        push("oc" + str(wave), ref, ref, "c", " ow"[wave])

    def cross_o(wave, dz):
        ref = go.at[piece(0, dz)]
        push("oy" + str(wave), ref, ref, "y", " ow"[wave])

    def cross_half(buf, dz, n):
        ref = rows_of(buf.at[piece(0, dz)], n)
        push("iy" + str(dz) + "h" + str(n), ref, ref, "y")

    def take_cross_half(buf, dz, n):
        take("iy" + str(dz) + "h" + str(n), rows_of(buf.at[piece(1, dz)], n))

    def quarter(col, sign, over_y):
        rows = 96 * (1 - lead(sign)) + (0 if over_y else 32)
        return gi.at[piece(col == "oth", -opp(sign) * (2 if over_y else 1)), pl.ds(rows, 32 if over_y else 64)]

    tile = {
        "own+": xm * 2 + yh, "own-": xp * 2 + yh,
        "par+": xm * 2 + 1 - yh, "par-": xp * 2 + 1 - yh,
        "ownf": xf * 2 + yh, "parf": xf * 2 + 1 - yh,
    }

    def acts_half(t, i, sign):
        return xg.at[t, pl.ds(i * PATCHES + lead(sign) * 128, 128)]

    def acts_par(i):
        ref = image(xg.at[x * 2 + 1 - yh], i)
        take("ah" + str(i), ref)
        for sign in "+-":
            push("ax" + sign + "par" + str(i), ref, ref, "x" + sign, "ab"[i])

    def acts_step(who, i):
        for sign in "+-":
            t = tile[who + sign]
            take("ax" + sign + who + str(i), image(xg.at[t], i))
            ref = acts_half(t, i, sign)
            push("ax" + sign + who + "f" + str(i), ref, ref, "x" + sign, "ab"[i])

    def acts_far(who, i):
        for sign in "+-":
            take("ax" + sign + who + "f" + str(i), acts_half(tile[who + "f"], i, sign))

    def relay(kind, buf, col, d, which, onward=True):
        for sign in "+-":
            n = lead(sign) if which == "lead" else 1 - lead(sign)
            take_z(kind, buf, col, sign, d, n)
            if onward and (d < 3 or (d == 3 and which == "lead")):
                push_z(kind, buf, col, sign, d + 1, n)

    def swap_both(col, d):
        for sign in "+-":
            swap(col, -opp(sign) * d)

    def o_ref(col, sign, d, at):
        ref = go.at[piece(col == "oth", -opp(sign) * at)]
        return rows_of(ref, lead(sign)) if d == 4 else ref

    def push_o(col, d):
        for sign in "+-":
            ref = o_ref(col, sign, d, d - 1)
            push("oz" + sign + str(d) + col, ref, ref, "z" + sign)

    def take_o(col, d):
        for sign in "+-":
            take("oz" + sign + str(d) + col, o_ref(col, sign, d, d))

    def offsets(d):
        return (d,) if d in (0, 4) else (-d, d)

    def first_wave(d):
        def step():
            if d:
                take_o("own", d)
            if d < 4:
                push_o("own", d + 1)
            for dz in offsets(d):
                cross_o(1, dz)
                swap_o(1, "own", dz)

        on(d % 2, step)

    def first_wave_over():
        take("oy1", go.at[pl.ds(0, 4)])
        for which in (0, 1):
            def step(which=which):
                for d in range(which, 5, 2):
                    for dz in offsets(d):
                        swap_o(1, "oth", dz)

            on(which, step)

    def second_wave_cross():
        on(1, lambda: cross_o(2, 0))

    def push_two(col, d):
        for step in (2, 1):
            for sign in "+-":
                ref = o_ref(col, sign, d + step, d)
                push("oz" + sign + str(d + step) + col + "w", ref, ref, "z" + sign * step, "w")

    def take_two(col, d):
        for sign in "+-":
            take("oz" + sign + str(d) + col + "w", o_ref(col, sign, d, d))
        for dz in offsets(d):
            swap_o(2, col, dz)

    def second_wave_start():
        def step():
            push_two("own", 0)
            swap_o(2, "own", 0)
            take("oy2", go.at[piece(1, 0)])
            push_two("oth", 0)
            swap_o(2, "oth", 0)

        on(1, step)

    def second_wave_relay(col):
        def step():
            for sign in "+-":
                take("oz" + sign + "2" + col + "w", o_ref(col, sign, 2, 2))
            push_two(col, 2)
            for dz in offsets(2):
                swap_o(2, col, dz)

        on(1, step)

    def second_wave_leaf():
        def even():
            for d in (1, 3):
                for col in ("own", "oth"):
                    take_two(col, d)

        def odd():
            for col in ("own", "oth"):
                take_two(col, 4)

        on(0, even)
        on(1, odd)

    def lane_tiles(t, rows):
        return [xg[t, rows, j * 128:(j + 1) * 128].astype(F32) for j in range(6)]

    def measure(t, image_, first=False):
        def step(i, carry):
            for part_ in range(4):
                rows = pl.ds(pl.multiple_of(i * 128 + part_ * 32, 32), 32)
                tiles = lane_tiles(t, rows)
                total = tiles[0]
                for v in tiles[1:]:
                    total = total + v
                mean = jnp.sum(total, -1, keepdims=True) * (1.0 / 768)
                square = jnp.zeros((32, 128), F32)
                for v in tiles:
                    v = v - mean
                    square = square + v * v
                means[t, rows, :] = jnp.broadcast_to(mean, (32, 128))
                spread[rows, :] = square if first else spread[rows, :] + square
            return carry

        lax.fori_loop(2 * image_, 2 * image_ + 2, step, 0)

    def norm_rows(i, carry):
        for part_ in range(4):
            rows = pl.ds(pl.multiple_of(i * 128 + part_ * 32, 32), 32)
            mean = means[0, rows, :]
            for t in range(1, 8):
                mean = mean + means[t, rows, :]
            mean = mean * (1.0 / 8)
            apart = jnp.zeros((32, 128), F32)
            for t in range(8):
                v = means[t, rows, :] - mean
                apart = apart + v * v
            variance = (jnp.sum(spread[rows, :], -1, keepdims=True) + 768.0 * apart) * (1.0 / D)
            scale = lax.rsqrt(variance + EPS)
            for t in range(8):
                for j, v in enumerate(lane_tiles(t, rows)):
                    gain = gain_ref[pl.ds(t * 768 + j * 128, 128)].reshape(1, 128)
                    xg[t, rows, j * 128:(j + 1) * 128] = ((v - mean) * scale * gain).astype(BF16)
        return carry

    near_k, far_k = yl * 4, (1 - yl) * 4
    last = lax.div(lax.rem(z + 4, NZ), 2)
    odd = lax.rem(z, 2)

    def near_chunks(i, j):
        rows = pl.ds(i * PATCHES, PATCHES)
        total = None
        for k in (near_k + j, near_k + j + 1):
            w = gi[pl.ds(k * 4, 4)].reshape(768, 1152)
            value = jnp.dot(xg[k, rows], w, preferred_element_type=F32)
            total = value if total is None else total + value
        acc[rows] = total if j == 0 else acc[rows] + total

    def far_chunk(j, rows=slice(None)):
        k = far_k + lax.rem(last + (1 + odd, 2 + odd, 3 - 2 * odd, 4)[j], 4)
        return jnp.dot(xg[k, rows], gi[pl.ds(k * 4, 4)].reshape(768, 1152), preferred_element_type=F32)

    for i in (0, 1):
        measure(me_t, i, True)
    relay("i", gi, "own", 1, "lead")
    relay("i", gi, "own", 1, "rest")
    for dz, n in ((1, 1), (-1, 0), (1, 0), (-1, 1)):
        cross_half(gi, dz, n)
    for dz in (1, -1):
        swap("own", dz)
    first_wave(0)
    acts_par(0)
    acts_step("own", 0)
    relay("i", gi, "own", 2, "lead")
    relay("i", gi, "own", 2, "rest")
    for sign in "-+":
        ref = quarter("own", sign, True)
        push("iyq" + sign, ref, ref, "y")
    push("iy0", own_w, own_w, "y")
    second_wave_cross()
    swap_both("own", 2)
    measure(x * 2 + 1 - yh, 0)
    for sign in "+-":
        measure(tile["own" + sign], 0)
    relay("i", gi, "own", 3, "lead")
    first_wave(1)
    acts_step("par", 0)
    acts_par(1)
    acts_step("own", 1)
    for dz, sign in ((1, "-"), (-1, "+")):
        take_cross_half(gi, dz, lead(sign))
        push_z("i", gi, "oth", sign, 2, lead(sign))
    for sign in "+-":
        measure(tile["par" + sign], 0)
    relay("i", gi, "own", 3, "rest")
    swap_both("own", 3)
    acts_far("own", 0)
    measure(tile["ownf"], 0)
    acts_far("par", 0)
    measure(tile["parf"], 0)
    for dz, sign in ((1, "-"), (-1, "+")):
        take_cross_half(gi, dz, 1 - lead(sign))
        ref = quarter("oth", sign, False)
        push("izq" + sign, ref, ref, "z" + sign)
        swap("oth", dz)
    relay("i", gi, "own", 4, "lead", False)
    swap("own", 4)
    sent("a")
    lax.fori_loop(0, 2, norm_rows, 0)
    first_wave(2)
    take("icown", gi.at[pl.ds(0, 8)])
    near_chunks(0, 0)
    relay("i", gi, "oth", 2, "lead")
    acts_step("par", 1)
    near_chunks(0, 2)
    for sign in "+-":
        take("iyq" + sign, quarter("oth", sign, True))
        rows = 96 * (1 - lead(sign)) + 32
        take("izq" + sign, gi.at[piece(1, -2 * opp(sign)), pl.ds(rows, 64)])
        push_z("i", gi, "oth", sign, 3, 1 - lead(sign))
    swap_both("oth", 2)
    measure(x * 2 + 1 - yh, 1)
    for who in ("own", "par"):
        for sign in "+-":
            measure(tile[who + sign], 1)
    acts_far("own", 1)
    measure(tile["ownf"], 1)
    first_wave(3)
    acts_far("par", 1)
    measure(tile["parf"], 1)
    take("iy0", gi.at[piece(1, 0)])
    swap("oth", 0)
    sent("b")
    lax.fori_loop(2, 3, norm_rows, 0)
    relay("i", gi, "oth", 3, "lead")
    lax.fori_loop(3, 4, norm_rows, 0)
    near_chunks(1, 0)
    relay("i", gi, "oth", 3, "rest")
    swap_both("oth", 3)
    first_wave(4)
    near_chunks(1, 2)
    second_wave_start()
    take("icoth", gi.at[pl.ds(0, 5)])
    acc[...] += far_chunk(0) + far_chunk(1)
    take("ic3", gi.at[pl.ds(0, 2)])
    relay("i", gi, "oth", 4, "lead", False)
    swap("oth", 4)
    acc[...] += far_chunk(2)
    first_wave_over()
    take("ic4", gi.at[piece(1, 4, 1)])

    def head_norm(v, gain):
        v = v - jnp.mean(v, -1, keepdims=True)
        var = jnp.mean(v * v, -1, keepdims=True)
        return (v * lax.rsqrt(var + EPS) * gain).astype(BF16)

    def attend(i):
        rows = pl.ds(i * PATCHES, PATCHES)
        acc[rows] += far_chunk(3, rows)
        for h in range(3):
            lo = h * 3 * HEAD_DIM
            q = head_norm(acc[rows, lo:lo + HEAD_DIM], qg_ref[...].reshape(1, HEAD_DIM))
            k = head_norm(acc[rows, lo + HEAD_DIM:lo + 2 * HEAD_DIM], kg_ref[...].reshape(1, HEAD_DIM))
            v = acc[rows, lo + 2 * HEAD_DIM:lo + 3 * HEAD_DIM].astype(BF16)
            s = dot_nt(q, k) / math.sqrt(HEAD_DIM)
            e = jnp.exp(s - jnp.max(s, -1, keepdims=True))
            p = (e / jnp.sum(e, -1, keepdims=True)).astype(BF16)
            o = jnp.dot(p, v, preferred_element_type=F32)
            mixed[rows, h * HEAD_DIM:(h + 1) * HEAD_DIM] = o.astype(BF16)


    def out_part(t, n):
        w = go[pl.ds(t * 4 + n * 2, 2)].reshape(384, 384)
        part[t, n] = dot_nt(mixed[...], w).astype(BF16)

    a_rows, b_rows = pl.ds(0, 256), pl.ds(256, 256)
    span = {"+": a_rows, "-": b_rows}
    other = {"+": b_rows, "-": a_rows}
    near_o = {"+": xp * 2 + yh, "-": xm * 2 + yh}
    near_p = {"+": xp * 2 + 1 - yh, "-": xm * 2 + 1 - yh}
    far_o, far_p = xf * 2 + yh, xf * 2 + 1 - yh
    mine, theirs = x * 2 + yh, x * 2 + 1 - yh
    signs = tuple(enumerate("+-"))

    def launch_near(n, i):
        rows = pl.ds(i * PATCHES, PATCHES)
        w_of = lambda t: go[pl.ds(t * 4 + n * 2, 2)].reshape(384, 384)
        for k, sign in signs:
            t = near_p[sign]
            part[t, n, rows] = dot_nt(mixed[rows], w_of(t)).astype(BF16)
            ref = part.at[t, n, rows]
            push("n" + sign + "p" + str(n) + str(i), ref, r2.at[0, k, n, rows], "x" + sign, "r")

    def launch_far(n, i):
        rows = pl.ds(i * PATCHES, PATCHES)
        w = go[pl.ds(far_p * 4 + n * 2, 2)].reshape(384, 384)
        part[far_p, n, rows] = dot_nt(mixed[rows], w).astype(BF16)
        push("fh" + str(n) + str(i), part.at[far_p, n, rows], r4.at[n, rows], "h", "r")

    def direct(n, j):
        for i, sign in signs:
            rows = pl.ds((256 if sign == "+" else 0) + 128 * j, 128)
            ref = part.at[near_o[sign], n, rows]
            push("n" + sign + "d" + str(n) + str(j), ref, r2.at[1, i, n, rows], "x" + sign, "r")

    def launch_rest(n):
        for i, sign in signs:
            out_part(near_o[sign], n)
        direct(n, 0)
        out_part(far_o, n)
        out_part(theirs, n)
        out_part(mine, n)

    def plus(a, b):
        return (a.astype(F32) + b.astype(F32)).astype(BF16)

    def far(n):
        for i, sign in signs:
            rows = span[sign]
            take("fh" + str(n) + str(i), r4.at[n, rows])
            part[far_o, n, rows] = plus(part[far_o, n, rows], r4[n, rows])
            push("f" + sign + str(n), part.at[far_o, n, rows], r1.at[n, i], "x" + sign, "r")

    def near_add(n):
        for i, sign in signs:
            t, rows = near_o[sign], span[sign]
            take("f" + sign + str(n), r1.at[n, i])
            part[t, n, rows] = plus(part[t, n, rows], r1[n, i])

    def near_push(n):
        for i, sign in signs:
            t, rows = near_o[sign], span[sign]
            push("n" + sign + "s" + str(n), part.at[t, n, rows], r2.at[1, i, n, rows], "x" + sign, "r")

    def hand_over(n):
        for j in (0, 1):
            for i, sign in signs:
                take("n" + sign + "p" + str(n) + str(j), r2.at[0, i, n, pl.ds(j * PATCHES, PATCHES)])
        total = part[theirs, n].astype(F32) + r2[0, 0, n].astype(F32) + r2[0, 1, n].astype(F32)
        tsum[n] = total.astype(BF16)
        push("t" + str(n), tsum.at[n], r3.at[n], "h", "r")

    done = []

    def finish(n):
        take("t" + str(n), r3.at[n])
        for i, sign in signs:
            for j in (0, 1):
                rows = pl.ds((256 if sign == "+" else 0) + 128 * j, 128)
                take("n" + sign + "d" + str(n) + str(j), r2.at[1, i, n, rows])
        for i, sign in signs:
            take("n" + sign + "s" + str(n), r2.at[1, i, n, span[sign]])
            rows = span[sign]
            total = part[mine, n, rows].astype(F32) + r2[1, 0, n, rows].astype(F32)
            total = total + r2[1, 1, n, rows].astype(F32)
            stage[n, rows] = (total + r3[n, rows].astype(F32)).astype(BF16)
            copy = pltpu.make_async_copy(
                stage.at[n, rows], out_ref.at[rows, pl.ds(n * 384, 384)], local.at[2 * n + i]
            )
            copy.start()
            done.append(copy)

    def squares(ref, r, total):
        v = ref[r].astype(F32)
        v = v * v
        row = v[:, :128]
        for j in range(1, v.shape[1] // 128):
            row = row + v[:, j * 128:(j + 1) * 128]
        return total + jnp.sum(row.reshape(24, 8, 128), 0)

    zero = jnp.zeros((8, 128), F32)
    x1 = x + 1 - 2 * lax.rem(x, 2)
    dev["n0"] = dev["c"]
    dev["n1"] = (rep, x1 * 2 + yh)
    dev["n2"] = (rep, (NX - 1 - x) * 2 + yh)
    dev["n3"] = dev["h"]

    def norm_push(k):
        push("norm" + str(k), nown.at[k], nrecv.at[k], "n" + str(k), "s")

    def norm_take(k):
        take("norm" + str(k), nrecv.at[k])
        nown[k + 1] = nown[k] + nrecv[k]

    attend(0)
    take("oc1", go.at[pl.ds(0, 8)])
    launch_near(0, 0)
    launch_far(0, 0)
    second_wave_relay("own")
    attend(1)
    launch_near(0, 1)
    launch_far(0, 1)
    second_wave_relay("oth")
    launch_rest(0)
    nown[0, pl.ds(0, 8), :] = lax.fori_loop(0, 16, lambda r, t: squares(gi, 2 * r + c, t), zero)
    far(0)
    direct(0, 1)
    hand_over(0)
    second_wave_leaf()
    near_add(0)
    near_push(0)
    take("oc2", go.at[pl.ds(0, 8)])
    for i in (0, 1):
        launch_near(1, i)
        launch_far(1, i)
    launch_rest(1)
    nown[0, pl.ds(8, 8), :] = lax.fori_loop(0, 16, lambda r, t: squares(go, 2 * r + c, t), zero)
    norm_push(0)
    norm_take(0)
    norm_push(1)
    hand_over(1)
    far(1)
    direct(1, 1)
    norm_take(1)
    norm_push(2)
    near_add(1)
    near_push(1)
    norm_take(2)
    norm_push(3)
    finish(0)
    norm_take(3)
    total_in = jnp.sum(nown[4, pl.ds(0, 8), :], keepdims=True)
    total_out = jnp.sum(nown[4, pl.ds(8, 8), :], keepdims=True)
    norm_ref[0] = jnp.sqrt(total_in / (3 * HEADS * HEAD_DIM))[0, 0]
    norm_ref[1] = jnp.sqrt(total_out / D)[0, 0]
    finish(1)
    for copy in done:
        copy.wait()
    for group in "irs":
        sent(group)
    for which in (0, 1):
        pl.when(lax.rem(z, 2) == which)(lambda which=which: (sent("o", which), sent("w", which))[0])
    assert len(ids) == NSEM, len(ids)


def deliver(out_ref, norm_ref, to_ref, norms_ref, held, sems, norm_sem):
    norms = pltpu.make_async_copy(norm_ref, norms_ref, norm_sem)
    norms.start()
    parts = held.shape[0]
    rows = held.shape[1]
    into, away = [], []
    for i in range(parts):
        span = pl.ds(i * rows, rows)
        into.append(pltpu.make_async_copy(out_ref.at[span], held.at[i], sems.at[0, i]))
        away.append(pltpu.make_async_copy(held.at[i], to_ref.at[span], sems.at[1, i]))
        into[-1].start()
    for i in range(parts):
        into[i].wait()
        away[i].start()
    for copy in away:
        copy.wait()
    norms.wait()


def shards(activations, norm_gain, query_gain, key_gain, project_in, project_out):
    rows, cols = activations.shape
    hbm = pl.BlockSpec(memory_space=pl.ANY)
    vmem = pl.BlockSpec(memory_space=pltpu.VMEM)
    out, norms = pl.pallas_call(
        kernel,
        name="block",
        out_shape=(jax.ShapeDtypeStruct((rows, cols), BF16), jax.ShapeDtypeStruct((2,), F32)),
        in_specs=[hbm, vmem, vmem, vmem, hbm, hbm],
        out_specs=(hbm, pl.BlockSpec(memory_space=pltpu.SMEM)),
        scratch_shapes=[
            pltpu.VMEM((32, 192, 1152), BF16),
            pltpu.VMEM((32, 192, 384), BF16),
            pltpu.VMEM((8, 512, 768), BF16),
            pltpu.VMEM((8, 512, 128), F32),
            pltpu.VMEM((512, 128), F32),
            pltpu.VMEM((2, 512, 384), BF16),
            pltpu.VMEM((512, 1152), F32),
            pltpu.VMEM((512, 384), BF16),
            pltpu.VMEM((8, 2, 512, 384), BF16),
            pltpu.VMEM((2, 2, 256, 384), BF16),
            pltpu.VMEM((2, 2, 2, 512, 384), BF16),
            pltpu.VMEM((2, 512, 384), BF16),
            pltpu.VMEM((2, 512, 384), BF16),
            pltpu.VMEM((2, 512, 384), BF16),
            pltpu.VMEM((5, 16, 128), F32),
            pltpu.VMEM((4, 16, 128), F32),
            pltpu.SemaphoreType.DMA((7,)),
            pltpu.SemaphoreType.DMA((NSEM,)),
            pltpu.SemaphoreType.DMA((5,)),
        ],
        compiler_params=pltpu.CompilerParams(
            collective_id=0, has_side_effects=True, vmem_limit_bytes=63 * 1024 * 1024
        ),
    )(
        activations,
        norm_gain,
        query_gain,
        key_gain,
        project_in.transpose(1, 0, 2),
        project_out,
    )
    return pl.pallas_call(
        deliver,
        name="deliver",
        out_shape=(jax.ShapeDtypeStruct((rows, cols), BF16), jax.ShapeDtypeStruct((2,), F32)),
        in_specs=(hbm, hbm),
        out_specs=(hbm, hbm),
        scratch_shapes=[pltpu.VMEM((4, rows // 4, cols), BF16), pltpu.SemaphoreType.DMA((2, 4)), pltpu.SemaphoreType.DMA],
        compiler_params=pltpu.CompilerParams(vmem_limit_bytes=63 * 1024 * 1024),
    )(out, norms)


def solution(mesh):
    return jax.shard_map(
        shards,
        mesh=mesh,
        in_specs=(P("rep", "tp"), P(), P(), P(), P("rep", "tp", None), P("rep", "tp")),
        out_specs=(P("rep", "tp"), P()),
        check_vma=False,
    )
```

```python
import math

import jax
import jax.numpy as jnp
from jax import lax
from jax.experimental import pallas as pl
from jax.experimental.pallas import tpu as pltpu
from jax.sharding import PartitionSpec as P

D = 6144
HEADS = 24
HEAD_DIM = 128
PATCHES = 256
NX, NZ = 4, 8
MESH = pl.DeviceIdType.MESH
F32, BF16 = jnp.float32, jnp.bfloat16
EPS = 1e-06
NSEM = 115


def dot_nt(a, b):
    return lax.dot_general(a, b, (((1,), (1,)), ((), ())), preferred_element_type=F32)


def kernel(
    x_ref, gain_ref, qg_ref, kg_ref, w_ref, wo_ref, out_ref, norm_ref,
    gi, go, xg, means, spread, stage, acc, mixed, part, r1, r2, r3, r4, tsum, nown, nrecv,
    send, recv, local,
):
    rep, tp = lax.axis_index("rep"), lax.axis_index("tp")
    c = lax.rem(rep, 2)
    z = lax.rem(lax.div(rep, 2), NZ)
    yl = lax.div(rep, 2 * NZ)
    x, yh = lax.div(tp, 2), lax.rem(tp, 2)

    def rep_of(yl_, z_, c_):
        return (yl_ * NZ + z_) * 2 + c_

    zp, zm = lax.rem(z + 1, NZ), lax.rem(z + NZ - 1, NZ)
    xp, xm = lax.rem(x + 1, NX), lax.rem(x + NX - 1, NX)
    xf = lax.rem(x + 2, NX)
    dev = {
        "z+": (rep_of(yl, zp, c), tp),
        "z-": (rep_of(yl, zm, c), tp),
        "z++": (rep_of(yl, lax.rem(z + 2, NZ), c), tp),
        "z--": (rep_of(yl, lax.rem(z + NZ - 2, NZ), c), tp),
        "c": (rep_of(yl, z, 1 - c), tp),
        "y": (rep_of(1 - yl, z, c), tp),
        "x+": (rep, xp * 2 + yh),
        "x-": (rep, xm * 2 + yh),
        "h": (rep, x * 2 + 1 - yh),
    }

    ids, parity = {}, [None]
    groups = "abiorsw"
    sizes = {(g, which): 0 for g in groups for which in (None, 0, 1)}

    def on(which, action):
        @pl.when(lax.rem(z, 2) == which)
        def _():
            parity[0] = which
            action()
            parity[0] = None

    def ident(name):
        return ids.setdefault(name, len(ids))

    def push(name, src, dst, to, group=None):
        k = ident(name)
        group = group or name[0]
        pltpu.make_async_remote_copy(
            src_ref=src, dst_ref=dst, send_sem=send.at[groups.index(group)], recv_sem=recv.at[k],
            device_id=dev[to], device_id_type=MESH,
        ).start()
        sizes[group, parity[0]] += math.prod(src.shape)

    def take(name, dst):
        k = ident(name)
        pltpu.make_async_remote_copy(
            src_ref=dst, dst_ref=dst, send_sem=send.at[0], recv_sem=recv.at[k],
            device_id=dev["c"], device_id_type=MESH,
        ).wait_recv()

    def sent(group, which=None):
        if group in "ab":
            assert sizes[group, None] == 7 * 256 * 768
            ref = xg.at[pl.ds(0, 7), pl.ds(0, 256)]
            pltpu.make_async_remote_copy(
                src_ref=ref, dst_ref=ref, send_sem=send.at[groups.index(group)], recv_sem=recv.at[0],
                device_id=dev["c"], device_id_type=MESH,
            ).wait_send()
            return
        like = {"i": gi, "o": go, "w": go, "r": part, "s": nown}[group]
        total = sizes[group, None] + (sizes[group, which] if which is not None else 0)
        count, rest = divmod(total, math.prod(like.shape[1:]))
        assert rest == 0 and count <= like.shape[0]
        ref = like.at[pl.ds(0, count)]
        pltpu.make_async_remote_copy(
            src_ref=ref, dst_ref=ref, send_sem=send.at[groups.index(group)], recv_sem=recv.at[0],
            device_id=dev["c"], device_id_type=MESH,
        ).wait_send()

    table = {
        (other, dz, partner): rep_of(
            1 - yl if other else yl, lax.rem(z + dz + NZ, NZ), 1 - c if partner else c
        )
        for other in (0, 1) for dz in range(-4, 5) for partner in (0, 1)
    }

    def piece(other, dz, partner=0):
        return table[int(other), dz, partner]

    me_r, me_t = piece(0, 0), tp
    own_x, own_w, own_o = xg.at[me_t], gi.at[me_r], go.at[me_r]
    fetch = [pltpu.make_async_copy(x_ref, own_x, local.at[0])]
    for h in range(3):
        fetch.append(pltpu.make_async_copy(w_ref.at[h], own_w.at[:, pl.ds(h * 384, 384)], local.at[1 + h]))
    fetch.append(pltpu.make_async_copy(wo_ref, own_o, local.at[4]))
    for copy in fetch:
        copy.start()

    barrier = pltpu.get_barrier_semaphore()
    for d in dev.values():
        pl.semaphore_signal(barrier, inc=1, device_id=d, device_id_type=MESH)
    pl.semaphore_wait(barrier, len(dev))

    fetch[0].wait()
    def image(ref, i):
        return ref.at[pl.ds(i * PATCHES, PATCHES)]

    for i in (0, 1):
        ref = image(own_x, i)
        push("ah" + str(i), ref, ref, "h", "ab"[i])
        for sign in "+-":
            push("ax" + sign + "own" + str(i), ref, ref, "x" + sign, "ab"[i])
    for copy in fetch[1:4]:
        copy.wait()
    rows96 = (pl.ds(0, 96), pl.ds(96, 96))
    for n in (0, 1):
        for sign, m in (("+", n), ("-", 1 - n)):
            ref = gi.at[me_r, rows96[m]]
            push("iz" + sign + "1own" + str(m), ref, ref, "z" + sign)
    push("icown", own_w, own_w, "c")
    fetch[4].wait()

    def rows_of(ref, n):
        rows = ref.shape[0] // 2
        return ref.at[pl.ds(n * rows, rows)]

    def opp(sign):
        return 1 if sign == "+" else -1

    def lead(sign):
        return 0 if sign == "+" else 1

    def take_z(kind, buf, col, sign, d, n):
        ref = rows_of(buf.at[piece(col == "oth", -opp(sign) * d)], n)
        take(kind + "z" + sign + str(d) + col + str(n), ref)

    def push_z(kind, buf, col, sign, d, n):
        ref = rows_of(buf.at[piece(col == "oth", -opp(sign) * (d - 1))], n)
        push(kind + "z" + sign + str(d) + col + str(n), ref, ref, "z" + sign)

    def swap(col, dz):
        ref = gi.at[piece(col == "oth", dz)]
        push("ic" + (col if abs(dz) < 3 or col == "own" else str(abs(dz))), ref, ref, "c")

    def swap_o(wave, col, dz):
        ref = go.at[piece(col == "oth", dz)]
        push("oc" + str(wave), ref, ref, "c", " ow"[wave])

    def cross_o(wave, dz):
        ref = go.at[piece(0, dz)]
        push("oy" + str(wave), ref, ref, "y", " ow"[wave])

    def cross_half(buf, dz, n):
        ref = rows_of(buf.at[piece(0, dz)], n)
        push("iy" + str(dz) + "h" + str(n), ref, ref, "y")

    def take_cross_half(buf, dz, n):
        take("iy" + str(dz) + "h" + str(n), rows_of(buf.at[piece(1, dz)], n))

    def quarter(col, sign, over_y):
        rows = 96 * (1 - lead(sign)) + (0 if over_y else 32)
        return gi.at[piece(col == "oth", -opp(sign) * (2 if over_y else 1)), pl.ds(rows, 32 if over_y else 64)]

    tile = {
        "own+": xm * 2 + yh, "own-": xp * 2 + yh,
        "par+": xm * 2 + 1 - yh, "par-": xp * 2 + 1 - yh,
        "ownf": xf * 2 + yh, "parf": xf * 2 + 1 - yh,
    }

    def acts_half(t, i, sign):
        return xg.at[t, pl.ds(i * PATCHES + lead(sign) * 128, 128)]

    def acts_par(i):
        ref = image(xg.at[x * 2 + 1 - yh], i)
        take("ah" + str(i), ref)
        for sign in "+-":
            push("ax" + sign + "par" + str(i), ref, ref, "x" + sign, "ab"[i])

    def acts_step(who, i):
        for sign in "+-":
            t = tile[who + sign]
            take("ax" + sign + who + str(i), image(xg.at[t], i))
            ref = acts_half(t, i, sign)
            push("ax" + sign + who + "f" + str(i), ref, ref, "x" + sign, "ab"[i])

    def acts_far(who, i):
        for sign in "+-":
            take("ax" + sign + who + "f" + str(i), acts_half(tile[who + "f"], i, sign))

    def relay(kind, buf, col, d, which, onward=True):
        for sign in "+-":
            n = lead(sign) if which == "lead" else 1 - lead(sign)
            take_z(kind, buf, col, sign, d, n)
            if onward and (d < 3 or (d == 3 and which == "lead")):
                push_z(kind, buf, col, sign, d + 1, n)

    def swap_both(col, d):
        for sign in "+-":
            swap(col, -opp(sign) * d)

    def o_ref(col, sign, d, at):
        ref = go.at[piece(col == "oth", -opp(sign) * at)]
        return rows_of(ref, lead(sign)) if d == 4 else ref

    def push_o(col, d):
        for sign in "+-":
            ref = o_ref(col, sign, d, d - 1)
            push("oz" + sign + str(d) + col, ref, ref, "z" + sign)

    def take_o(col, d):
        for sign in "+-":
            take("oz" + sign + str(d) + col, o_ref(col, sign, d, d))

    def offsets(d):
        return (d,) if d in (0, 4) else (-d, d)

    def first_wave(d):
        def step():
            if d:
                take_o("own", d)
            if d < 4:
                push_o("own", d + 1)
            for dz in offsets(d):
                cross_o(1, dz)
                swap_o(1, "own", dz)

        on(d % 2, step)

    def first_wave_over():
        take("oy1", go.at[pl.ds(0, 4)])
        for which in (0, 1):
            def step(which=which):
                for d in range(which, 5, 2):
                    for dz in offsets(d):
                        swap_o(1, "oth", dz)

            on(which, step)

    def second_wave_cross():
        on(1, lambda: cross_o(2, 0))

    def push_two(col, d):
        for step in (2, 1):
            for sign in "+-":
                ref = o_ref(col, sign, d + step, d)
                push("oz" + sign + str(d + step) + col + "w", ref, ref, "z" + sign * step, "w")

    def take_two(col, d):
        for sign in "+-":
            take("oz" + sign + str(d) + col + "w", o_ref(col, sign, d, d))
        for dz in offsets(d):
            swap_o(2, col, dz)

    def second_wave_start():
        def step():
            push_two("own", 0)
            swap_o(2, "own", 0)
            take("oy2", go.at[piece(1, 0)])
            push_two("oth", 0)
            swap_o(2, "oth", 0)

        on(1, step)

    def second_wave_relay(col):
        def step():
            for sign in "+-":
                take("oz" + sign + "2" + col + "w", o_ref(col, sign, 2, 2))
            push_two(col, 2)
            for dz in offsets(2):
                swap_o(2, col, dz)

        on(1, step)

    def second_wave_leaf():
        def even():
            for d in (1, 3):
                for col in ("own", "oth"):
                    take_two(col, d)

        def odd():
            for col in ("own", "oth"):
                take_two(col, 4)

        on(0, even)
        on(1, odd)

    def lane_tiles(t, rows):
        return [xg[t, rows, j * 128:(j + 1) * 128].astype(F32) for j in range(6)]

    def measure(t, image_, first=False):
        def step(i, carry):
            for part_ in range(4):
                rows = pl.ds(pl.multiple_of(i * 128 + part_ * 32, 32), 32)
                tiles = lane_tiles(t, rows)
                total = tiles[0]
                for v in tiles[1:]:
                    total = total + v
                mean = jnp.sum(total, -1, keepdims=True) * (1.0 / 768)
                square = jnp.zeros((32, 128), F32)
                for v in tiles:
                    v = v - mean
                    square = square + v * v
                means[t, rows, :] = jnp.broadcast_to(mean, (32, 128))
                spread[rows, :] = square if first else spread[rows, :] + square
            return carry

        lax.fori_loop(2 * image_, 2 * image_ + 2, step, 0)

    def norm_rows(i, carry):
        for part_ in range(4):
            rows = pl.ds(pl.multiple_of(i * 128 + part_ * 32, 32), 32)
            mean = means[0, rows, :]
            for t in range(1, 8):
                mean = mean + means[t, rows, :]
            mean = mean * (1.0 / 8)
            apart = jnp.zeros((32, 128), F32)
            for t in range(8):
                v = means[t, rows, :] - mean
                apart = apart + v * v
            variance = (jnp.sum(spread[rows, :], -1, keepdims=True) + 768.0 * apart) * (1.0 / D)
            scale = lax.rsqrt(variance + EPS)
            for t in range(8):
                for j, v in enumerate(lane_tiles(t, rows)):
                    gain = gain_ref[pl.ds(t * 768 + j * 128, 128)].reshape(1, 128)
                    xg[t, rows, j * 128:(j + 1) * 128] = ((v - mean) * scale * gain).astype(BF16)
        return carry

    near_k, far_k = yl * 4, (1 - yl) * 4
    last = lax.div(lax.rem(z + 4, NZ), 2)
    odd = lax.rem(z, 2)

    def near_chunks(i, j):
        rows = pl.ds(i * PATCHES, PATCHES)
        total = None
        for k in (near_k + j, near_k + j + 1):
            w = gi[pl.ds(k * 4, 4)].reshape(768, 1152)
            value = jnp.dot(xg[k, rows], w, preferred_element_type=F32)
            total = value if total is None else total + value
        acc[rows] = total if j == 0 else acc[rows] + total

    def far_chunk(j, rows=slice(None)):
        k = far_k + lax.rem(last + (1 + odd, 2 + odd, 3 - 2 * odd, 4)[j], 4)
        return jnp.dot(xg[k, rows], gi[pl.ds(k * 4, 4)].reshape(768, 1152), preferred_element_type=F32)

    for i in (0, 1):
        measure(me_t, i, True)
    relay("i", gi, "own", 1, "lead")
    relay("i", gi, "own", 1, "rest")
    for dz, n in ((1, 1), (-1, 0), (1, 0), (-1, 1)):
        cross_half(gi, dz, n)
    for dz in (1, -1):
        swap("own", dz)
    first_wave(0)
    acts_par(0)
    acts_step("own", 0)
    relay("i", gi, "own", 2, "lead")
    relay("i", gi, "own", 2, "rest")
    for sign in "-+":
        ref = quarter("own", sign, True)
        push("iyq" + sign, ref, ref, "y")
    push("iy0", own_w, own_w, "y")
    second_wave_cross()
    swap_both("own", 2)
    measure(x * 2 + 1 - yh, 0)
    for sign in "+-":
        measure(tile["own" + sign], 0)
    relay("i", gi, "own", 3, "lead")
    first_wave(1)
    acts_step("par", 0)
    acts_par(1)
    acts_step("own", 1)
    for dz, sign in ((1, "-"), (-1, "+")):
        take_cross_half(gi, dz, lead(sign))
        push_z("i", gi, "oth", sign, 2, lead(sign))
    for sign in "+-":
        measure(tile["par" + sign], 0)
    relay("i", gi, "own", 3, "rest")
    swap_both("own", 3)
    acts_far("own", 0)
    measure(tile["ownf"], 0)
    acts_far("par", 0)
    measure(tile["parf"], 0)
    for dz, sign in ((1, "-"), (-1, "+")):
        take_cross_half(gi, dz, 1 - lead(sign))
        ref = quarter("oth", sign, False)
        push("izq" + sign, ref, ref, "z" + sign)
        swap("oth", dz)
    relay("i", gi, "own", 4, "lead", False)
    swap("own", 4)
    sent("a")
    lax.fori_loop(0, 2, norm_rows, 0)
    first_wave(2)
    take("icown", gi.at[pl.ds(0, 8)])
    near_chunks(0, 0)
    relay("i", gi, "oth", 2, "lead")
    acts_step("par", 1)
    near_chunks(0, 2)
    for sign in "+-":
        take("iyq" + sign, quarter("oth", sign, True))
        rows = 96 * (1 - lead(sign)) + 32
        take("izq" + sign, gi.at[piece(1, -2 * opp(sign)), pl.ds(rows, 64)])
        push_z("i", gi, "oth", sign, 3, 1 - lead(sign))
    swap_both("oth", 2)
    measure(x * 2 + 1 - yh, 1)
    for who in ("own", "par"):
        for sign in "+-":
            measure(tile[who + sign], 1)
    acts_far("own", 1)
    measure(tile["ownf"], 1)
    first_wave(3)
    acts_far("par", 1)
    measure(tile["parf"], 1)
    take("iy0", gi.at[piece(1, 0)])
    swap("oth", 0)
    sent("b")
    lax.fori_loop(2, 3, norm_rows, 0)
    relay("i", gi, "oth", 3, "lead")
    lax.fori_loop(3, 4, norm_rows, 0)
    near_chunks(1, 0)
    relay("i", gi, "oth", 3, "rest")
    swap_both("oth", 3)
    first_wave(4)
    near_chunks(1, 2)
    second_wave_start()
    take("icoth", gi.at[pl.ds(0, 5)])
    acc[...] += far_chunk(0) + far_chunk(1)
    take("ic3", gi.at[pl.ds(0, 2)])
    relay("i", gi, "oth", 4, "lead", False)
    swap("oth", 4)
    acc[...] += far_chunk(2)
    first_wave_over()
    take("ic4", gi.at[piece(1, 4, 1)])

    def head_norm(v, gain):
        v = v - jnp.mean(v, -1, keepdims=True)
        var = jnp.mean(v * v, -1, keepdims=True)
        return (v * lax.rsqrt(var + EPS) * gain).astype(BF16)

    def attend(i):
        rows = pl.ds(i * PATCHES, PATCHES)
        acc[rows] += far_chunk(3, rows)
        for h in range(3):
            lo = h * 3 * HEAD_DIM
            q = head_norm(acc[rows, lo:lo + HEAD_DIM], qg_ref[...].reshape(1, HEAD_DIM))
            k = head_norm(acc[rows, lo + HEAD_DIM:lo + 2 * HEAD_DIM], kg_ref[...].reshape(1, HEAD_DIM))
            v = acc[rows, lo + 2 * HEAD_DIM:lo + 3 * HEAD_DIM].astype(BF16)
            s = dot_nt(q, k) / math.sqrt(HEAD_DIM)
            e = jnp.exp(s - jnp.max(s, -1, keepdims=True))
            p = (e / jnp.sum(e, -1, keepdims=True)).astype(BF16)
            o = jnp.dot(p, v, preferred_element_type=F32)
            mixed[rows, h * HEAD_DIM:(h + 1) * HEAD_DIM] = o.astype(BF16)


    def out_part(t, n):
        w = go[pl.ds(t * 4 + n * 2, 2)].reshape(384, 384)
        part[t, n] = dot_nt(mixed[...], w).astype(BF16)

    a_rows, b_rows = pl.ds(0, 256), pl.ds(256, 256)
    span = {"+": a_rows, "-": b_rows}
    other = {"+": b_rows, "-": a_rows}
    near_o = {"+": xp * 2 + yh, "-": xm * 2 + yh}
    near_p = {"+": xp * 2 + 1 - yh, "-": xm * 2 + 1 - yh}
    far_o, far_p = xf * 2 + yh, xf * 2 + 1 - yh
    mine, theirs = x * 2 + yh, x * 2 + 1 - yh
    signs = tuple(enumerate("+-"))

    def launch_near(n, i):
        rows = pl.ds(i * PATCHES, PATCHES)
        w_of = lambda t: go[pl.ds(t * 4 + n * 2, 2)].reshape(384, 384)
        for k, sign in signs:
            t = near_p[sign]
            part[t, n, rows] = dot_nt(mixed[rows], w_of(t)).astype(BF16)
            ref = part.at[t, n, rows]
            push("n" + sign + "p" + str(n) + str(i), ref, r2.at[0, k, n, rows], "x" + sign, "r")

    def launch_far(n, i):
        rows = pl.ds(i * PATCHES, PATCHES)
        w = go[pl.ds(far_p * 4 + n * 2, 2)].reshape(384, 384)
        part[far_p, n, rows] = dot_nt(mixed[rows], w).astype(BF16)
        push("fh" + str(n) + str(i), part.at[far_p, n, rows], r4.at[n, rows], "h", "r")

    def direct(n, j):
        for i, sign in signs:
            rows = pl.ds((256 if sign == "+" else 0) + 128 * j, 128)
            ref = part.at[near_o[sign], n, rows]
            push("n" + sign + "d" + str(n) + str(j), ref, r2.at[1, i, n, rows], "x" + sign, "r")

    def launch_rest(n):
        for i, sign in signs:
            out_part(near_o[sign], n)
        direct(n, 0)
        out_part(far_o, n)
        out_part(theirs, n)
        out_part(mine, n)

    def plus(a, b):
        return (a.astype(F32) + b.astype(F32)).astype(BF16)

    def far(n):
        for i, sign in signs:
            rows = span[sign]
            take("fh" + str(n) + str(i), r4.at[n, rows])
            part[far_o, n, rows] = plus(part[far_o, n, rows], r4[n, rows])
            push("f" + sign + str(n), part.at[far_o, n, rows], r1.at[n, i], "x" + sign, "r")

    def near_add(n):
        for i, sign in signs:
            t, rows = near_o[sign], span[sign]
            take("f" + sign + str(n), r1.at[n, i])
            part[t, n, rows] = plus(part[t, n, rows], r1[n, i])

    def near_push(n):
        for i, sign in signs:
            t, rows = near_o[sign], span[sign]
            push("n" + sign + "s" + str(n), part.at[t, n, rows], r2.at[1, i, n, rows], "x" + sign, "r")

    def hand_over(n):
        for j in (0, 1):
            for i, sign in signs:
                take("n" + sign + "p" + str(n) + str(j), r2.at[0, i, n, pl.ds(j * PATCHES, PATCHES)])
        total = part[theirs, n].astype(F32) + r2[0, 0, n].astype(F32) + r2[0, 1, n].astype(F32)
        tsum[n] = total.astype(BF16)
        push("t" + str(n), tsum.at[n], r3.at[n], "h", "r")

    done = []

    def finish(n):
        take("t" + str(n), r3.at[n])
        for i, sign in signs:
            for j in (0, 1):
                rows = pl.ds((256 if sign == "+" else 0) + 128 * j, 128)
                take("n" + sign + "d" + str(n) + str(j), r2.at[1, i, n, rows])
        for i, sign in signs:
            take("n" + sign + "s" + str(n), r2.at[1, i, n, span[sign]])
            rows = span[sign]
            total = part[mine, n, rows].astype(F32) + r2[1, 0, n, rows].astype(F32)
            total = total + r2[1, 1, n, rows].astype(F32)
            stage[n, rows] = (total + r3[n, rows].astype(F32)).astype(BF16)
            copy = pltpu.make_async_copy(
                stage.at[n, rows], out_ref.at[rows, pl.ds(n * 384, 384)], local.at[2 * n + i]
            )
            copy.start()
            done.append(copy)

    def squares(ref, r, total):
        v = ref[r].astype(F32)
        v = v * v
        row = v[:, :128]
        for j in range(1, v.shape[1] // 128):
            row = row + v[:, j * 128:(j + 1) * 128]
        return total + jnp.sum(row.reshape(24, 8, 128), 0)

    zero = jnp.zeros((8, 128), F32)
    x1 = x + 1 - 2 * lax.rem(x, 2)
    dev["n0"] = dev["c"]
    dev["n1"] = (rep, x1 * 2 + yh)
    dev["n2"] = (rep, (NX - 1 - x) * 2 + yh)
    dev["n3"] = dev["h"]

    def norm_push(k):
        push("norm" + str(k), nown.at[k], nrecv.at[k], "n" + str(k), "s")

    def norm_take(k):
        take("norm" + str(k), nrecv.at[k])
        nown[k + 1] = nown[k] + nrecv[k]

    attend(0)
    take("oc1", go.at[pl.ds(0, 8)])
    launch_near(0, 0)
    launch_far(0, 0)
    second_wave_relay("own")
    attend(1)
    launch_near(0, 1)
    launch_far(0, 1)
    second_wave_relay("oth")
    launch_rest(0)
    nown[0, pl.ds(0, 8), :] = lax.fori_loop(0, 16, lambda r, t: squares(gi, 2 * r + c, t), zero)
    far(0)
    direct(0, 1)
    second_wave_leaf()
    take("oc2", go.at[pl.ds(0, 8)])
    for i in (0, 1):
        launch_near(1, i)
        launch_far(1, i)
    hand_over(0)
    near_add(0)
    near_push(0)
    launch_rest(1)
    nown[0, pl.ds(8, 8), :] = lax.fori_loop(0, 16, lambda r, t: squares(go, 2 * r + c, t), zero)
    norm_push(0)
    far(1)
    direct(1, 1)
    norm_take(0)
    norm_push(1)
    hand_over(1)
    norm_take(1)
    norm_push(2)
    near_add(1)
    near_push(1)
    norm_take(2)
    norm_push(3)
    finish(0)
    finish(1)
    norm_take(3)
    total_in = jnp.sum(nown[4, pl.ds(0, 8), :], keepdims=True)
    total_out = jnp.sum(nown[4, pl.ds(8, 8), :], keepdims=True)
    norm_ref[0] = jnp.sqrt(total_in / (3 * HEADS * HEAD_DIM))[0, 0]
    norm_ref[1] = jnp.sqrt(total_out / D)[0, 0]
    for copy in done:
        copy.wait()
    for group in "irs":
        sent(group)
    for which in (0, 1):
        pl.when(lax.rem(z, 2) == which)(lambda which=which: (sent("o", which), sent("w", which))[0])
    assert len(ids) == NSEM, len(ids)


def deliver(out_ref, norm_ref, to_ref, norms_ref, held, sems, norm_sem):
    norms = pltpu.make_async_copy(norm_ref, norms_ref, norm_sem)
    norms.start()
    parts = held.shape[0]
    rows = held.shape[1]
    into, away = [], []
    for i in range(parts):
        span = pl.ds(i * rows, rows)
        into.append(pltpu.make_async_copy(out_ref.at[span], held.at[i], sems.at[0, i]))
        away.append(pltpu.make_async_copy(held.at[i], to_ref.at[span], sems.at[1, i]))
        into[-1].start()
    for i in range(parts):
        into[i].wait()
        away[i].start()
    for copy in away:
        copy.wait()
    norms.wait()


def shards(activations, norm_gain, query_gain, key_gain, project_in, project_out):
    rows, cols = activations.shape
    hbm = pl.BlockSpec(memory_space=pl.ANY)
    vmem = pl.BlockSpec(memory_space=pltpu.VMEM)
    out, norms = pl.pallas_call(
        kernel,
        name="block",
        out_shape=(jax.ShapeDtypeStruct((rows, cols), BF16), jax.ShapeDtypeStruct((2,), F32)),
        in_specs=[hbm, vmem, vmem, vmem, hbm, hbm],
        out_specs=(hbm, pl.BlockSpec(memory_space=pltpu.SMEM)),
        scratch_shapes=[
            pltpu.VMEM((32, 192, 1152), BF16),
            pltpu.VMEM((32, 192, 384), BF16),
            pltpu.VMEM((8, 512, 768), BF16),
            pltpu.VMEM((8, 512, 128), F32),
            pltpu.VMEM((512, 128), F32),
            pltpu.VMEM((2, 512, 384), BF16),
            pltpu.VMEM((512, 1152), F32),
            pltpu.VMEM((512, 384), BF16),
            pltpu.VMEM((8, 2, 512, 384), BF16),
            pltpu.VMEM((2, 2, 256, 384), BF16),
            pltpu.VMEM((2, 2, 2, 512, 384), BF16),
            pltpu.VMEM((2, 512, 384), BF16),
            pltpu.VMEM((2, 512, 384), BF16),
            pltpu.VMEM((2, 512, 384), BF16),
            pltpu.VMEM((5, 16, 128), F32),
            pltpu.VMEM((4, 16, 128), F32),
            pltpu.SemaphoreType.DMA((7,)),
            pltpu.SemaphoreType.DMA((NSEM,)),
            pltpu.SemaphoreType.DMA((5,)),
        ],
        compiler_params=pltpu.CompilerParams(
            collective_id=0, has_side_effects=True, vmem_limit_bytes=63 * 1024 * 1024
        ),
    )(
        activations,
        norm_gain,
        query_gain,
        key_gain,
        project_in.transpose(1, 0, 2),
        project_out,
    )
    return pl.pallas_call(
        deliver,
        name="deliver",
        out_shape=(jax.ShapeDtypeStruct((rows, cols), BF16), jax.ShapeDtypeStruct((2,), F32)),
        in_specs=(hbm, hbm),
        out_specs=(hbm, hbm),
        scratch_shapes=[pltpu.VMEM((4, rows // 4, cols), BF16), pltpu.SemaphoreType.DMA((2, 4)), pltpu.SemaphoreType.DMA],
        compiler_params=pltpu.CompilerParams(vmem_limit_bytes=63 * 1024 * 1024),
    )(out, norms)


def solution(mesh):
    return jax.shard_map(
        shards,
        mesh=mesh,
        in_specs=(P("rep", "tp"), P(), P(), P(), P("rep", "tp", None), P("rep", "tp")),
        out_specs=(P("rep", "tp"), P()),
        check_vma=False,
    )
```

```python
import math

import jax
import jax.numpy as jnp
from jax import lax
from jax.experimental import pallas as pl
from jax.experimental.pallas import tpu as pltpu
from jax.sharding import PartitionSpec as P

D = 6144
HEADS = 24
HEAD_DIM = 128
PATCHES = 256
NX, NZ = 4, 8
MESH = pl.DeviceIdType.MESH
F32, BF16 = jnp.float32, jnp.bfloat16
EPS = 1e-06
NSEM = 115


def dot_nt(a, b):
    return lax.dot_general(a, b, (((1,), (1,)), ((), ())), preferred_element_type=F32)


def kernel(
    x_ref, gain_ref, qg_ref, kg_ref, w_ref, wo_ref, out_ref, norm_ref,
    gi, go, xg, means, spread, stage, acc, mixed, part, r1, r2, r3, r4, tsum, nown, nrecv,
    send, recv, local,
):
    rep, tp = lax.axis_index("rep"), lax.axis_index("tp")
    c = lax.rem(rep, 2)
    z = lax.rem(lax.div(rep, 2), NZ)
    yl = lax.div(rep, 2 * NZ)
    x, yh = lax.div(tp, 2), lax.rem(tp, 2)

    def rep_of(yl_, z_, c_):
        return (yl_ * NZ + z_) * 2 + c_

    zp, zm = lax.rem(z + 1, NZ), lax.rem(z + NZ - 1, NZ)
    xp, xm = lax.rem(x + 1, NX), lax.rem(x + NX - 1, NX)
    xf = lax.rem(x + 2, NX)
    dev = {
        "z+": (rep_of(yl, zp, c), tp),
        "z-": (rep_of(yl, zm, c), tp),
        "z++": (rep_of(yl, lax.rem(z + 2, NZ), c), tp),
        "z--": (rep_of(yl, lax.rem(z + NZ - 2, NZ), c), tp),
        "c": (rep_of(yl, z, 1 - c), tp),
        "y": (rep_of(1 - yl, z, c), tp),
        "x+": (rep, xp * 2 + yh),
        "x-": (rep, xm * 2 + yh),
        "h": (rep, x * 2 + 1 - yh),
    }

    ids, parity = {}, [None]
    groups = "abiorsw"
    sizes = {(g, which): 0 for g in groups for which in (None, 0, 1)}

    def on(which, action):
        @pl.when(lax.rem(z, 2) == which)
        def _():
            parity[0] = which
            action()
            parity[0] = None

    def ident(name):
        return ids.setdefault(name, len(ids))

    def push(name, src, dst, to, group=None):
        k = ident(name)
        group = group or name[0]
        pltpu.make_async_remote_copy(
            src_ref=src, dst_ref=dst, send_sem=send.at[groups.index(group)], recv_sem=recv.at[k],
            device_id=dev[to], device_id_type=MESH,
        ).start()
        sizes[group, parity[0]] += math.prod(src.shape)

    def take(name, dst):
        k = ident(name)
        pltpu.make_async_remote_copy(
            src_ref=dst, dst_ref=dst, send_sem=send.at[0], recv_sem=recv.at[k],
            device_id=dev["c"], device_id_type=MESH,
        ).wait_recv()

    def sent(group, which=None):
        if group in "ab":
            assert sizes[group, None] == 7 * 256 * 768
            ref = xg.at[pl.ds(0, 7), pl.ds(0, 256)]
            pltpu.make_async_remote_copy(
                src_ref=ref, dst_ref=ref, send_sem=send.at[groups.index(group)], recv_sem=recv.at[0],
                device_id=dev["c"], device_id_type=MESH,
            ).wait_send()
            return
        like = {"i": gi, "o": go, "w": go, "r": part, "s": nown}[group]
        total = sizes[group, None] + (sizes[group, which] if which is not None else 0)
        count, rest = divmod(total, math.prod(like.shape[1:]))
        assert rest == 0 and count <= like.shape[0]
        ref = like.at[pl.ds(0, count)]
        pltpu.make_async_remote_copy(
            src_ref=ref, dst_ref=ref, send_sem=send.at[groups.index(group)], recv_sem=recv.at[0],
            device_id=dev["c"], device_id_type=MESH,
        ).wait_send()

    table = {
        (other, dz, partner): rep_of(
            1 - yl if other else yl, lax.rem(z + dz + NZ, NZ), 1 - c if partner else c
        )
        for other in (0, 1) for dz in range(-4, 5) for partner in (0, 1)
    }

    def piece(other, dz, partner=0):
        return table[int(other), dz, partner]

    me_r, me_t = piece(0, 0), tp
    own_x, own_w, own_o = xg.at[me_t], gi.at[me_r], go.at[me_r]
    fetch = [pltpu.make_async_copy(x_ref, own_x, local.at[0])]
    for h in range(3):
        fetch.append(pltpu.make_async_copy(w_ref.at[h], own_w.at[:, pl.ds(h * 384, 384)], local.at[1 + h]))
    fetch.append(pltpu.make_async_copy(wo_ref, own_o, local.at[4]))
    for copy in fetch:
        copy.start()

    barrier = pltpu.get_barrier_semaphore()
    for d in dev.values():
        pl.semaphore_signal(barrier, inc=1, device_id=d, device_id_type=MESH)
    pl.semaphore_wait(barrier, len(dev))

    fetch[0].wait()
    def image(ref, i):
        return ref.at[pl.ds(i * PATCHES, PATCHES)]

    for i in (0, 1):
        ref = image(own_x, i)
        push("ah" + str(i), ref, ref, "h", "ab"[i])
        for sign in "+-":
            push("ax" + sign + "own" + str(i), ref, ref, "x" + sign, "ab"[i])
    for copy in fetch[1:4]:
        copy.wait()
    rows96 = (pl.ds(0, 96), pl.ds(96, 96))
    for n in (0, 1):
        for sign, m in (("+", n), ("-", 1 - n)):
            ref = gi.at[me_r, rows96[m]]
            push("iz" + sign + "1own" + str(m), ref, ref, "z" + sign)
    push("icown", own_w, own_w, "c")
    fetch[4].wait()

    def rows_of(ref, n):
        rows = ref.shape[0] // 2
        return ref.at[pl.ds(n * rows, rows)]

    def opp(sign):
        return 1 if sign == "+" else -1

    def lead(sign):
        return 0 if sign == "+" else 1

    def take_z(kind, buf, col, sign, d, n):
        ref = rows_of(buf.at[piece(col == "oth", -opp(sign) * d)], n)
        take(kind + "z" + sign + str(d) + col + str(n), ref)

    def push_z(kind, buf, col, sign, d, n):
        ref = rows_of(buf.at[piece(col == "oth", -opp(sign) * (d - 1))], n)
        push(kind + "z" + sign + str(d) + col + str(n), ref, ref, "z" + sign)

    def swap(col, dz):
        ref = gi.at[piece(col == "oth", dz)]
        push("ic" + (col if abs(dz) < 3 or col == "own" else str(abs(dz))), ref, ref, "c")

    def swap_o(wave, col, dz):
        ref = go.at[piece(col == "oth", dz)]
        push("oc" + str(wave), ref, ref, "c", " ow"[wave])

    def cross_o(wave, dz):
        ref = go.at[piece(0, dz)]
        push("oy" + str(wave), ref, ref, "y", " ow"[wave])

    def cross_half(buf, dz, n):
        ref = rows_of(buf.at[piece(0, dz)], n)
        push("iy" + str(dz) + "h" + str(n), ref, ref, "y")

    def take_cross_half(buf, dz, n):
        take("iy" + str(dz) + "h" + str(n), rows_of(buf.at[piece(1, dz)], n))

    def quarter(col, sign, over_y):
        rows = 96 * (1 - lead(sign)) + (0 if over_y else 32)
        return gi.at[piece(col == "oth", -opp(sign) * (2 if over_y else 1)), pl.ds(rows, 32 if over_y else 64)]

    tile = {
        "own+": xm * 2 + yh, "own-": xp * 2 + yh,
        "par+": xm * 2 + 1 - yh, "par-": xp * 2 + 1 - yh,
        "ownf": xf * 2 + yh, "parf": xf * 2 + 1 - yh,
    }

    def acts_half(t, i, sign):
        return xg.at[t, pl.ds(i * PATCHES + lead(sign) * 128, 128)]

    def acts_par(i):
        ref = image(xg.at[x * 2 + 1 - yh], i)
        take("ah" + str(i), ref)
        for sign in "+-":
            push("ax" + sign + "par" + str(i), ref, ref, "x" + sign, "ab"[i])

    def acts_step(who, i):
        for sign in "+-":
            t = tile[who + sign]
            take("ax" + sign + who + str(i), image(xg.at[t], i))
            ref = acts_half(t, i, sign)
            push("ax" + sign + who + "f" + str(i), ref, ref, "x" + sign, "ab"[i])

    def acts_far(who, i):
        for sign in "+-":
            take("ax" + sign + who + "f" + str(i), acts_half(tile[who + "f"], i, sign))

    def relay(kind, buf, col, d, which, onward=True):
        for sign in "+-":
            n = lead(sign) if which == "lead" else 1 - lead(sign)
            take_z(kind, buf, col, sign, d, n)
            if onward and (d < 3 or (d == 3 and which == "lead")):
                push_z(kind, buf, col, sign, d + 1, n)

    def swap_both(col, d):
        for sign in "+-":
            swap(col, -opp(sign) * d)

    def o_ref(col, sign, d, at):
        ref = go.at[piece(col == "oth", -opp(sign) * at)]
        return rows_of(ref, lead(sign)) if d == 4 else ref

    def push_o(col, d):
        for sign in "+-":
            ref = o_ref(col, sign, d, d - 1)
            push("oz" + sign + str(d) + col, ref, ref, "z" + sign)

    def take_o(col, d):
        for sign in "+-":
            take("oz" + sign + str(d) + col, o_ref(col, sign, d, d))

    def offsets(d):
        return (d,) if d in (0, 4) else (-d, d)

    def first_wave(d):
        def step():
            if d:
                take_o("own", d)
            if d < 4:
                push_o("own", d + 1)
            for dz in offsets(d):
                cross_o(1, dz)
                swap_o(1, "own", dz)

        on(d % 2, step)

    def first_wave_over():
        take("oy1", go.at[pl.ds(0, 4)])
        for which in (0, 1):
            def step(which=which):
                for d in range(which, 5, 2):
                    for dz in offsets(d):
                        swap_o(1, "oth", dz)

            on(which, step)

    def second_wave_cross():
        on(1, lambda: cross_o(2, 0))

    def push_two(col, d):
        for step in (2, 1):
            for sign in "+-":
                ref = o_ref(col, sign, d + step, d)
                push("oz" + sign + str(d + step) + col + "w", ref, ref, "z" + sign * step, "w")

    def take_two(col, d):
        for sign in "+-":
            take("oz" + sign + str(d) + col + "w", o_ref(col, sign, d, d))
        for dz in offsets(d):
            swap_o(2, col, dz)

    def second_wave_start():
        def step():
            push_two("own", 0)
            swap_o(2, "own", 0)
            take("oy2", go.at[piece(1, 0)])
            push_two("oth", 0)
            swap_o(2, "oth", 0)

        on(1, step)

    def second_wave_relay(col):
        def step():
            for sign in "+-":
                take("oz" + sign + "2" + col + "w", o_ref(col, sign, 2, 2))
            push_two(col, 2)
            for dz in offsets(2):
                swap_o(2, col, dz)

        on(1, step)

    def second_wave_leaf():
        def even():
            for d in (1, 3):
                for col in ("own", "oth"):
                    take_two(col, d)

        def odd():
            for col in ("own", "oth"):
                take_two(col, 4)

        on(0, even)
        on(1, odd)

    def lane_tiles(t, rows):
        return [xg[t, rows, j * 128:(j + 1) * 128].astype(F32) for j in range(6)]

    def measure(t, image_, first=False):
        def step(i, carry):
            for part_ in range(4):
                rows = pl.ds(pl.multiple_of(i * 128 + part_ * 32, 32), 32)
                tiles = lane_tiles(t, rows)
                total = tiles[0]
                for v in tiles[1:]:
                    total = total + v
                mean = jnp.sum(total, -1, keepdims=True) * (1.0 / 768)
                square = jnp.zeros((32, 128), F32)
                for v in tiles:
                    v = v - mean
                    square = square + v * v
                means[t, rows, :] = jnp.broadcast_to(mean, (32, 128))
                spread[rows, :] = square if first else spread[rows, :] + square
            return carry

        lax.fori_loop(2 * image_, 2 * image_ + 2, step, 0)

    def norm_rows(i, carry):
        for part_ in range(4):
            rows = pl.ds(pl.multiple_of(i * 128 + part_ * 32, 32), 32)
            mean = means[0, rows, :]
            for t in range(1, 8):
                mean = mean + means[t, rows, :]
            mean = mean * (1.0 / 8)
            apart = jnp.zeros((32, 128), F32)
            for t in range(8):
                v = means[t, rows, :] - mean
                apart = apart + v * v
            variance = (jnp.sum(spread[rows, :], -1, keepdims=True) + 768.0 * apart) * (1.0 / D)
            scale = lax.rsqrt(variance + EPS)
            for t in range(8):
                for j, v in enumerate(lane_tiles(t, rows)):
                    gain = gain_ref[pl.ds(t * 768 + j * 128, 128)].reshape(1, 128)
                    xg[t, rows, j * 128:(j + 1) * 128] = ((v - mean) * scale * gain).astype(BF16)
        return carry

    near_k, far_k = yl * 4, (1 - yl) * 4
    last = lax.div(lax.rem(z + 4, NZ), 2)
    odd = lax.rem(z, 2)

    def near_chunks(i, j):
        rows = pl.ds(i * PATCHES, PATCHES)
        total = None
        for k in (near_k + j, near_k + j + 1):
            w = gi[pl.ds(k * 4, 4)].reshape(768, 1152)
            value = jnp.dot(xg[k, rows], w, preferred_element_type=F32)
            total = value if total is None else total + value
        acc[rows] = total if j == 0 else acc[rows] + total

    def far_chunk(j, rows=slice(None)):
        k = far_k + lax.rem(last + (1 + odd, 2 + odd, 3 - 2 * odd, 4)[j], 4)
        return jnp.dot(xg[k, rows], gi[pl.ds(k * 4, 4)].reshape(768, 1152), preferred_element_type=F32)

    for i in (0, 1):
        measure(me_t, i, True)
    relay("i", gi, "own", 1, "lead")
    relay("i", gi, "own", 1, "rest")
    for dz, n in ((1, 1), (-1, 0), (1, 0), (-1, 1)):
        cross_half(gi, dz, n)
    for dz in (1, -1):
        swap("own", dz)
    first_wave(0)
    acts_par(0)
    acts_step("own", 0)
    relay("i", gi, "own", 2, "lead")
    relay("i", gi, "own", 2, "rest")
    for sign in "-+":
        ref = quarter("own", sign, True)
        push("iyq" + sign, ref, ref, "y")
    push("iy0", own_w, own_w, "y")
    second_wave_cross()
    swap_both("own", 2)
    measure(x * 2 + 1 - yh, 0)
    for sign in "+-":
        measure(tile["own" + sign], 0)
    relay("i", gi, "own", 3, "lead")
    first_wave(1)
    acts_step("par", 0)
    acts_par(1)
    acts_step("own", 1)
    for dz, sign in ((1, "-"), (-1, "+")):
        take_cross_half(gi, dz, lead(sign))
        push_z("i", gi, "oth", sign, 2, lead(sign))
    for sign in "+-":
        measure(tile["par" + sign], 0)
    relay("i", gi, "own", 3, "rest")
    swap_both("own", 3)
    acts_far("own", 0)
    measure(tile["ownf"], 0)
    acts_far("par", 0)
    measure(tile["parf"], 0)
    for dz, sign in ((1, "-"), (-1, "+")):
        take_cross_half(gi, dz, 1 - lead(sign))
        ref = quarter("oth", sign, False)
        push("izq" + sign, ref, ref, "z" + sign)
        swap("oth", dz)
    relay("i", gi, "own", 4, "lead", False)
    swap("own", 4)
    sent("a")
    lax.fori_loop(0, 2, norm_rows, 0)
    first_wave(2)
    take("icown", gi.at[pl.ds(0, 8)])
    near_chunks(0, 0)
    relay("i", gi, "oth", 2, "lead")
    acts_step("par", 1)
    near_chunks(0, 2)
    for sign in "+-":
        take("iyq" + sign, quarter("oth", sign, True))
        rows = 96 * (1 - lead(sign)) + 32
        take("izq" + sign, gi.at[piece(1, -2 * opp(sign)), pl.ds(rows, 64)])
        push_z("i", gi, "oth", sign, 3, 1 - lead(sign))
    swap_both("oth", 2)
    measure(x * 2 + 1 - yh, 1)
    for who in ("own", "par"):
        for sign in "+-":
            measure(tile[who + sign], 1)
    acts_far("own", 1)
    measure(tile["ownf"], 1)
    first_wave(3)
    acts_far("par", 1)
    measure(tile["parf"], 1)
    take("iy0", gi.at[piece(1, 0)])
    swap("oth", 0)
    sent("b")
    lax.fori_loop(2, 3, norm_rows, 0)
    relay("i", gi, "oth", 3, "lead")
    lax.fori_loop(3, 4, norm_rows, 0)
    near_chunks(1, 0)
    relay("i", gi, "oth", 3, "rest")
    swap_both("oth", 3)
    first_wave(4)
    near_chunks(1, 2)
    second_wave_start()
    take("icoth", gi.at[pl.ds(0, 5)])
    acc[...] += far_chunk(0) + far_chunk(1)
    take("ic3", gi.at[pl.ds(0, 2)])
    relay("i", gi, "oth", 4, "lead", False)
    swap("oth", 4)
    acc[...] += far_chunk(2)
    first_wave_over()
    take("ic4", gi.at[piece(1, 4, 1)])

    def head_norm(v, gain):
        v = v - jnp.mean(v, -1, keepdims=True)
        var = jnp.mean(v * v, -1, keepdims=True)
        return (v * lax.rsqrt(var + EPS) * gain).astype(BF16)

    def attend(i):
        rows = pl.ds(i * PATCHES, PATCHES)
        acc[rows] += far_chunk(3, rows)
        for h in range(3):
            lo = h * 3 * HEAD_DIM
            q = head_norm(acc[rows, lo:lo + HEAD_DIM], qg_ref[...].reshape(1, HEAD_DIM))
            k = head_norm(acc[rows, lo + HEAD_DIM:lo + 2 * HEAD_DIM], kg_ref[...].reshape(1, HEAD_DIM))
            v = acc[rows, lo + 2 * HEAD_DIM:lo + 3 * HEAD_DIM].astype(BF16)
            s = dot_nt(q, k) / math.sqrt(HEAD_DIM)
            e = jnp.exp(s - jnp.max(s, -1, keepdims=True))
            p = (e / jnp.sum(e, -1, keepdims=True)).astype(BF16)
            o = jnp.dot(p, v, preferred_element_type=F32)
            mixed[rows, h * HEAD_DIM:(h + 1) * HEAD_DIM] = o.astype(BF16)


    def out_part(t, n):
        w = go[pl.ds(t * 4 + n * 2, 2)].reshape(384, 384)
        part[t, n] = dot_nt(mixed[...], w).astype(BF16)

    a_rows, b_rows = pl.ds(0, 256), pl.ds(256, 256)
    span = {"+": a_rows, "-": b_rows}
    other = {"+": b_rows, "-": a_rows}
    near_o = {"+": xp * 2 + yh, "-": xm * 2 + yh}
    near_p = {"+": xp * 2 + 1 - yh, "-": xm * 2 + 1 - yh}
    far_o, far_p = xf * 2 + yh, xf * 2 + 1 - yh
    mine, theirs = x * 2 + yh, x * 2 + 1 - yh
    signs = tuple(enumerate("+-"))

    def launch_near(n, i):
        rows = pl.ds(i * PATCHES, PATCHES)
        w_of = lambda t: go[pl.ds(t * 4 + n * 2, 2)].reshape(384, 384)
        for k, sign in signs:
            t = near_p[sign]
            part[t, n, rows] = dot_nt(mixed[rows], w_of(t)).astype(BF16)
            ref = part.at[t, n, rows]
            push("n" + sign + "p" + str(n) + str(i), ref, r2.at[0, k, n, rows], "x" + sign, "r")

    def launch_far(n, i):
        rows = pl.ds(i * PATCHES, PATCHES)
        w = go[pl.ds(far_p * 4 + n * 2, 2)].reshape(384, 384)
        part[far_p, n, rows] = dot_nt(mixed[rows], w).astype(BF16)
        push("fh" + str(n) + str(i), part.at[far_p, n, rows], r4.at[n, rows], "h", "r")

    def direct(n, j):
        for i, sign in signs:
            rows = pl.ds((256 if sign == "+" else 0) + 128 * j, 128)
            ref = part.at[near_o[sign], n, rows]
            push("n" + sign + "d" + str(n) + str(j), ref, r2.at[1, i, n, rows], "x" + sign, "r")

    def launch_rest(n):
        for i, sign in signs:
            out_part(near_o[sign], n)
        direct(n, 0)
        out_part(far_o, n)
        out_part(theirs, n)
        out_part(mine, n)

    def plus(a, b):
        return (a.astype(F32) + b.astype(F32)).astype(BF16)

    def far(n):
        for i, sign in signs:
            rows = span[sign]
            take("fh" + str(n) + str(i), r4.at[n, rows])
            part[far_o, n, rows] = plus(part[far_o, n, rows], r4[n, rows])
            push("f" + sign + str(n), part.at[far_o, n, rows], r1.at[n, i], "x" + sign, "r")

    def near_add(n):
        for i, sign in signs:
            t, rows = near_o[sign], span[sign]
            take("f" + sign + str(n), r1.at[n, i])
            part[t, n, rows] = plus(part[t, n, rows], r1[n, i])

    def near_push(n):
        for i, sign in signs:
            t, rows = near_o[sign], span[sign]
            push("n" + sign + "s" + str(n), part.at[t, n, rows], r2.at[1, i, n, rows], "x" + sign, "r")

    def hand_over(n):
        for j in (0, 1):
            for i, sign in signs:
                take("n" + sign + "p" + str(n) + str(j), r2.at[0, i, n, pl.ds(j * PATCHES, PATCHES)])
        total = part[theirs, n].astype(F32) + r2[0, 0, n].astype(F32) + r2[0, 1, n].astype(F32)
        tsum[n] = total.astype(BF16)
        push("t" + str(n), tsum.at[n], r3.at[n], "h", "r")

    done = []

    def finish(n):
        take("t" + str(n), r3.at[n])
        for i, sign in signs:
            for j in (0, 1):
                rows = pl.ds((256 if sign == "+" else 0) + 128 * j, 128)
                take("n" + sign + "d" + str(n) + str(j), r2.at[1, i, n, rows])
        for i, sign in signs:
            take("n" + sign + "s" + str(n), r2.at[1, i, n, span[sign]])
            rows = span[sign]
            total = part[mine, n, rows].astype(F32) + r2[1, 0, n, rows].astype(F32)
            total = total + r2[1, 1, n, rows].astype(F32)
            stage[n, rows] = (total + r3[n, rows].astype(F32)).astype(BF16)
            copy = pltpu.make_async_copy(
                stage.at[n, rows], out_ref.at[rows, pl.ds(n * 384, 384)], local.at[2 * n + i]
            )
            copy.start()
            done.append(copy)

    def squares(ref, r, total):
        v = ref[r].astype(F32)
        v = v * v
        row = v[:, :128]
        for j in range(1, v.shape[1] // 128):
            row = row + v[:, j * 128:(j + 1) * 128]
        return total + jnp.sum(row.reshape(24, 8, 128), 0)

    zero = jnp.zeros((8, 128), F32)
    x1 = x + 1 - 2 * lax.rem(x, 2)
    dev["n0"] = dev["c"]
    dev["n1"] = (rep, x1 * 2 + yh)
    dev["n2"] = (rep, (NX - 1 - x) * 2 + yh)
    dev["n3"] = dev["h"]

    def norm_push(k):
        push("norm" + str(k), nown.at[k], nrecv.at[k], "n" + str(k), "s")

    def norm_take(k):
        take("norm" + str(k), nrecv.at[k])
        nown[k + 1] = nown[k] + nrecv[k]

    attend(0)
    take("oc1", go.at[pl.ds(0, 8)])
    launch_near(0, 0)
    launch_far(0, 0)
    second_wave_relay("own")
    attend(1)
    launch_near(0, 1)
    launch_far(0, 1)
    second_wave_relay("oth")
    launch_rest(0)
    nown[0, pl.ds(0, 8), :] = lax.fori_loop(0, 16, lambda r, t: squares(gi, 2 * r + c, t), zero)
    far(0)
    direct(0, 1)
    second_wave_leaf()
    take("oc2", go.at[pl.ds(0, 8)])
    for i in (0, 1):
        launch_near(1, i)
        launch_far(1, i)
    hand_over(0)
    near_add(0)
    near_push(0)
    launch_rest(1)
    nown[0, pl.ds(8, 8), :] = lax.fori_loop(0, 16, lambda r, t: squares(go, 2 * r + c, t), zero)
    norm_push(0)
    norm_take(0)
    norm_push(1)
    far(1)
    direct(1, 1)
    hand_over(1)
    norm_take(1)
    norm_push(2)
    near_add(1)
    near_push(1)
    norm_take(2)
    norm_push(3)
    finish(0)
    finish(1)
    norm_take(3)
    total_in = jnp.sum(nown[4, pl.ds(0, 8), :], keepdims=True)
    total_out = jnp.sum(nown[4, pl.ds(8, 8), :], keepdims=True)
    norm_ref[0] = jnp.sqrt(total_in / (3 * HEADS * HEAD_DIM))[0, 0]
    norm_ref[1] = jnp.sqrt(total_out / D)[0, 0]
    for copy in done:
        copy.wait()
    for group in "irs":
        sent(group)
    for which in (0, 1):
        pl.when(lax.rem(z, 2) == which)(lambda which=which: (sent("o", which), sent("w", which))[0])
    assert len(ids) == NSEM, len(ids)


def deliver(out_ref, norm_ref, to_ref, norms_ref, held, sems, norm_sem):
    norms = pltpu.make_async_copy(norm_ref, norms_ref, norm_sem)
    norms.start()
    parts = held.shape[0]
    rows = held.shape[1]
    into, away = [], []
    for i in range(parts):
        span = pl.ds(i * rows, rows)
        into.append(pltpu.make_async_copy(out_ref.at[span], held.at[i], sems.at[0, i]))
        away.append(pltpu.make_async_copy(held.at[i], to_ref.at[span], sems.at[1, i]))
        into[-1].start()
    for i in range(parts):
        into[i].wait()
        away[i].start()
    for copy in away:
        copy.wait()
    norms.wait()


def shards(activations, norm_gain, query_gain, key_gain, project_in, project_out):
    rows, cols = activations.shape
    hbm = pl.BlockSpec(memory_space=pl.ANY)
    vmem = pl.BlockSpec(memory_space=pltpu.VMEM)
    out, norms = pl.pallas_call(
        kernel,
        name="block",
        out_shape=(jax.ShapeDtypeStruct((rows, cols), BF16), jax.ShapeDtypeStruct((2,), F32)),
        in_specs=[hbm, vmem, vmem, vmem, hbm, hbm],
        out_specs=(hbm, pl.BlockSpec(memory_space=pltpu.SMEM)),
        scratch_shapes=[
            pltpu.VMEM((32, 192, 1152), BF16),
            pltpu.VMEM((32, 192, 384), BF16),
            pltpu.VMEM((8, 512, 768), BF16),
            pltpu.VMEM((8, 512, 128), F32),
            pltpu.VMEM((512, 128), F32),
            pltpu.VMEM((2, 512, 384), BF16),
            pltpu.VMEM((512, 1152), F32),
            pltpu.VMEM((512, 384), BF16),
            pltpu.VMEM((8, 2, 512, 384), BF16),
            pltpu.VMEM((2, 2, 256, 384), BF16),
            pltpu.VMEM((2, 2, 2, 512, 384), BF16),
            pltpu.VMEM((2, 512, 384), BF16),
            pltpu.VMEM((2, 512, 384), BF16),
            pltpu.VMEM((2, 512, 384), BF16),
            pltpu.VMEM((5, 16, 128), F32),
            pltpu.VMEM((4, 16, 128), F32),
            pltpu.SemaphoreType.DMA((7,)),
            pltpu.SemaphoreType.DMA((NSEM,)),
            pltpu.SemaphoreType.DMA((5,)),
        ],
        compiler_params=pltpu.CompilerParams(
            collective_id=0, has_side_effects=True, vmem_limit_bytes=63 * 1024 * 1024
        ),
    )(
        activations,
        norm_gain,
        query_gain,
        key_gain,
        project_in.transpose(1, 0, 2),
        project_out,
    )
    return pl.pallas_call(
        deliver,
        name="deliver",
        out_shape=(jax.ShapeDtypeStruct((rows, cols), BF16), jax.ShapeDtypeStruct((2,), F32)),
        in_specs=(hbm, hbm),
        out_specs=(hbm, hbm),
        scratch_shapes=[pltpu.VMEM((4, rows // 4, cols), BF16), pltpu.SemaphoreType.DMA((2, 4)), pltpu.SemaphoreType.DMA],
        compiler_params=pltpu.CompilerParams(vmem_limit_bytes=63 * 1024 * 1024),
    )(out, norms)


def solution(mesh):
    return jax.shard_map(
        shards,
        mesh=mesh,
        in_specs=(P("rep", "tp"), P(), P(), P(), P("rep", "tp", None), P("rep", "tp")),
        out_specs=(P("rep", "tp"), P()),
        check_vma=False,
    )
```
